32 devices in a mesh: dp: 4 (over y, x), fsdp: 8 (over z, core).
Axes of the slice: x: 2, y: 2, z: 4, core: 2. Of those that a mesh axis runs over, the one named last changes fastest.
Arguments:
- hidden_in: bfloat16 [32768, 1024], P(('dp', 'fsdp')), may hold values from -6 to 6
- w_query: float32 [1048576], P(('dp', 'fsdp')), may hold values from -0.1875 to 0.1875
- w_latent: float32 [524288], P(('dp', 'fsdp')), may hold values from -0.1875 to 0.1875
- w_key_up: float32 [262144], P(('dp', 'fsdp')), may hold values from -0.375 to 0.375
- w_value_up: float32 [262144], P(('dp', 'fsdp')), may hold values from -0.375 to 0.375
- w_decay: float32 [1048576], P(('dp', 'fsdp')), may hold values from -0.1875 to 0.1875
- w_outgate: float32 [1048576], P(('dp', 'fsdp')), may hold values from -0.1875 to 0.1875
- w_out: float32 [1048576], P(('dp', 'fsdp')), may hold values from -0.1875 to 0.1875
- w_gate: float32 [2883584], P(('dp', 'fsdp')), may hold values from -0.1875 to 0.1875
- w_up: float32 [2883584], P(('dp', 'fsdp')), may hold values from -0.1875 to 0.1875
- w_down: float32 [2883584], P(('dp', 'fsdp')), may hold values from -0.109375 to 0.109375
- vectors: float32 [4096], P(('dp', 'fsdp')), may hold values from -3 to 5, as said below
- seg_ids: int32 [32768], P(('dp', 'fsdp')), may hold values from 0 to 127, never falling along the last dimension, each value on 1 to 1024 neighbouring positions
- pad_mask: int32 [32768], P(('dp', 'fsdp')), may hold values 0 or 1
- cotangent: bfloat16 [32768, 1024], P(('dp', 'fsdp')), may hold values from -6 to 6
Outputs:
- block_out: bfloat16 [32768, 1024], P(('dp', 'fsdp'))
- grad_input: float32 [32768, 1024], P(('dp', 'fsdp'))
- grad_query: float32 [1048576], P(('dp', 'fsdp'))
- grad_latent: float32 [524288], P(('dp', 'fsdp'))
- grad_key_up: float32 [262144], P(('dp', 'fsdp'))
- grad_value_up: float32 [262144], P(('dp', 'fsdp'))
- grad_decay: float32 [1048576], P(('dp', 'fsdp'))
- grad_outgate: float32 [1048576], P(('dp', 'fsdp'))
- grad_out: float32 [1048576], P(('dp', 'fsdp'))
- grad_gate: float32 [2883584], P(('dp', 'fsdp'))
- grad_up: float32 [2883584], P(('dp', 'fsdp'))
- grad_down: float32 [2883584], P(('dp', 'fsdp'))
- grad_vectors: float32 [4096], P(('dp', 'fsdp'))
The draws below stay inside these ranges and needn't reach their ends.
Inputs may be any that keep to these rules, and one draw needn't show every extreme that they name: `vectors`: the first 2048 entries and the last 1024 entries are norm gains between 0.5 and 1.5.
All inputs are finite; a program needn't handle non-finite values. No bound on the sum of `pad_mask` on one device may be relied on, other than what follows from the above.
Results may differ from the reference program's by a relative error of at most 0.0095.
The reference program's roundings to bfloat16 on the way count: a program that leaves them out, or rounds other values in their place, can miss the bound.
Values may be sent and summed in bfloat16 or wider, within the bound.
A program may use at most 384 MiB of HBM per device.

```python
import math
from functools import partial
import jax
import jax.numpy as jnp
import numpy as np
from jax import lax

D = 1024
HEADS = 16
HEAD_DIM = 64
GROUPS = 2
LATENT = 256
FF = 2816
LEN = 1024
ROWS = 32
TOKENS = 32768


def draw_vectors(key, part):
    first_key, second_key = jax.random.split(jax.random.fold_in(key, 7))
    width = HEADS * HEAD_DIM
    gains = jax.random.uniform(first_key, (2 * D + width,), jnp.float32, 0.6, 1.4)
    biases = jax.random.uniform(second_key, (width,), jnp.float32, -3.0, 5.0)
    return jnp.concatenate([gains[:2 * D], biases, gains[2 * D:]])


def set_ends(array, own_key, low, high):
    longest = array.shape.index(max(array.shape))
    spots = []
    for shift in (0, 1):
        where = [jax.random.randint(jax.random.fold_in(own_key, axis), (), 0, length) for axis, length in enumerate(array.shape)]
        where[longest] = (where[longest] + shift) % array.shape[longest]
        spots.append(tuple(where))
    return array.at[spots[0]].set(low).at[spots[1]].set(high)


def block_levels(rng, dims, pieces, low, largest):
    def one(position, parts):
        steps = jax.random.uniform(jax.random.fold_in(jax.random.fold_in(rng, 6), position), (parts,), jnp.float32, low / len(pieces), largest / len(pieces))
        return jnp.repeat(jnp.exp(steps), dims[position] // parts).reshape((-1,) + (1,) * (len(dims) - position - 1))

    level = one(*pieces[0])
    for cut in pieces[1:]:
        level = level * one(*cut)
    return level


def length_profile(amount, total, most, slope):
    portions = [(1 << 20) // math.isqrt(standing ** slope) + 1 for standing in range(2, amount + 1)]
    rest, given = total - most - (amount - 1), [1] * (amount - 1)
    while rest > 0:
        movable = [i for i in range(amount - 1) if given[i] < most]
        mass, budget = sum([portions[i] for i in movable]), rest
        for i in movable:
            extra = min(most - given[i], max(1, budget * portions[i] // mass), rest)
            given[i] = given[i] + extra
            rest = rest - extra
    return np.array([most] + given)


def uneven(stream_key, count, total, bound, lean):
    if count == 2:
        one = jax.random.randint(stream_key, (), max(1, total - bound), min(bound, total - 1) + 1)
        return jnp.stack([one, total - one])
    tallies = jnp.asarray(length_profile(count, total, bound, lean), jnp.int32)
    couples = (count - 1) // 2
    donor, receiver = tallies[1:1 + 2 * couples:2], tallies[2:2 + 2 * couples:2]
    margin = jnp.minimum(donor - 1, bound - receiver)
    moved = jax.random.randint(jax.random.fold_in(stream_key, 1), (couples,), 0, 1 << 20) % (margin + 1)
    tallies = tallies.at[1:1 + 2 * couples:2].set(donor - moved).at[2:2 + 2 * couples:2].set(receiver + moved)
    return tallies[jax.random.permutation(jax.random.fold_in(stream_key, 2), count)]


def gaussian(key, extent, scale, limit, pieces=(), held_as=jnp.bfloat16):
    factor_of = block_levels(key, extent, pieces, -0.22, 0.18) if pieces else 1.0
    entries = jax.random.normal(key, extent, jnp.float32) * scale * factor_of
    return jnp.minimum(jnp.maximum(entries, -limit), limit).astype(held_as)


def setup_inputs(seed: int = 0) -> dict:
    key_list = jax.random.split(jax.random.key(seed), 16)
    return {
        "hidden_in": gaussian(key_list[0], (TOKENS, D), 1.0, 6.0, ((0, 32),)),
        "w_query": gaussian(key_list[1], (D * HEADS * HEAD_DIM,), D ** -0.5, 0.1875, ((0, 32),), jnp.float32),
        "w_latent": gaussian(key_list[2], (D * GROUPS * LATENT,), D ** -0.5, 0.1875, ((0, 32),), jnp.float32),
        "w_key_up": gaussian(key_list[3], (GROUPS * LATENT * (HEADS // GROUPS) * HEAD_DIM,), LATENT ** -0.5, 0.375, ((0, 32),), jnp.float32),
        "w_value_up": gaussian(key_list[4], (GROUPS * LATENT * (HEADS // GROUPS) * HEAD_DIM,), LATENT ** -0.5, 0.375, ((0, 32),), jnp.float32),
        "w_decay": gaussian(key_list[5], (D * HEADS * HEAD_DIM,), D ** -0.5, 0.1875, ((0, 32),), jnp.float32),
        "w_outgate": gaussian(key_list[6], (D * HEADS * HEAD_DIM,), D ** -0.5, 0.1875, ((0, 32),), jnp.float32),
        "w_out": gaussian(key_list[7], (HEADS * HEAD_DIM * D,), (HEADS * HEAD_DIM) ** -0.5, 0.1875, ((0, 32),), jnp.float32),
        "w_gate": gaussian(key_list[8], (D * FF,), D ** -0.5, 0.1875, ((0, 32),), jnp.float32),
        "w_up": gaussian(key_list[9], (D * FF,), D ** -0.5, 0.1875, ((0, 32),), jnp.float32),
        "w_down": gaussian(key_list[10], (FF * D,), FF ** -0.5, 0.109375, ((0, 32),), jnp.float32),
        "vectors": draw_vectors(jax.random.fold_in(key_list[15], 71), 0),
        "seg_ids": jnp.searchsorted(jnp.cumsum(uneven(key_list[12], 4 * ROWS, TOKENS, LEN, 2)), jnp.arange(TOKENS), side="right").astype(jnp.int32),
        "pad_mask": set_ends((jax.random.randint(key_list[13], (TOKENS,), 0, 8) < 7).astype(jnp.int32), jax.random.fold_in(key_list[13], 1), 0, 1),
        "cotangent": gaussian(key_list[14], (TOKENS, D), 1.0, 6.0, ((0, 32),)),
    }


@jax.custom_vjp
def low(v):
    return lax.optimization_barrier(v.astype(jnp.bfloat16)).astype(jnp.float32)

@jax.custom_vjp
def low_back(v):
    return v

def low_keep(v):
    return (low(v), None)

def low_pass(kept, grad):
    return (grad,)

def back_keep(v):
    return (v, None)

def back_low(kept, grad):
    return (low(grad),)
low.defvjp(low_keep, low_pass)
low_back.defvjp(back_keep, back_low)
highest = lax.Precision.HIGHEST

def matmul(left, right):
    return jnp.dot(left, right, preferred_element_type=jnp.float32, precision=highest)

def rms_scale(values, gain_vec):
    return values * lax.rsqrt(lax.optimization_barrier(jnp.mean(values * values, axis=-1, keepdims=True)) + 1e-05) * gain_vec

def up_project(latent, weight):
    grouped = latent.reshape(latent.shape[0], GROUPS, LATENT)
    result = jnp.einsum('tgl,glm->tgm', grouped, weight, precision=highest)
    return result.reshape(latent.shape[0], -1)

def mixer_row(query, keys, values, decay_in, gate_in, out_gain, keep_flag, pad_flag):
    log_decay = jax.nn.log_sigmoid(decay_in) / 16.0 * pad_flag[:, None]
    scaled = (query * HEAD_DIM ** (-0.5)).reshape(LEN, HEADS, HEAD_DIM)
    masked = (keys * pad_flag[:, None]).reshape(LEN, HEADS, HEAD_DIM)
    value_rows = values.reshape(LEN, HEADS, HEAD_DIM)
    decay_rows = log_decay.reshape(LEN, HEADS, HEAD_DIM)

    def advance(carry_state, inputs):
        query_t, key_t, value_t, decay_t, flag_t = inputs
        carry_state = carry_state * (flag_t * jnp.exp(decay_t))[:, :, None] + key_t[:, :, None] * value_t[:, None, :]
        result = jnp.einsum('hd,hde->he', query_t, carry_state, precision=highest)
        return (carry_state, result)
    start_state = jnp.zeros((HEADS, HEAD_DIM, HEAD_DIM), jnp.float32)
    _, heads_out = lax.scan(advance, start_state, (scaled, masked, value_rows, decay_rows, keep_flag))
    normed = heads_out * lax.rsqrt(lax.optimization_barrier(jnp.mean(heads_out * heads_out, axis=-1, keepdims=True)) + 0.01)
    return normed.reshape(LEN, HEADS * HEAD_DIM) * out_gain * jax.nn.silu(gate_in)

def layer_row(row_data, weights):
    inputs, keep_flag, pad_flag = row_data
    w_query, w_latent, w_keyup, w_valup, w_decay, w_outgate, w_output, w_gate, w_upward, w_down, vector_all = weights
    width = HEADS * HEAD_DIM
    gain_in = vector_all[:D]
    gain_mid = vector_all[D:2 * D]
    decay_bias = vector_all[2 * D:2 * D + width]
    out_gain = vector_all[2 * D + width:]
    normed = low(rms_scale(inputs, gain_in))
    query = low_back(matmul(normed, w_query))
    latent = low(low_back(matmul(normed, w_latent)))
    keys = low_back(up_project(latent, w_keyup))
    values = low_back(up_project(latent, w_valup))
    decay_in = low_back(matmul(normed, w_decay)) + decay_bias
    gate_in = low_back(matmul(normed, w_outgate))
    mixed = low(mixer_row(query, keys, values, decay_in, gate_in, out_gain, keep_flag, pad_flag))
    middle = inputs + low_back(matmul(mixed, w_output))
    normed_mid = low(rms_scale(middle, gain_mid))
    gate_val = low_back(matmul(normed_mid, w_gate))
    up_val = low_back(matmul(normed_mid, w_upward))
    hidden = low(jax.nn.silu(gate_val) * up_val)
    return middle + low_back(matmul(hidden, w_down))

def shape_weights(params):
    width = HEADS * HEAD_DIM
    per_group = HEADS // GROUPS * HEAD_DIM
    return (params[0].reshape(D, width), params[1].reshape(D, GROUPS * LATENT), params[2].reshape(GROUPS, LATENT, per_group), params[3].reshape(GROUPS, LATENT, per_group), params[4].reshape(D, width), params[5].reshape(D, width), params[6].reshape(width, D), params[7].reshape(D, FF), params[8].reshape(D, FF), params[9].reshape(FF, D), params[10])

def reference(hidden_in, w_query, w_latent, w_key_up, w_value_up, w_decay, w_outgate, w_out, w_gate, w_up, w_down, vectors, seg_ids, pad_mask, cotangent):
    seg_rows = seg_ids.reshape(ROWS, LEN)
    same_doc = (seg_rows[:, 1:] == seg_rows[:, :-1]).astype(jnp.float32)
    keep_rows = jnp.concatenate([jnp.zeros((ROWS, 1), jnp.float32), same_doc], axis=1)
    pad_flag = pad_mask.astype(jnp.float32)
    pad_rows = pad_flag.reshape(ROWS, LEN)

    def forward(inputs, *params):
        weights = shape_weights([low(piece) for piece in params])
        rows_in = inputs.reshape(ROWS, LEN, D)
        row_step = jax.checkpoint(partial(layer_row, weights=weights))
        result = lax.map(row_step, (rows_in, keep_rows, pad_rows))
        return result.reshape(ROWS * LEN, D)
    block_out, pull = jax.vjp(forward, hidden_in.astype(jnp.float32), w_query, w_latent, w_key_up, w_value_up, w_decay, w_outgate, w_out, w_gate, w_up, w_down, vectors)
    grads = pull(cotangent.astype(jnp.float32) * pad_flag[:, None])
    return (block_out.astype(jnp.bfloat16), grads[0], grads[1], grads[2], grads[3], grads[4], grads[5], grads[6], grads[7], grads[8], grads[9], grads[10], grads[11])
```

```python
from functools import partial

import jax
import jax.numpy as jnp
from jax import lax
from jax.experimental import pallas as pl
from jax.experimental.pallas import tpu as pltpu
from jax.sharding import PartitionSpec as P

D = 1024
HEADS = 16
HEAD_DIM = 64
GROUPS = 2
LATENT = 256
FF = 2816
LEN = 1024
WIDTH = HEADS * HEAD_DIM
SPAN = 128
LANES = 256
PACK = LANES // HEAD_DIM
BANDS = WIDTH // LANES
CHUNKS = LEN // SPAN
LIMIT = 85.0
AXES = ("dp", "fsdp")
BF = jnp.bfloat16
F32 = jnp.float32


def mm(left, right):
    return lax.dot_general(left, right, (((1,), (0,)), ((), ())), preferred_element_type=F32)


def mm_nt(left, right):
    return lax.dot_general(left, right, (((1,), (1,)), ((), ())), preferred_element_type=F32)


def mm_tn(left, right):
    return lax.dot_general(left, right, (((0,), (0,)), ((), ())), preferred_element_type=F32)


def halves(value):
    high = value.astype(BF)
    return high, (value - high.astype(F32)).astype(BF)


def exact_left(ones, value):
    high, rest = halves(value)
    return mm(ones, high) + mm(ones, rest)


def exact_right(value, ones):
    high, rest = halves(value)
    return mm(high, ones) + mm(rest, ones)


def head_masks():
    lane = lax.broadcasted_iota(jnp.int32, (1, LANES), 1) // HEAD_DIM
    return [lane == head for head in range(PACK)]


def stacked(value, masks):
    zero = jnp.zeros_like(value)
    return jnp.concatenate([jnp.where(mask, value, zero) for mask in masks], axis=0)


def side_by_side(value):
    return jnp.concatenate([value[h * SPAN : (h + 1) * SPAN] for h in range(PACK)], axis=1)


def same_head():
    row = lax.broadcasted_iota(jnp.int32, (LANES, LANES), 0) // HEAD_DIM
    col = lax.broadcasted_iota(jnp.int32, (LANES, LANES), 1) // HEAD_DIM
    return row == col


def triangle(lower):
    row = lax.broadcasted_iota(jnp.int32, (SPAN, SPAN), 0)
    col = lax.broadcasted_iota(jnp.int32, (SPAN, SPAN), 1)
    return (row >= col) if lower else (row <= col)


def decays(decay, pad, lower_ones):
    small = jnp.exp(-jnp.abs(decay))
    log_sig = jnp.minimum(decay, 0.0) - jnp.log(1.0 + small)
    total = exact_left(lower_ones, log_sig * (pad * (1.0 / 16.0)))
    ending = total[SPAN - 1 : SPAN]
    middle = 0.5 * ending
    centred = total - middle
    up = jnp.exp(jnp.minimum(centred, LIMIT))
    down = jnp.exp(jnp.minimum(-centred, LIMIT))
    half = jnp.exp(middle)
    return up, down, half, small


def flags(cols_ref, seg_ref, rows, index):
    cols = cols_ref[rows, :]
    seg_col, fresh, to_end, pad = cols[:, 0:1], cols[:, 1:2], cols[:, 2:3], cols[:, 3:4]
    allowed = (seg_col == seg_ref[index]) & triangle(True)
    return fresh, to_end, pad, allowed, fresh[SPAN - 1 : SPAN]


def mixer_fwd_kernel(
    q_ref, k_ref, v_ref, decay_ref, gate_ref, gain_ref, cols_ref, seg_ref, mixed_ref, heads_ref, states_ref, state
):
    masks = head_masks()
    diag = same_head()
    diag_ones = diag.astype(F32).astype(BF)
    lower_ones = triangle(True).astype(F32).astype(BF)
    state[...] = jnp.zeros_like(state)
    gain = gain_ref[...]

    def chunk(index, carry):
        rows = pl.ds(pl.multiple_of(index * SPAN, SPAN), SPAN)
        fresh, to_end, pad, allowed, keep = flags(cols_ref, seg_ref, rows, index)
        up, down, half, _ = decays(decay_ref[rows, :], pad, lower_ones)
        query = q_ref[rows, :] * (HEAD_DIM**-0.5) * up
        key = k_ref[rows, :] * pad * down
        value = v_ref[rows, :].astype(BF)
        query_low, key_low = query.astype(BF), key.astype(BF)
        scores = mm_nt(stacked(query_low, masks), key_low)
        scores = scores.reshape(PACK, SPAN, SPAN)
        scores = jnp.where(allowed[None], scores, 0.0).astype(BF).reshape(PACK * SPAN, SPAN)
        old = state[...]
        old_low = old.astype(BF)
        states_ref[0, index] = old_low
        heads = mm(side_by_side(scores), stacked(value, masks))
        heads += mm_nt((query * (half * fresh)).astype(BF), old_low)
        tail = (key * (half * to_end)).astype(BF)
        state[...] = old * (half * half * keep) + jnp.where(diag, mm_tn(value, tail), 0.0)
        heads_ref[rows, :] = heads
        scale = lax.rsqrt(exact_right(heads * heads, diag_ones) * (1.0 / HEAD_DIM) + 1e-2)
        gate = gate_ref[rows, :]
        silu = gate / (1.0 + jnp.exp(-gate))
        mixed_ref[rows, :] = (heads * scale * gain * silu).astype(BF)
        return carry

    lax.fori_loop(0, CHUNKS, chunk, 0)


def mixer_bwd_kernel(
    q_ref,
    k_ref,
    v_ref,
    decay_ref,
    gate_ref,
    gain_ref,
    cols_ref,
    seg_ref,
    heads_ref,
    states_ref,
    dmix_ref,
    dq_ref,
    dk_ref,
    dv_ref,
    ddecay_ref,
    dgate_ref,
    dbias_ref,
    dgain_ref,
    state,
):
    masks = head_masks()
    diag = same_head()
    diag_ones = diag.astype(F32).astype(BF)
    lower_ones = triangle(True).astype(F32).astype(BF)
    upper_ones = triangle(False).astype(F32).astype(BF)
    state[...] = jnp.zeros_like(state)
    dbias_ref[...] = jnp.zeros_like(dbias_ref)
    dgain_ref[...] = jnp.zeros_like(dgain_ref)
    gain = gain_ref[...]

    def chunk(step, carry):
        index = CHUNKS - 1 - step
        rows = pl.ds(pl.multiple_of(index * SPAN, SPAN), SPAN)
        fresh, to_end, pad, allowed, keep = flags(cols_ref, seg_ref, rows, index)
        heads = heads_ref[rows, :]
        scale = lax.rsqrt(exact_right(heads * heads, diag_ones) * (1.0 / HEAD_DIM) + 1e-2)
        normed = heads * scale
        gate = gate_ref[rows, :]
        sig = 1.0 / (1.0 + jnp.exp(-gate))
        silu = gate * sig
        dmix = dmix_ref[rows, :]
        both = dmix * normed
        dgain_ref[...] += jnp.sum(both * silu, axis=0, keepdims=True)
        dgate_ref[rows, :] = (both * gain * (sig * (1.0 + gate * (1.0 - sig)))).astype(BF)
        dnormed = dmix * gain * silu
        mean = exact_right(dnormed * normed, diag_ones) * (1.0 / HEAD_DIM)
        dheads = (scale * (dnormed - normed * mean)).astype(BF)
        decay = decay_ref[rows, :]
        up, down, half, small = decays(decay, pad, lower_ones)
        unit = HEAD_DIM**-0.5
        query = q_ref[rows, :] * unit * up
        key = k_ref[rows, :] * pad * down
        value = v_ref[rows, :].astype(BF)
        query_low, key_low = query.astype(BF), key.astype(BF)
        enter = half * fresh
        leave = half * to_end
        query_in = (query * enter).astype(BF)
        tail = (key * leave).astype(BF)
        query_stack = stacked(query_low, masks)
        dheads_stack = stacked(dheads, masks)
        scores = mm_nt(query_stack, key_low).reshape(PACK, SPAN, SPAN)
        scores = jnp.where(allowed[None], scores, 0.0).astype(BF).reshape(PACK * SPAN, SPAN)
        dscores = mm_nt(dheads_stack, value).reshape(PACK, SPAN, SPAN)
        dscores = jnp.where(allowed[None], dscores, 0.0).astype(BF).reshape(PACK * SPAN, SPAN)
        dstate = state[...]
        dstate_low = dstate.astype(BF)
        old = states_ref[0, index]
        dvalue = mm_tn(scores, dheads_stack) + mm_nt(tail, dstate_low)
        dv_ref[rows, :] = dvalue.astype(BF)
        dquery = mm(side_by_side(dscores), stacked(key_low, masks))
        dkey = mm_tn(dscores, query_stack)
        dquery_in = mm(dheads, old)
        dtail = mm(value, dstate_low)
        whole = half * half * keep
        state[...] = dstate * whole + jnp.where(diag, mm_tn(dheads, query_in), 0.0)
        dq_ref[rows, :] = ((dquery + dquery_in * enter) * (up * unit)).astype(BF)
        dk_ref[rows, :] = ((dkey + dtail * leave) * (down * pad)).astype(BF)
        from_tail = dtail * tail.astype(F32)
        dtotal = (
            dquery * query_low.astype(F32)
            - dkey * key_low.astype(F32)
            + dquery_in * query_in.astype(F32)
            - from_tail
        )
        ends = jnp.sum(from_tail, axis=0, keepdims=True)
        ends += whole * jnp.sum(dstate * old.astype(F32), axis=0, keepdims=True)
        dlog = exact_left(upper_ones, dtotal) + ends
        other = jnp.where(decay >= 0, small, 1.0) / (1.0 + small)
        ddecay = dlog * (pad * (1.0 / 16.0)) * other
        dbias_ref[...] += jnp.sum(ddecay, axis=0, keepdims=True)
        ddecay_ref[rows, :] = ddecay.astype(BF)
        return carry

    lax.fori_loop(0, CHUNKS, chunk, 0)


def band_specs():
    tokens = pl.BlockSpec((LEN, LANES), lambda band: (0, band))
    vector = pl.BlockSpec((1, LANES), lambda band: (0, band))
    cols = pl.BlockSpec((LEN, 128), lambda band: (0, 0))
    segs = pl.BlockSpec((CHUNKS, 1, SPAN), lambda band: (0, 0, 0))
    states = pl.BlockSpec((1, CHUNKS, LANES, LANES), lambda band: (band, 0, 0, 0))
    return tokens, vector, cols, segs, states


def mixer_fwd(query, keys, values, decay_in, gate_in, out_gain, cols, segs):
    tokens, vector, cols_spec, segs_spec, states = band_specs()
    return pl.pallas_call(
        mixer_fwd_kernel,
        grid=(BANDS,),
        in_specs=[tokens] * 5 + [vector, cols_spec, segs_spec],
        out_specs=[tokens, tokens, states],
        out_shape=[
            jax.ShapeDtypeStruct((LEN, WIDTH), BF),
            jax.ShapeDtypeStruct((LEN, WIDTH), F32),
            jax.ShapeDtypeStruct((BANDS, CHUNKS, LANES, LANES), BF),
        ],
        scratch_shapes=[pltpu.VMEM((LANES, LANES), F32)],
        compiler_params=pltpu.CompilerParams(vmem_limit_bytes=48 << 20),
        name="mixer_fwd",
    )(query, keys, values, decay_in, gate_in, out_gain, cols, segs)


def mixer_bwd(query, keys, values, decay_in, gate_in, out_gain, cols, segs, heads, states_in, dmix):
    tokens, vector, cols_spec, segs_spec, states = band_specs()
    low = jax.ShapeDtypeStruct((LEN, WIDTH), BF)
    sums = jax.ShapeDtypeStruct((1, WIDTH), F32)
    return pl.pallas_call(
        mixer_bwd_kernel,
        grid=(BANDS,),
        in_specs=[tokens] * 5 + [vector, cols_spec, segs_spec, tokens, states, tokens],
        out_specs=[tokens] * 5 + [vector, vector],
        out_shape=[low] * 5 + [sums, sums],
        scratch_shapes=[pltpu.VMEM((LANES, LANES), F32)],
        compiler_params=pltpu.CompilerParams(vmem_limit_bytes=56 << 20),
        name="mixer_bwd",
    )(query, keys, values, decay_in, gate_in, out_gain, cols, segs, heads, states_in, dmix)


def rms_factor(values, eps):
    return lax.rsqrt(jnp.mean(values * values, axis=-1, keepdims=True) + eps)


def rms_back(grad, values, factor, gain):
    scaled = values * factor
    dscaled = grad * gain
    dvalues = factor * (dscaled - scaled * jnp.mean(dscaled * scaled, axis=-1, keepdims=True))
    return dvalues, jnp.sum(grad * scaled, axis=0)


def gather(shards):
    return [lax.all_gather(piece, AXES, axis=0) for piece in shards]


def scatter(grads):
    return [lax.psum_scatter(piece, AXES, scatter_dimension=0) for piece in grads]


def per_device(
    hidden_in,
    w_query,
    w_latent,
    w_key_up,
    w_value_up,
    w_decay,
    w_outgate,
    w_out,
    w_gate,
    w_up,
    w_down,
    vectors,
    seg_ids,
    pad_mask,
    cotangent,
    *,
    count,
):
    per_group = WIDTH // GROUPS
    latents = GROUPS * LATENT
    rows_d, rows_kv, rows_ff = D // count, latents // count, FF // count

    def rows_of(piece, rows):
        return piece.astype(BF).reshape(rows, -1)

    in_shard = jnp.concatenate(
        [rows_of(piece, rows_d) for piece in (w_query, w_decay, w_outgate, w_latent)], axis=1
    )
    kv_shard = jnp.concatenate([rows_of(w_key_up, rows_kv), rows_of(w_value_up, rows_kv)], axis=1)
    out_shard = rows_of(w_out, rows_d)
    ff_shard = jnp.concatenate([rows_of(w_gate, rows_d), rows_of(w_up, rows_d)], axis=1)
    down_shard = rows_of(w_down, rows_ff)
    vec_shard = rows_of(vectors, 1)
    w_in, w_kv, w_output, w_ff, w_dn, vecs = gather(
        (in_shard, kv_shard, out_shard, ff_shard, down_shard, vec_shard)
    )
    w_in = w_in.reshape(D, 3 * WIDTH + latents)
    w_kv = w_kv.reshape(GROUPS, LATENT, 2 * per_group)
    w_output = w_output.reshape(WIDTH, D)
    w_ff = w_ff.reshape(D, 2 * FF)
    w_dn = w_dn.reshape(FF, D)
    vecs = vecs.reshape(-1).astype(F32)
    gain_in, gain_mid = vecs[:D], vecs[D : 2 * D]
    decay_bias, out_gain = vecs[2 * D : 2 * D + WIDTH], vecs[2 * D + WIDTH :]

    seg = seg_ids.reshape(CHUNKS, SPAN)
    before = jnp.concatenate([jnp.full((1,), -1, seg.dtype), seg[:-1, -1]])
    fresh = (seg == before[:, None]).astype(F32).reshape(LEN, 1)
    to_end = (seg == seg[:, -1:]).astype(F32).reshape(LEN, 1)
    pad = pad_mask.astype(F32).reshape(LEN, 1)
    seg_col = seg_ids.astype(F32).reshape(LEN, 1)
    cols = jnp.concatenate(
        [seg_col, fresh, to_end, pad, jnp.zeros((LEN, 124), F32)], axis=1
    )
    segs = seg_ids.astype(F32).reshape(CHUNKS, 1, SPAN)

    inputs = hidden_in.astype(F32)
    factor_in = rms_factor(inputs, 1e-5)
    normed = (inputs * factor_in * gain_in).astype(BF)
    query = mm(normed, w_in[:, :WIDTH])
    decay_in = mm(normed, w_in[:, WIDTH : 2 * WIDTH]) + decay_bias
    gate_in = mm(normed, w_in[:, 2 * WIDTH : 3 * WIDTH])
    latent = mm(normed, w_in[:, 3 * WIDTH :]).astype(BF)
    keys = jnp.concatenate(
        [mm(latent[:, g * LATENT : (g + 1) * LATENT], w_kv[g, :, :per_group]) for g in range(GROUPS)], axis=1
    )
    values = jnp.concatenate(
        [mm(latent[:, g * LATENT : (g + 1) * LATENT], w_kv[g, :, per_group:]) for g in range(GROUPS)], axis=1
    )
    gain_row = out_gain.reshape(1, WIDTH)
    mixed, heads, states = mixer_fwd(query, keys, values, decay_in, gate_in, gain_row, cols, segs)
    middle = inputs + mm(mixed, w_output)
    factor_mid = rms_factor(middle, 1e-5)
    normed_mid = (middle * factor_mid * gain_mid).astype(BF)
    gate_val = mm(normed_mid, w_ff[:, :FF])
    up_val = mm(normed_mid, w_ff[:, FF:])
    sig = jax.nn.sigmoid(gate_val)
    silu = gate_val * sig
    hidden = (silu * up_val).astype(BF)
    block_out = (middle + mm(hidden, w_dn)).astype(BF)

    d_outf = cotangent.astype(F32) * pad
    d_ffn = d_outf.astype(BF)
    grad_down = mm_tn(hidden, d_ffn)
    d_hidden = mm_nt(d_ffn, w_dn)
    d_gate = (d_hidden * up_val * (sig * (1.0 + gate_val * (1.0 - sig)))).astype(BF)
    d_up = (d_hidden * silu).astype(BF)
    d_both = jnp.concatenate([d_gate, d_up], axis=1)
    grad_ff = mm_tn(normed_mid, d_both)
    d_normed_mid = mm_nt(d_both, w_ff)
    d_middle, d_gain_mid = rms_back(d_normed_mid, middle, factor_mid, gain_mid)
    d_middle = d_middle + d_outf
    d_branch = d_middle.astype(BF)
    grad_out = mm_tn(mixed, d_branch)
    d_mixed = mm_nt(d_branch, w_output)

    d_query, d_keys, d_values, d_decay, d_gatein, d_bias, d_out_gain = mixer_bwd(
        query, keys, values, decay_in, gate_in, gain_row, cols, segs, heads, states, d_mixed
    )
    grad_kv, d_latent = [], []
    for g in range(GROUPS):
        d_kv = jnp.concatenate(
            [part[:, g * per_group : (g + 1) * per_group] for part in (d_keys, d_values)], axis=1
        )
        grad_kv.append(mm_tn(latent[:, g * LATENT : (g + 1) * LATENT], d_kv))
        d_latent.append(mm_nt(d_kv, w_kv[g]))
    grad_kv = jnp.concatenate(grad_kv, axis=0)
    d_latent = jnp.concatenate(d_latent, axis=1).astype(BF)
    d_in = jnp.concatenate([d_query, d_decay, d_gatein, d_latent], axis=1)
    grad_in = mm_tn(normed, d_in)
    d_normed = mm_nt(d_in, w_in)
    d_inputs, d_gain_in = rms_back(d_normed, inputs, factor_in, gain_in)
    grad_input = d_middle + d_inputs
    grad_vec = jnp.concatenate([d_gain_in, d_gain_mid, d_bias.reshape(-1), d_out_gain.reshape(-1)])

    own_in, own_kv, own_out, own_ff, own_down, own_vec = scatter(
        (
            grad_in.reshape(count, rows_d, -1),
            grad_kv.reshape(count, rows_kv, -1),
            grad_out.reshape(count, rows_d, -1),
            grad_ff.reshape(count, rows_d, -1),
            grad_down.reshape(count, rows_ff, -1),
            grad_vec.reshape(count, 1, -1),
        )
    )
    return (
        block_out,
        grad_input,
        own_in[:, :WIDTH].reshape(-1),
        own_in[:, 3 * WIDTH :].reshape(-1),
        own_kv[:, :per_group].reshape(-1),
        own_kv[:, per_group:].reshape(-1),
        own_in[:, WIDTH : 2 * WIDTH].reshape(-1),
        own_in[:, 2 * WIDTH : 3 * WIDTH].reshape(-1),
        own_out.reshape(-1),
        own_ff[:, :FF].reshape(-1),
        own_ff[:, FF:].reshape(-1),
        own_down.reshape(-1),
        own_vec.reshape(-1),
    )


def solution(mesh):
    count = mesh.shape["dp"] * mesh.shape["fsdp"]
    rows, flat = P(AXES, None), P(AXES)
    in_specs = (rows,) + (flat,) * 13 + (rows,)
    out_specs = (rows, rows) + (flat,) * 11
    return jax.shard_map(
        partial(per_device, count=count), mesh=mesh, in_specs=in_specs, out_specs=out_specs, check_vma=False
    )
```

```python
from functools import partial

import jax
import jax.numpy as jnp
from jax import lax
from jax.experimental import pallas as pl
from jax.experimental.pallas import tpu as pltpu
from jax.sharding import PartitionSpec as P

D = 1024
HEADS = 16
HEAD_DIM = 64
GROUPS = 2
LATENT = 256
FF = 2816
LEN = 1024
WIDTH = HEADS * HEAD_DIM
SPAN = 128
LANES = 256
PACK = LANES // HEAD_DIM
BANDS = WIDTH // LANES
CHUNKS = LEN // SPAN
LIMIT = 85.0
AXES = ("dp", "fsdp")
BF = jnp.bfloat16
F32 = jnp.float32
MESH = pl.DeviceIdType.MESH


def mm(left, right):
    return lax.dot_general(left, right, (((1,), (0,)), ((), ())), preferred_element_type=F32)


def mm_nt(left, right):
    return lax.dot_general(left, right, (((1,), (1,)), ((), ())), preferred_element_type=F32)


def mm_tn(left, right):
    return lax.dot_general(left, right, (((0,), (0,)), ((), ())), preferred_element_type=F32)


def halves(value):
    high = value.astype(BF)
    return high, (value - high.astype(F32)).astype(BF)


def exact_left(ones, value):
    high, rest = halves(value)
    return mm(ones, high) + mm(ones, rest)


def exact_right(value, ones):
    high, rest = halves(value)
    return mm(high, ones) + mm(rest, ones)


def head_masks():
    lane = lax.broadcasted_iota(jnp.int32, (1, LANES), 1) // HEAD_DIM
    return [lane == head for head in range(PACK)]


def stacked(value, masks):
    zero = jnp.zeros_like(value)
    return jnp.concatenate([jnp.where(mask, value, zero) for mask in masks], axis=0)


def side_by_side(value):
    return jnp.concatenate([value[h * SPAN : (h + 1) * SPAN] for h in range(PACK)], axis=1)


def same_head():
    row = lax.broadcasted_iota(jnp.int32, (LANES, LANES), 0) // HEAD_DIM
    col = lax.broadcasted_iota(jnp.int32, (LANES, LANES), 1) // HEAD_DIM
    return row == col


def triangle(lower):
    row = lax.broadcasted_iota(jnp.int32, (SPAN, SPAN), 0)
    col = lax.broadcasted_iota(jnp.int32, (SPAN, SPAN), 1)
    return (row >= col) if lower else (row <= col)


def decays(decay, pad, lower_ones):
    small = jnp.exp(-jnp.abs(decay))
    log_sig = jnp.minimum(decay, 0.0) - jnp.log(1.0 + small)
    total = exact_left(lower_ones, log_sig * (pad * (1.0 / 16.0)))
    ending = total[SPAN - 1 : SPAN]
    middle = 0.5 * ending
    centred = total - middle
    up = jnp.exp(jnp.minimum(centred, LIMIT))
    down = jnp.exp(jnp.minimum(-centred, LIMIT))
    half = jnp.exp(middle)
    return up, down, half, small


def flags(cols_ref, seg_ref, rows, index):
    cols = cols_ref[rows, :]
    seg_col, fresh, to_end, pad = cols[:, 0:1], cols[:, 1:2], cols[:, 2:3], cols[:, 3:4]
    allowed = (seg_col == seg_ref[index]) & triangle(True)
    return fresh, to_end, pad, allowed, fresh[SPAN - 1 : SPAN]


def mixer_fwd_kernel(
    q_ref, k_ref, v_ref, decay_ref, gate_ref, gain_ref, cols_ref, seg_ref, mixed_ref, heads_ref, states_ref, state
):
    masks = head_masks()
    diag = same_head()
    diag_ones = diag.astype(F32).astype(BF)
    lower_ones = triangle(True).astype(F32).astype(BF)
    state[...] = jnp.zeros_like(state)
    gain = gain_ref[...]

    def chunk(index, carry):
        rows = pl.ds(pl.multiple_of(index * SPAN, SPAN), SPAN)
        fresh, to_end, pad, allowed, keep = flags(cols_ref, seg_ref, rows, index)
        up, down, half, _ = decays(decay_ref[rows, :], pad, lower_ones)
        query = q_ref[rows, :] * (HEAD_DIM**-0.5) * up
        key = k_ref[rows, :] * pad * down
        value = v_ref[rows, :].astype(BF)
        query_low, key_low = query.astype(BF), key.astype(BF)
        scores = mm_nt(stacked(query_low, masks), key_low)
        scores = scores.reshape(PACK, SPAN, SPAN)
        scores = jnp.where(allowed[None], scores, 0.0).astype(BF).reshape(PACK * SPAN, SPAN)
        old = state[...]
        old_low = old.astype(BF)
        states_ref[0, index] = old_low
        heads = mm(side_by_side(scores), stacked(value, masks))
        heads += mm_nt((query * (half * fresh)).astype(BF), old_low)
        tail = (key * (half * to_end)).astype(BF)
        state[...] = old * (half * half * keep) + jnp.where(diag, mm_tn(value, tail), 0.0)
        heads_ref[rows, :] = heads
        scale = lax.rsqrt(exact_right(heads * heads, diag_ones) * (1.0 / HEAD_DIM) + 1e-2)
        gate = gate_ref[rows, :]
        silu = gate / (1.0 + jnp.exp(-gate))
        mixed_ref[rows, :] = (heads * scale * gain * silu).astype(BF)
        return carry

    lax.fori_loop(0, CHUNKS, chunk, 0)


def mixer_bwd_kernel(
    q_ref,
    k_ref,
    v_ref,
    decay_ref,
    gate_ref,
    gain_ref,
    cols_ref,
    seg_ref,
    heads_ref,
    states_ref,
    dmix_ref,
    dq_ref,
    dk_ref,
    dv_ref,
    ddecay_ref,
    dgate_ref,
    dbias_ref,
    dgain_ref,
    state,
):
    masks = head_masks()
    diag = same_head()
    diag_ones = diag.astype(F32).astype(BF)
    lower_ones = triangle(True).astype(F32).astype(BF)
    upper_ones = triangle(False).astype(F32).astype(BF)
    state[...] = jnp.zeros_like(state)
    dbias_ref[...] = jnp.zeros_like(dbias_ref)
    dgain_ref[...] = jnp.zeros_like(dgain_ref)
    gain = gain_ref[...]

    def chunk(step, carry):
        index = CHUNKS - 1 - step
        rows = pl.ds(pl.multiple_of(index * SPAN, SPAN), SPAN)
        fresh, to_end, pad, allowed, keep = flags(cols_ref, seg_ref, rows, index)
        heads = heads_ref[rows, :]
        scale = lax.rsqrt(exact_right(heads * heads, diag_ones) * (1.0 / HEAD_DIM) + 1e-2)
        normed = heads * scale
        gate = gate_ref[rows, :]
        sig = 1.0 / (1.0 + jnp.exp(-gate))
        silu = gate * sig
        dmix = dmix_ref[rows, :]
        both = dmix * normed
        dgain_ref[...] += jnp.sum(both * silu, axis=0, keepdims=True)
        dgate_ref[rows, :] = (both * gain * (sig * (1.0 + gate * (1.0 - sig)))).astype(BF)
        dnormed = dmix * gain * silu
        mean = exact_right(dnormed * normed, diag_ones) * (1.0 / HEAD_DIM)
        dheads = (scale * (dnormed - normed * mean)).astype(BF)
        decay = decay_ref[rows, :]
        up, down, half, small = decays(decay, pad, lower_ones)
        unit = HEAD_DIM**-0.5
        query = q_ref[rows, :] * unit * up
        key = k_ref[rows, :] * pad * down
        value = v_ref[rows, :].astype(BF)
        query_low, key_low = query.astype(BF), key.astype(BF)
        enter = half * fresh
        leave = half * to_end
        query_in = (query * enter).astype(BF)
        tail = (key * leave).astype(BF)
        query_stack = stacked(query_low, masks)
        dheads_stack = stacked(dheads, masks)
        scores = mm_nt(query_stack, key_low).reshape(PACK, SPAN, SPAN)
        scores = jnp.where(allowed[None], scores, 0.0).astype(BF).reshape(PACK * SPAN, SPAN)
        dscores = mm_nt(dheads_stack, value).reshape(PACK, SPAN, SPAN)
        dscores = jnp.where(allowed[None], dscores, 0.0).astype(BF).reshape(PACK * SPAN, SPAN)
        dstate = state[...]
        dstate_low = dstate.astype(BF)
        old = states_ref[0, index]
        dvalue = mm_tn(scores, dheads_stack) + mm_nt(tail, dstate_low)
        dv_ref[rows, :] = dvalue.astype(BF)
        dquery = mm(side_by_side(dscores), stacked(key_low, masks))
        dkey = mm_tn(dscores, query_stack)
        dquery_in = mm(dheads, old)
        dtail = mm(value, dstate_low)
        whole = half * half * keep
        state[...] = dstate * whole + jnp.where(diag, mm_tn(dheads, query_in), 0.0)
        dq_ref[rows, :] = ((dquery + dquery_in * enter) * (up * unit)).astype(BF)
        dk_ref[rows, :] = ((dkey + dtail * leave) * (down * pad)).astype(BF)
        from_tail = dtail * tail.astype(F32)
        dtotal = (
            dquery * query_low.astype(F32)
            - dkey * key_low.astype(F32)
            + dquery_in * query_in.astype(F32)
            - from_tail
        )
        ends = jnp.sum(from_tail, axis=0, keepdims=True)
        ends += whole * jnp.sum(dstate * old.astype(F32), axis=0, keepdims=True)
        dlog = exact_left(upper_ones, dtotal) + ends
        other = jnp.where(decay >= 0, small, 1.0) / (1.0 + small)
        ddecay = dlog * (pad * (1.0 / 16.0)) * other
        dbias_ref[...] += jnp.sum(ddecay, axis=0, keepdims=True)
        ddecay_ref[rows, :] = ddecay.astype(BF)
        return carry

    lax.fori_loop(0, CHUNKS, chunk, 0)


def band_specs():
    tokens = pl.BlockSpec((LEN, LANES), lambda band: (0, band))
    vector = pl.BlockSpec((1, LANES), lambda band: (0, band))
    cols = pl.BlockSpec((LEN, 128), lambda band: (0, 0))
    segs = pl.BlockSpec((CHUNKS, 1, SPAN), lambda band: (0, 0, 0))
    states = pl.BlockSpec((1, CHUNKS, LANES, LANES), lambda band: (band, 0, 0, 0))
    return tokens, vector, cols, segs, states


def mixer_fwd(query, keys, values, decay_in, gate_in, out_gain, cols, segs):
    tokens, vector, cols_spec, segs_spec, states = band_specs()
    return pl.pallas_call(
        mixer_fwd_kernel,
        grid=(BANDS,),
        in_specs=[tokens] * 5 + [vector, cols_spec, segs_spec],
        out_specs=[tokens, tokens, states],
        out_shape=[
            jax.ShapeDtypeStruct((LEN, WIDTH), BF),
            jax.ShapeDtypeStruct((LEN, WIDTH), F32),
            jax.ShapeDtypeStruct((BANDS, CHUNKS, LANES, LANES), BF),
        ],
        scratch_shapes=[pltpu.VMEM((LANES, LANES), F32)],
        compiler_params=pltpu.CompilerParams(vmem_limit_bytes=48 << 20),
        name="mixer_fwd",
    )(query, keys, values, decay_in, gate_in, out_gain, cols, segs)


def mixer_bwd(query, keys, values, decay_in, gate_in, out_gain, cols, segs, heads, states_in, dmix):
    tokens, vector, cols_spec, segs_spec, states = band_specs()
    low = jax.ShapeDtypeStruct((LEN, WIDTH), BF)
    sums = jax.ShapeDtypeStruct((1, WIDTH), F32)
    return pl.pallas_call(
        mixer_bwd_kernel,
        grid=(BANDS,),
        in_specs=[tokens] * 5 + [vector, cols_spec, segs_spec, tokens, states, tokens],
        out_specs=[tokens] * 5 + [vector, vector],
        out_shape=[low] * 5 + [sums, sums],
        scratch_shapes=[pltpu.VMEM((LANES, LANES), F32)],
        compiler_params=pltpu.CompilerParams(vmem_limit_bytes=56 << 20),
        name="mixer_bwd",
    )(query, keys, values, decay_in, gate_in, out_gain, cols, segs, heads, states_in, dmix)


class Place:
    def __init__(self, ring_size, line_size):
        self.ring_size, self.line_size = ring_size, line_size
        self.d, f = lax.axis_index("dp"), lax.axis_index("fsdp")
        self.z, self.core = f // 2, f % 2
        self.pos = self.at_ring(self.d)

    def at_ring(self, index):
        if self.ring_size != 4:
            return index
        return index + (index // 2) * (1 - 2 * (index % 2))

    def ring(self, offset):
        return self.at_ring((self.pos + offset + self.ring_size) % self.ring_size)

    def far(self, i):
        n = self.line_size
        low = self.z < n // 2
        near = jnp.where(low, self.z, n - 1 - self.z)
        if i == n - 1:
            return self.z
        line = n - 1 - i - jnp.where(n - 1 - i <= near, 1, 0)
        return jnp.where(low, line, n - 1 - line)

    def device(self, d, z, core):
        return (d, 2 * z + core)

    def slot(self, d, z, core):
        return d * (2 * self.line_size) + 2 * z + core


def greet(place, peers):
    barrier = pltpu.get_barrier_semaphore()
    for peer in peers:
        pl.semaphore_signal(barrier, inc=1, device_id=peer, device_id_type=MESH)
    pl.semaphore_wait(barrier, len(peers))


def peers_of(place):
    me = place
    peers = [me.device(me.d, me.z, 1 - me.core)]
    peers += [me.device(me.ring(step), me.z, me.core) for step in (1, -1)]
    peers += [me.device(me.d, me.far(i), me.core) for i in range(me.line_size - 1)]
    return peers


def send(src, dst, send_sem, recv_sem, device):
    return pltpu.make_async_remote_copy(
        src_ref=src, dst_ref=dst, send_sem=send_sem, recv_sem=recv_sem, device_id=device, device_id_type=MESH
    )


def scatter_kernel(ring_size, line_size, ways, *refs):
    kinds = len(ways)
    grads, outs = refs[:kinds], refs[kinds : 2 * kinds]
    accs, parts, hops, tails = (refs[(2 + k) * kinds : (3 + k) * kinds] for k in range(4))
    load_sem, psend, precv, hsend, hrecv, tsend, trecv = refs[6 * kinds :]
    me = Place(ring_size, line_size)
    last = line_size - 1
    order = [me.far(i) for i in range(line_size)]
    waves = [
        (step, wave - step)
        for wave in range(1, ring_size + line_size)
        for step in range(1, ring_size + 1)
        if 0 <= wave - step < line_size
    ]

    def dest(a, step):
        return me.ring(-step * ways[a])

    def load(a, step, i):
        src = grads[a].at[me.slot(dest(a, step), order[i], me.core)]
        return pltpu.make_async_copy(src, accs[a].at[step - 1, i], load_sem.at[a, step - 1, i])

    def to_pair(a, step, i):
        src = grads[a].at[me.slot(dest(a, step), order[i], 1 - me.core)]
        return send(
            src,
            parts[a].at[step - 1, i],
            psend.at[a, step - 1, i],
            precv.at[a, step - 1, i],
            me.device(me.d, me.z, 1 - me.core),
        )

    def to_ring(a, step, i):
        return send(
            accs[a].at[step - 1, i],
            hops[a].at[step - 1, i],
            hsend.at[a, step - 1, i],
            hrecv.at[a, step - 1, i],
            me.device(me.ring(ways[a]), me.z, me.core),
        )

    def to_line(a, i):
        return send(
            accs[a].at[ring_size - 1, i],
            tails[a].at[me.z],
            tsend.at[a, i],
            trecv.at[a, me.z],
            me.device(me.d, order[i], me.core),
        )

    def from_line(a, i):
        here = tails[a].at[order[i]]
        return send(here, here, tsend.at[a, i], trecv.at[a, order[i]], me.device(me.d, order[i], me.core))

    for step, i in waves:
        for a in range(kinds):
            load(a, step, i).start()
    greet(me, peers_of(me))
    for step, i in waves:
        for a in range(kinds):
            to_pair(a, step, i).start()

    def blocks(a):
        width = grads[a].shape[-1]
        block = 512 if width % 512 == 0 else width
        return width // block, block

    def add_up(a, step, i):
        number, block = blocks(a)

        def body(j, carry):
            cols = pl.ds(pl.multiple_of(j * block, block), block)
            total = accs[a][step - 1, i, :, cols].astype(F32) + parts[a][step - 1, i, :, cols].astype(F32)
            if step > 1:
                total += hops[a][step - 2, i, :, cols].astype(F32)
            if step == ring_size and i == last:
                outs[a][:, cols] = total
            else:
                accs[a][step - 1, i, :, cols] = total.astype(accs[a].dtype)
            return carry

        lax.fori_loop(0, number, body, 0)

    for step, i in waves:
        for a in range(kinds):
            load(a, step, i).wait()
            to_pair(a, step, i).wait_recv()
            if step > 1:
                to_ring(a, step - 1, i).wait_recv()
            add_up(a, step, i)
            if step < ring_size:
                to_ring(a, step, i).start()
            elif i < last:
                to_line(a, i).start()

    def finish(a):
        number, block = blocks(a)

        def body(j, carry):
            cols = pl.ds(pl.multiple_of(j * block, block), block)
            total = outs[a][:, cols]
            for i in range(last):
                total += tails[a][order[i], :, cols].astype(F32)
            outs[a][:, cols] = total
            return carry

        lax.fori_loop(0, number, body, 0)

    for a in range(kinds):
        for i in range(last):
            from_line(a, i).wait_recv()
        finish(a)
    for step, i in waves:
        for a in range(kinds):
            to_pair(a, step, i).wait_send()
            if step < ring_size:
                to_ring(a, step, i).wait_send()
            elif i < last:
                to_line(a, i).wait_send()


def scatter(grads, ways, ring_size, line_size, ident):
    kinds = len(grads)
    shapes = [grad.shape[1:] for grad in grads]
    types = [grad.dtype for grad in grads]

    def room(*lead):
        return [pltpu.VMEM(lead + shape, dtype) for shape, dtype in zip(shapes, types)]

    sems = pltpu.SemaphoreType.DMA
    return pl.pallas_call(
        partial(scatter_kernel, ring_size, line_size, ways),
        in_specs=[pl.BlockSpec(memory_space=pl.ANY)] * kinds,
        out_specs=[pl.BlockSpec(memory_space=pltpu.VMEM)] * kinds,
        out_shape=[jax.ShapeDtypeStruct(shape, F32) for shape in shapes],
        scratch_shapes=room(ring_size, line_size)
        + room(ring_size, line_size)
        + room(ring_size - 1, line_size)
        + room(line_size)
        + [sems((kinds, ring_size, line_size))] * 5
        + [sems((kinds, line_size))] * 2,
        compiler_params=pltpu.CompilerParams(
            collective_id=ident, has_side_effects=True, vmem_limit_bytes=60 << 20
        ),
        name="scatter_sums",
    )(*grads)


def gather_kernel(ring_size, line_size, *refs):
    sem_refs = refs[-11:]
    kinds = (len(refs) - 11) // 2
    shards, outs = refs[:kinds], refs[kinds : 2 * kinds]
    own_sem, zsend, zrecv, hsend, hrecv, osend, orecv, psend, precv, qsend, qrecv = sem_refs
    me = Place(ring_size, line_size)
    order = [me.far(line_size - 1 - i) for i in range(line_size)]
    pair = me.device(me.d, me.z, 1 - me.core)
    ways = (1, -1)
    mine = me.slot(me.d, me.z, me.core)

    def half(a, way):
        width = shards[a].shape[-1]
        if width % 256:
            return pl.ds(0, width)
        return pl.ds(0 if way == 0 else width // 2, width // 2)

    def halved(a, way):
        return shards[a].shape[-1] % 256 == 0 or way == 0

    def own(a):
        return pltpu.make_async_copy(shards[a], outs[a].at[mine], own_sem.at[a])

    def to_line(a, i):
        return send(
            shards[a], outs[a].at[mine], zsend.at[a, i], zrecv.at[a, me.z], me.device(me.d, order[i], me.core)
        )

    def from_line(a, i):
        here = outs[a].at[me.slot(me.d, order[i], me.core)]
        return send(here, here, zsend.at[a, i], zrecv.at[a, order[i]], me.device(me.d, order[i], me.core))

    def to_ring(a, i, way):
        here = outs[a].at[me.slot(me.d, order[i], me.core)]
        src = shards[a] if i == 0 else here
        return send(
            src, here, hsend.at[a, way, i], hrecv.at[a, way, i], me.device(me.ring(ways[way]), me.z, me.core)
        )

    def came(a, i, way):
        return outs[a].at[me.slot(me.ring(-ways[way]), order[i], me.core)]

    def from_ring(a, i, way):
        here = came(a, i, way)
        return send(
            here, here, hsend.at[a, way, i], hrecv.at[a, way, i], me.device(me.ring(-ways[way]), me.z, me.core)
        )

    def onward(a, i, way):
        here = came(a, i, way).at[:, half(a, way)]
        return send(
            here, here, osend.at[a, way, i], orecv.at[a, way, i], me.device(me.ring(ways[way]), me.z, me.core)
        )

    def from_onward(a, i, way):
        here = outs[a].at[me.slot(me.ring(2), order[i], me.core), :, half(a, way)]
        return send(
            here, here, osend.at[a, way, i], orecv.at[a, way, i], me.device(me.ring(-ways[way]), me.z, me.core)
        )

    def to_pair(a, i, lane, core):
        offset = (0, -ways[0], -ways[1])[lane]
        here = outs[a].at[me.slot(me.ring(offset), order[i], core)]
        src = shards[a] if (lane == 0 and i == 0 and core is me.core) else here
        return send(src, here, psend.at[a, lane, i], precv.at[a, lane, i], pair)

    def to_pair_half(a, i, way, core):
        here = outs[a].at[me.slot(me.ring(2), order[i], core), :, half(a, way)]
        return send(here, here, qsend.at[a, way, i], qrecv.at[a, way, i], pair)

    every = range(kinds)
    for a in every:
        own(a).start()
    greet(me, peers_of(me))
    for a in every:
        for way in range(2):
            to_ring(a, 0, way).start()
        for i in range(1, line_size):
            to_line(a, i).start()
    for a in every:
        to_pair(a, 0, 0, me.core).start()

    def line_stage(i):
        for a in every:
            from_line(a, i).wait_recv()
            for way in range(2):
                to_ring(a, i, way).start()
            to_pair(a, i, 0, me.core).start()

    def ring_stage(i):
        for way in range(2):
            for a in every:
                from_ring(a, i, way).wait_recv()
                if halved(a, way):
                    onward(a, i, way).start()
                to_pair(a, i, 1 + way, me.core).start()

    def far_stage(i):
        for way in range(2):
            for a in every:
                if halved(a, way):
                    from_onward(a, i, way).wait_recv()
                    to_pair_half(a, i, way, me.core).start()

    for wave in range(line_size + 2):
        if 1 <= wave < line_size:
            line_stage(wave)
        if 1 <= wave <= line_size:
            ring_stage(wave - 1)
        if 2 <= wave:
            far_stage(wave - 2)
    for a in every:
        own(a).wait()
        for i in range(line_size):
            for lane in range(3):
                to_pair(a, i, lane, 1 - me.core).wait_recv()
                to_pair(a, i, lane, me.core).wait_send()
            for way in range(2):
                to_ring(a, i, way).wait_send()
                if halved(a, way):
                    to_pair_half(a, i, way, 1 - me.core).wait_recv()
                    to_pair_half(a, i, way, me.core).wait_send()
                    onward(a, i, way).wait_send()
            if i:
                to_line(a, i).wait_send()


def gather(shards, ring_size, line_size, ident):
    kinds = len(shards)
    count = 2 * ring_size * line_size
    sems = pltpu.SemaphoreType.DMA
    return pl.pallas_call(
        partial(gather_kernel, ring_size, line_size),
        in_specs=[pl.BlockSpec(memory_space=pltpu.VMEM)] * kinds,
        out_specs=[pl.BlockSpec(memory_space=pl.ANY)] * kinds,
        out_shape=[jax.ShapeDtypeStruct((count,) + piece.shape, piece.dtype) for piece in shards],
        scratch_shapes=[sems((kinds,))]
        + [sems((kinds, line_size))] * 2
        + [sems((kinds, 2, line_size))] * 4
        + [sems((kinds, 3, line_size))] * 2
        + [sems((kinds, 2, line_size))] * 2,
        compiler_params=pltpu.CompilerParams(collective_id=ident, has_side_effects=True),
        name="gather_shards",
    )(*shards)


def rms_factor(values, eps):
    return lax.rsqrt(jnp.mean(values * values, axis=-1, keepdims=True) + eps)


def rms_back(grad, values, factor, gain):
    scaled = values * factor
    dscaled = grad * gain
    dvalues = factor * (dscaled - scaled * jnp.mean(dscaled * scaled, axis=-1, keepdims=True))
    return dvalues, jnp.sum(grad * scaled, axis=0)


def by_kernel(sizes, ring_size, fsdp_size):
    return ring_size == 4 and fsdp_size % 2 == 0 and all(size % 8 == 0 for size in sizes)


def gather_all(shards, sizes, ring_size, fsdp_size):
    if by_kernel(sizes, ring_size, fsdp_size):
        return gather(shards, ring_size, fsdp_size // 2, 0)
    return [lax.all_gather(piece, AXES, axis=0) for piece in shards]


def scatter_all(grads, ways, sizes, ring_size, fsdp_size):
    if by_kernel(sizes, ring_size, fsdp_size):
        return scatter(grads, ways, ring_size, fsdp_size // 2, 1)
    return [lax.psum_scatter(piece.astype(F32), AXES, scatter_dimension=0) for piece in grads]


def per_device(
    hidden_in,
    w_query,
    w_latent,
    w_key_up,
    w_value_up,
    w_decay,
    w_outgate,
    w_out,
    w_gate,
    w_up,
    w_down,
    vectors,
    seg_ids,
    pad_mask,
    cotangent,
    *,
    ring_size,
    fsdp_size,
):
    count = ring_size * fsdp_size
    per_group = WIDTH // GROUPS
    latents = GROUPS * LATENT
    rows_d, rows_kv, rows_ff = D // count, latents // count, FF // count
    rows_all = (rows_d, rows_kv, rows_ff)
    vec_size = (2 * D + 2 * WIDTH) // count

    def rows_of(piece, rows):
        return piece.astype(BF).reshape(rows, -1)

    in_shard = jnp.concatenate(
        [rows_of(piece, rows_d) for piece in (w_query, w_decay, w_outgate, w_latent)], axis=1
    )
    kv_shard = jnp.concatenate([rows_of(w_key_up, rows_kv), rows_of(w_value_up, rows_kv)], axis=1)
    out_shard = rows_of(w_out, rows_d)
    ff_shard = jnp.concatenate([rows_of(w_gate, rows_d), rows_of(w_up, rows_d)], axis=1)
    down_shard = rows_of(w_down, rows_ff)
    vec_shard = jnp.broadcast_to(lax.reduce_precision(vectors, 8, 7).reshape(1, -1), (8, vec_size))
    w_in, w_kv, w_output, w_ff, w_dn, vecs = gather_all(
        (in_shard, kv_shard, out_shard, ff_shard, down_shard, vec_shard), rows_all, ring_size, fsdp_size
    )
    w_in = w_in.reshape(D, 3 * WIDTH + latents)
    w_kv = w_kv.reshape(GROUPS, LATENT, 2 * per_group)
    w_output = w_output.reshape(WIDTH, D)
    w_ff = w_ff.reshape(D, 2 * FF)
    w_dn = w_dn.reshape(FF, D)
    vecs = vecs[:, 0].reshape(-1)
    gain_in, gain_mid = vecs[:D], vecs[D : 2 * D]
    decay_bias, out_gain = vecs[2 * D : 2 * D + WIDTH], vecs[2 * D + WIDTH :]

    seg = seg_ids.reshape(CHUNKS, SPAN)
    before = jnp.concatenate([jnp.full((1,), -1, seg.dtype), seg[:-1, -1]])
    fresh = (seg == before[:, None]).astype(F32).reshape(LEN, 1)
    to_end = (seg == seg[:, -1:]).astype(F32).reshape(LEN, 1)
    pad = pad_mask.astype(F32).reshape(LEN, 1)
    seg_col = seg_ids.astype(F32).reshape(LEN, 1)
    cols = jnp.concatenate(
        [seg_col, fresh, to_end, pad, jnp.zeros((LEN, 124), F32)], axis=1
    )
    segs = seg_ids.astype(F32).reshape(CHUNKS, 1, SPAN)

    inputs = hidden_in.astype(F32)
    factor_in = rms_factor(inputs, 1e-5)
    normed = (inputs * factor_in * gain_in).astype(BF)
    query = mm(normed, w_in[:, :WIDTH])
    decay_in = mm(normed, w_in[:, WIDTH : 2 * WIDTH]) + decay_bias
    gate_in = mm(normed, w_in[:, 2 * WIDTH : 3 * WIDTH])
    latent = mm(normed, w_in[:, 3 * WIDTH :]).astype(BF)
    keys = jnp.concatenate(
        [mm(latent[:, g * LATENT : (g + 1) * LATENT], w_kv[g, :, :per_group]) for g in range(GROUPS)], axis=1
    )
    values = jnp.concatenate(
        [mm(latent[:, g * LATENT : (g + 1) * LATENT], w_kv[g, :, per_group:]) for g in range(GROUPS)], axis=1
    )
    gain_row = out_gain.reshape(1, WIDTH)
    mixed, heads, states = mixer_fwd(query, keys, values, decay_in, gate_in, gain_row, cols, segs)
    middle = inputs + mm(mixed, w_output)
    factor_mid = rms_factor(middle, 1e-5)
    normed_mid = (middle * factor_mid * gain_mid).astype(BF)
    gate_val = mm(normed_mid, w_ff[:, :FF])
    up_val = mm(normed_mid, w_ff[:, FF:])
    sig = jax.nn.sigmoid(gate_val)
    silu = gate_val * sig
    hidden = (silu * up_val).astype(BF)
    block_out = (middle + mm(hidden, w_dn)).astype(BF)

    d_outf = cotangent.astype(F32) * pad
    d_ffn = d_outf.astype(BF)
    grad_down = mm_tn(hidden, d_ffn)
    d_hidden = mm_nt(d_ffn, w_dn)
    d_gate = (d_hidden * up_val * (sig * (1.0 + gate_val * (1.0 - sig)))).astype(BF)
    d_up = (d_hidden * silu).astype(BF)
    d_both = jnp.concatenate([d_gate, d_up], axis=1)
    grad_ff = mm_tn(normed_mid, d_both)
    d_normed_mid = mm_nt(d_both, w_ff)
    d_middle, d_gain_mid = rms_back(d_normed_mid, middle, factor_mid, gain_mid)
    d_middle = d_middle + d_outf
    d_branch = d_middle.astype(BF)
    grad_out = mm_tn(mixed, d_branch)
    d_mixed = mm_nt(d_branch, w_output)

    d_query, d_keys, d_values, d_decay, d_gatein, d_bias, d_out_gain = mixer_bwd(
        query, keys, values, decay_in, gate_in, gain_row, cols, segs, heads, states, d_mixed
    )
    grad_kv, d_latent = [], []
    for g in range(GROUPS):
        d_kv = jnp.concatenate(
            [part[:, g * per_group : (g + 1) * per_group] for part in (d_keys, d_values)], axis=1
        )
        grad_kv.append(mm_tn(latent[:, g * LATENT : (g + 1) * LATENT], d_kv))
        d_latent.append(mm_nt(d_kv, w_kv[g]))
    grad_kv = jnp.concatenate(grad_kv, axis=0)
    d_latent = jnp.concatenate(d_latent, axis=1).astype(BF)
    d_in = jnp.concatenate([d_query, d_decay, d_gatein, d_latent], axis=1)
    grad_in = mm_tn(normed, d_in)
    d_normed = mm_nt(d_in, w_in)
    d_inputs, d_gain_in = rms_back(d_normed, inputs, factor_in, gain_in)
    grad_input = d_middle + d_inputs
    grad_vec = jnp.concatenate([d_gain_in, d_gain_mid, d_bias.reshape(-1), d_out_gain.reshape(-1)])

    grad_vec = jnp.broadcast_to(grad_vec.reshape(count, 1, vec_size), (count, 8, vec_size))
    own_in, own_kv, own_out, own_ff, own_down, own_vec = scatter_all(
        (
            grad_in.astype(BF).reshape(count, rows_d, -1),
            grad_kv.astype(BF).reshape(count, rows_kv, -1),
            grad_out.astype(BF).reshape(count, rows_d, -1),
            grad_ff.astype(BF).reshape(count, rows_d, -1),
            grad_down.astype(BF).reshape(count, rows_ff, -1),
            grad_vec,
        ),
        (-1, -1, 1, 1, -1, 1),
        rows_all,
        ring_size,
        fsdp_size,
    )
    return (
        block_out,
        grad_input,
        own_in[:, :WIDTH].reshape(-1),
        own_in[:, 3 * WIDTH :].reshape(-1),
        own_kv[:, :per_group].reshape(-1),
        own_kv[:, per_group:].reshape(-1),
        own_in[:, WIDTH : 2 * WIDTH].reshape(-1),
        own_in[:, 2 * WIDTH : 3 * WIDTH].reshape(-1),
        own_out.reshape(-1),
        own_ff[:, :FF].reshape(-1),
        own_ff[:, FF:].reshape(-1),
        own_down.reshape(-1),
        own_vec[0],
    )


def solution(mesh):
    sizes = {"ring_size": mesh.shape["dp"], "fsdp_size": mesh.shape["fsdp"]}
    rows, flat = P(AXES, None), P(AXES)
    in_specs = (rows,) + (flat,) * 13 + (rows,)
    out_specs = (rows, rows) + (flat,) * 11
    return jax.shard_map(
        partial(per_device, **sizes), mesh=mesh, in_specs=in_specs, out_specs=out_specs, check_vma=False
    )
```

```python
from functools import partial

import jax
import jax.numpy as jnp
from jax import lax
from jax.experimental import pallas as pl
from jax.experimental.pallas import tpu as pltpu
from jax.sharding import PartitionSpec as P

D = 1024
HEADS = 16
HEAD_DIM = 64
GROUPS = 2
LATENT = 256
FF = 2816
LEN = 1024
WIDTH = HEADS * HEAD_DIM
SPAN = 128
LANES = 256
PACK = LANES // HEAD_DIM
BANDS = WIDTH // LANES
CHUNKS = LEN // SPAN
LIMIT = 85.0
AXES = ("dp", "fsdp")
BF = jnp.bfloat16
F32 = jnp.float32
MESH = pl.DeviceIdType.MESH


def mm(left, right):
    return lax.dot_general(left, right, (((1,), (0,)), ((), ())), preferred_element_type=F32)


def mm_nt(left, right):
    return lax.dot_general(left, right, (((1,), (1,)), ((), ())), preferred_element_type=F32)


def mm_tn(left, right):
    return lax.dot_general(left, right, (((0,), (0,)), ((), ())), preferred_element_type=F32)


def halves(value):
    high = value.astype(BF)
    return high, (value - high.astype(F32)).astype(BF)


def exact_left(ones, value):
    high, rest = halves(value)
    return mm(ones, high) + mm(ones, rest)


def exact_right(value, ones):
    high, rest = halves(value)
    return mm(high, ones) + mm(rest, ones)


def head_masks():
    lane = lax.broadcasted_iota(jnp.int32, (1, LANES), 1) // HEAD_DIM
    return [lane == head for head in range(PACK)]


def stacked(value, masks):
    zero = jnp.zeros_like(value)
    return jnp.concatenate([jnp.where(mask, value, zero) for mask in masks], axis=0)


def side_by_side(value):
    return jnp.concatenate([value[h * SPAN : (h + 1) * SPAN] for h in range(PACK)], axis=1)


def same_head():
    row = lax.broadcasted_iota(jnp.int32, (LANES, LANES), 0) // HEAD_DIM
    col = lax.broadcasted_iota(jnp.int32, (LANES, LANES), 1) // HEAD_DIM
    return row == col


def triangle(lower):
    row = lax.broadcasted_iota(jnp.int32, (SPAN, SPAN), 0)
    col = lax.broadcasted_iota(jnp.int32, (SPAN, SPAN), 1)
    return (row >= col) if lower else (row <= col)


def decays(decay, pad, lower_ones):
    small = jnp.exp(-jnp.abs(decay))
    log_sig = jnp.minimum(decay, 0.0) - jnp.log(1.0 + small)
    total = exact_left(lower_ones, log_sig * (pad * (1.0 / 16.0)))
    ending = total[SPAN - 1 : SPAN]
    middle = 0.5 * ending
    centred = total - middle
    up = jnp.exp(jnp.minimum(centred, LIMIT))
    down = jnp.exp(jnp.minimum(-centred, LIMIT))
    half = jnp.exp(middle)
    return up, down, half, small


def flags(cols_ref, seg_ref, rows, index):
    cols = cols_ref[rows, :]
    seg_col, fresh, to_end, pad = cols[:, 0:1], cols[:, 1:2], cols[:, 2:3], cols[:, 3:4]
    allowed = (seg_col == seg_ref[index]) & triangle(True)
    return fresh, to_end, pad, allowed, fresh[SPAN - 1 : SPAN]


def mixer_fwd_kernel(comm, *refs):
    kinds = comm[2] if comm else 0
    normed_ref, latent_ref, wq_ref, wd_ref, wg_ref, wk_ref, wv_ref, bias_ref, gain_ref, cols_ref, seg_ref = refs[:11]
    shards, refs = refs[11 : 11 + kinds], refs[11 + kinds :]
    q_ref, k_ref, v_ref, decay_ref, gate_ref, mixed_ref, heads_ref, states_ref = refs[:8]
    gathered, state, sems = refs[8 : 8 + kinds], refs[8 + kinds], refs[9 + kinds :]
    band = pl.program_id(0)
    job = Gather(comm[0], comm[1], shards, gathered, sems) if comm else None
    stages = job.stages() if comm else []
    ticks = BANDS * (CHUNKS + 1)
    if comm:
        pl.when(band == 0)(job.begin)
    masks = head_masks()
    diag = same_head()
    diag_ones = diag.astype(F32).astype(BF)
    lower_ones = triangle(True).astype(F32).astype(BF)
    state[...] = jnp.zeros_like(state)
    gain = gain_ref[...]
    q_ref[...] = mm(normed_ref[...], wq_ref[...])
    decay_ref[...] = mm(normed_ref[...], wd_ref[...]) + bias_ref[...]
    gate_ref[...] = mm(normed_ref[...], wg_ref[...])
    k_ref[...] = mm(latent_ref[...], wk_ref[0])
    v_ref[...] = mm(latent_ref[...], wv_ref[0])

    def chunk(index, carry):
        spread(stages, band * (CHUNKS + 1) + index, ticks)
        rows = pl.ds(pl.multiple_of(index * SPAN, SPAN), SPAN)
        fresh, to_end, pad, allowed, keep = flags(cols_ref, seg_ref, rows, index)
        up, down, half, _ = decays(decay_ref[rows, :], pad, lower_ones)
        query = q_ref[rows, :] * (HEAD_DIM**-0.5) * up
        key = k_ref[rows, :] * pad * down
        value = v_ref[rows, :].astype(BF)
        query_low, key_low = query.astype(BF), key.astype(BF)
        scores = mm_nt(stacked(query_low, masks), key_low)
        scores = scores.reshape(PACK, SPAN, SPAN)
        scores = jnp.where(allowed[None], scores, 0.0).astype(BF).reshape(PACK * SPAN, SPAN)
        old = state[...]
        old_low = old.astype(BF)
        states_ref[0, index] = old_low
        heads = mm(side_by_side(scores), stacked(value, masks))
        heads += mm_nt((query * (half * fresh)).astype(BF), old_low)
        tail = (key * (half * to_end)).astype(BF)
        state[...] = old * (half * half * keep) + jnp.where(diag, mm_tn(value, tail), 0.0)
        heads_ref[rows, :] = heads
        scale = lax.rsqrt(exact_right(heads * heads, diag_ones) * (1.0 / HEAD_DIM) + 1e-2)
        gate = gate_ref[rows, :]
        silu = gate / (1.0 + jnp.exp(-gate))
        mixed_ref[rows, :] = (heads * scale * gain * silu).astype(BF)
        return carry

    lax.fori_loop(0, CHUNKS, chunk, 0)
    spread(stages, band * (CHUNKS + 1) + CHUNKS, ticks)
    if comm:
        pl.when(band == BANDS - 1)(job.finish)


def mixer_bwd_kernel(comm, *refs):
    kinds = comm[2] if comm else 0
    q_ref, k_ref, v_ref, decay_ref, gate_ref, gain_ref, cols_ref, seg_ref, heads_ref, states_ref = refs[:10]
    dbranch_ref, wo_ref = refs[10:12]
    grads, refs = refs[12 : 12 + kinds], refs[12 + kinds :]
    dq_ref, dk_ref, dv_ref, ddecay_ref, dgate_ref, dbias_ref, dgain_ref = refs[:7]
    sums, state, dmix_ref, scratch = refs[7 : 7 + kinds], refs[7 + kinds], refs[8 + kinds], refs[9 + kinds :]
    band = pl.program_id(0)
    job = scatter_of(comm[0], comm[1], grads, sums, scratch) if comm else None
    stages = job.stages() if comm else []
    ticks = BANDS * (CHUNKS + 1)
    if comm:
        pl.when(band == 0)(job.begin)
    dmix_ref[...] = mm_nt(dbranch_ref[...], wo_ref[...])
    masks = head_masks()
    diag = same_head()
    diag_ones = diag.astype(F32).astype(BF)
    lower_ones = triangle(True).astype(F32).astype(BF)
    upper_ones = triangle(False).astype(F32).astype(BF)
    state[...] = jnp.zeros_like(state)
    dbias_ref[...] = jnp.zeros_like(dbias_ref)
    dgain_ref[...] = jnp.zeros_like(dgain_ref)
    gain = gain_ref[...]

    def chunk(step, carry):
        spread(stages, band * (CHUNKS + 1) + step, ticks)
        index = CHUNKS - 1 - step
        rows = pl.ds(pl.multiple_of(index * SPAN, SPAN), SPAN)
        fresh, to_end, pad, allowed, keep = flags(cols_ref, seg_ref, rows, index)
        heads = heads_ref[rows, :]
        scale = lax.rsqrt(exact_right(heads * heads, diag_ones) * (1.0 / HEAD_DIM) + 1e-2)
        normed = heads * scale
        gate = gate_ref[rows, :]
        sig = 1.0 / (1.0 + jnp.exp(-gate))
        silu = gate * sig
        dmix = dmix_ref[rows, :]
        both = dmix * normed
        dgain_ref[...] += jnp.sum(both * silu, axis=0, keepdims=True)
        dgate_ref[rows, :] = (both * gain * (sig * (1.0 + gate * (1.0 - sig)))).astype(BF)
        dnormed = dmix * gain * silu
        mean = exact_right(dnormed * normed, diag_ones) * (1.0 / HEAD_DIM)
        dheads = (scale * (dnormed - normed * mean)).astype(BF)
        decay = decay_ref[rows, :]
        up, down, half, small = decays(decay, pad, lower_ones)
        unit = HEAD_DIM**-0.5
        query = q_ref[rows, :] * unit * up
        key = k_ref[rows, :] * pad * down
        value = v_ref[rows, :].astype(BF)
        query_low, key_low = query.astype(BF), key.astype(BF)
        enter = half * fresh
        leave = half * to_end
        query_in = (query * enter).astype(BF)
        tail = (key * leave).astype(BF)
        query_stack = stacked(query_low, masks)
        dheads_stack = stacked(dheads, masks)
        scores = mm_nt(query_stack, key_low).reshape(PACK, SPAN, SPAN)
        scores = jnp.where(allowed[None], scores, 0.0).astype(BF).reshape(PACK * SPAN, SPAN)
        dscores = mm_nt(dheads_stack, value).reshape(PACK, SPAN, SPAN)
        dscores = jnp.where(allowed[None], dscores, 0.0).astype(BF).reshape(PACK * SPAN, SPAN)
        dstate = state[...]
        dstate_low = dstate.astype(BF)
        old = states_ref[0, index]
        dvalue = mm_tn(scores, dheads_stack) + mm_nt(tail, dstate_low)
        dv_ref[rows, :] = dvalue.astype(BF)
        dquery = mm(side_by_side(dscores), stacked(key_low, masks))
        dkey = mm_tn(dscores, query_stack)
        dquery_in = mm(dheads, old)
        dtail = mm(value, dstate_low)
        whole = half * half * keep
        state[...] = dstate * whole + jnp.where(diag, mm_tn(dheads, query_in), 0.0)
        dq_ref[rows, :] = ((dquery + dquery_in * enter) * (up * unit)).astype(BF)
        dk_ref[rows, :] = ((dkey + dtail * leave) * (down * pad)).astype(BF)
        from_tail = dtail * tail.astype(F32)
        dtotal = (
            dquery * query_low.astype(F32)
            - dkey * key_low.astype(F32)
            + dquery_in * query_in.astype(F32)
            - from_tail
        )
        ends = jnp.sum(from_tail, axis=0, keepdims=True)
        ends += whole * jnp.sum(dstate * old.astype(F32), axis=0, keepdims=True)
        dlog = exact_left(upper_ones, dtotal) + ends
        other = jnp.where(decay >= 0, small, 1.0) / (1.0 + small)
        ddecay = dlog * (pad * (1.0 / 16.0)) * other
        dbias_ref[...] += jnp.sum(ddecay, axis=0, keepdims=True)
        ddecay_ref[rows, :] = ddecay.astype(BF)
        return carry

    lax.fori_loop(0, CHUNKS, chunk, 0)
    spread(stages, band * (CHUNKS + 1) + CHUNKS, ticks)
    if comm:
        pl.when(band == BANDS - 1)(job.finish)


def band_specs():
    tokens = pl.BlockSpec((LEN, LANES), lambda band: (0, band))
    vector = pl.BlockSpec((1, LANES), lambda band: (0, band))
    cols = pl.BlockSpec((LEN, 128), lambda band: (0, 0))
    segs = pl.BlockSpec((CHUNKS, 1, SPAN), lambda band: (0, 0, 0))
    states = pl.BlockSpec((1, CHUNKS, LANES, LANES), lambda band: (band, 0, 0, 0))
    return tokens, vector, cols, segs, states


def fixed(shape):
    return pl.BlockSpec(shape, lambda band: (0,) * len(shape), pipeline_mode=pl.Buffered(1))


def mixer_fwd(normed, latent, w_in, w_kv, bias, gain, cols, segs, shards, comm):
    tokens, vector, cols_spec, segs_spec, states = band_specs()
    kinds = len(shards)
    half_bands = BANDS // GROUPS
    in_specs = [fixed((LEN, D)), pl.BlockSpec((LEN, LATENT), lambda band: (0, band // half_bands))]
    for part in range(3):
        in_specs.append(pl.BlockSpec((D, LANES), lambda band, part=part: (0, part * BANDS + band)))
    for part in range(2):
        in_specs.append(
            pl.BlockSpec(
                (1, LATENT, LANES),
                lambda band, part=part: (band // half_bands, 0, part * half_bands + band % half_bands),
            )
        )
    in_specs += [vector, vector, cols_spec, segs_spec]
    wide = jax.ShapeDtypeStruct((LEN, WIDTH), F32)
    out_shape = [wide] * 5 + [
        jax.ShapeDtypeStruct((LEN, WIDTH), BF),
        wide,
        jax.ShapeDtypeStruct((BANDS, CHUNKS, LANES, LANES), BF),
    ]
    scratch = [pltpu.VMEM((LANES, LANES), F32)]
    params = {}
    if comm:
        count = 2 * comm[0] * comm[1]
        in_specs += [fixed(shard.shape) for shard in shards]
        out_shape += [jax.ShapeDtypeStruct((count,) + shard.shape, shard.dtype) for shard in shards]
        scratch += gather_scratch(kinds, comm[1])
        params = {"collective_id": comm[3], "has_side_effects": True}
        comm = comm[:2] + (kinds,)
    return pl.pallas_call(
        partial(mixer_fwd_kernel, comm),
        grid=(BANDS,),
        in_specs=in_specs,
        out_specs=[tokens] * 7 + [states] + [pl.BlockSpec(memory_space=pl.ANY)] * kinds,
        out_shape=out_shape,
        scratch_shapes=scratch,
        compiler_params=pltpu.CompilerParams(vmem_limit_bytes=52 << 20, **params),
        name="mixer_fwd",
    )(normed, latent, w_in, w_in, w_in, w_kv, w_kv, bias, gain, cols, segs, *shards)


def mixer_bwd(saved, d_branch, w_output, grads, comm):
    tokens, vector, cols_spec, segs_spec, states = band_specs()
    kinds = len(grads)
    low = jax.ShapeDtypeStruct((LEN, WIDTH), BF)
    sums = jax.ShapeDtypeStruct((1, WIDTH), F32)
    in_specs = [tokens] * 5 + [vector, cols_spec, segs_spec, tokens, states]
    in_specs += [fixed((LEN, D)), pl.BlockSpec((LANES, D), lambda band: (band, 0))]
    out_specs, out_shape = [tokens] * 5 + [vector, vector], [low] * 5 + [sums, sums]
    scratch = [pltpu.VMEM((LANES, LANES), F32), pltpu.VMEM((LEN, LANES), F32)]
    params = {}
    if comm:
        in_specs += [pl.BlockSpec(memory_space=pl.ANY)] * kinds
        out_specs += [fixed(grad.shape[1:]) for grad in grads]
        out_shape += [jax.ShapeDtypeStruct(grad.shape[1:], F32) for grad in grads]
        scratch += scatter_scratch(grads, comm[0], comm[1])
        params = {"collective_id": comm[3], "has_side_effects": True}
        comm = comm[:2] + (kinds,)
    return pl.pallas_call(
        partial(mixer_bwd_kernel, comm),
        grid=(BANDS,),
        in_specs=in_specs,
        out_specs=out_specs,
        out_shape=out_shape,
        scratch_shapes=scratch,
        compiler_params=pltpu.CompilerParams(vmem_limit_bytes=63 << 20, **params),
        name="mixer_bwd",
    )(*saved, d_branch, w_output, *grads)


class Place:
    def __init__(self, ring_size, line_size):
        self.ring_size, self.line_size = ring_size, line_size
        self.d, f = lax.axis_index("dp"), lax.axis_index("fsdp")
        self.z, self.core = f // 2, f % 2
        self.pos = self.at_ring(self.d)

    def at_ring(self, index):
        if self.ring_size != 4:
            return index
        return index + (index // 2) * (1 - 2 * (index % 2))

    def ring(self, offset):
        return self.at_ring((self.pos + offset + self.ring_size) % self.ring_size)

    def far(self, i):
        n = self.line_size
        low = self.z < n // 2
        near = jnp.where(low, self.z, n - 1 - self.z)
        if i == n - 1:
            return self.z
        line = n - 1 - i - jnp.where(n - 1 - i <= near, 1, 0)
        return jnp.where(low, line, n - 1 - line)

    def device(self, d, z, core):
        return (d, 2 * z + core)

    def slot(self, d, z, core):
        return d * (2 * self.line_size) + 2 * z + core


def greet(place, peers):
    barrier = pltpu.get_barrier_semaphore()
    for peer in peers:
        pl.semaphore_signal(barrier, inc=1, device_id=peer, device_id_type=MESH)
    pl.semaphore_wait(barrier, len(peers))


def peers_of(place):
    me = place
    peers = [me.device(me.d, me.z, 1 - me.core)]
    peers += [me.device(me.ring(step), me.z, me.core) for step in (1, -1)]
    peers += [me.device(me.d, me.far(i), me.core) for i in range(me.line_size - 1)]
    return peers


def send(src, dst, send_sem, recv_sem, device):
    return pltpu.make_async_remote_copy(
        src_ref=src, dst_ref=dst, send_sem=send_sem, recv_sem=recv_sem, device_id=device, device_id_type=MESH
    )


class Scatter:
    def __init__(self, ring_size, line_size, grads, outs, accs, parts, hops, tails, sems):
        self.ring_size, self.line_size = ring_size, line_size
        self.grads, self.outs = grads, outs
        self.accs, self.parts, self.hops, self.tails = accs, parts, hops, tails
        self.load_sem, self.psend, self.precv, self.hsend, self.hrecv, self.tsend, self.trecv = sems
        self.me = Place(ring_size, line_size)
        self.order = [self.me.far(i) for i in range(line_size)]
        self.every = range(len(grads))
        self.waves = [
            (step, wave - step)
            for wave in range(1, ring_size + line_size)
            for step in range(1, ring_size + 1)
            if 0 <= wave - step < line_size
        ]

    def way(self, a, i):
        return 1 if (a + i) % 2 == 0 else -1

    def dest(self, a, step, i, core):
        me = self.me
        return self.grads[a].at[me.slot(me.ring(-step * self.way(a, i)), self.order[i], core)]

    def load(self, a, step, i):
        return pltpu.make_async_copy(
            self.dest(a, step, i, self.me.core), self.accs[a].at[step - 1, i], self.load_sem.at[a, step - 1, i]
        )

    def to_pair(self, a, step, i):
        me = self.me
        return send(
            self.dest(a, step, i, 1 - me.core),
            self.parts[a].at[step - 1, i],
            self.psend.at[a, step - 1, i],
            self.precv.at[a, step - 1, i],
            me.device(me.d, me.z, 1 - me.core),
        )

    def to_ring(self, a, step, i):
        me = self.me
        return send(
            self.accs[a].at[step - 1, i],
            self.hops[a].at[step - 1, i],
            self.hsend.at[a, step - 1, i],
            self.hrecv.at[a, step - 1, i],
            me.device(me.ring(self.way(a, i)), me.z, me.core),
        )

    def to_line(self, a, i):
        me = self.me
        return send(
            self.accs[a].at[self.ring_size - 1, i],
            self.tails[a].at[me.z],
            self.tsend.at[a, i],
            self.trecv.at[a, me.z],
            me.device(me.d, self.order[i], me.core),
        )

    def from_line(self, a, i):
        me = self.me
        here = self.tails[a].at[self.order[i]]
        return send(
            here, here, self.tsend.at[a, i], self.trecv.at[a, self.order[i]], me.device(me.d, self.order[i], me.core)
        )

    def blocks(self, a):
        width = self.grads[a].shape[-1]
        block = 512 if width % 512 == 0 else width
        return width // block, block

    def add_up(self, a, step, i):
        number, block = self.blocks(a)
        acc, final = self.accs[a], step == self.ring_size and i == self.line_size - 1

        def body(j, carry):
            cols = pl.ds(pl.multiple_of(j * block, block), block)
            total = acc[step - 1, i, :, cols].astype(F32) + self.parts[a][step - 1, i, :, cols].astype(F32)
            if step > 1:
                total += self.hops[a][step - 2, i, :, cols].astype(F32)
            if final:
                self.outs[a][:, cols] = total
            else:
                acc[step - 1, i, :, cols] = total.astype(acc.dtype)
            return carry

        lax.fori_loop(0, number, body, 0)

    def begin(self):
        for step, i in self.waves:
            for a in self.every:
                self.load(a, step, i).start()
        greet(self.me, peers_of(self.me))
        for step, i in self.waves:
            for a in self.every:
                self.to_pair(a, step, i).start()

    def entry(self, step, i):
        for a in self.every:
            self.load(a, step, i).wait()
            self.to_pair(a, step, i).wait_recv()
            if step > 1:
                self.to_ring(a, step - 1, i).wait_recv()
            self.add_up(a, step, i)
            if step < self.ring_size:
                self.to_ring(a, step, i).start()
            elif i < self.line_size - 1:
                self.to_line(a, i).start()

    def stages(self):
        return [partial(self.entry, step, i) for step, i in self.waves]

    def finish(self):
        last = self.line_size - 1
        for a in self.every:
            for i in range(last):
                self.from_line(a, i).wait_recv()
            number, block = self.blocks(a)

            def body(j, carry, a=a, block=block):
                cols = pl.ds(pl.multiple_of(j * block, block), block)
                total = self.outs[a][:, cols]
                for i in range(last):
                    total += self.tails[a][self.order[i], :, cols].astype(F32)
                self.outs[a][:, cols] = total
                return carry

            lax.fori_loop(0, number, body, 0)
        for step, i in self.waves:
            for a in self.every:
                self.to_pair(a, step, i).wait_send()
                if step < self.ring_size:
                    self.to_ring(a, step, i).wait_send()
                elif i < last:
                    self.to_line(a, i).wait_send()


def scatter_scratch(grads, ring_size, line_size):
    kinds = len(grads)
    sems = pltpu.SemaphoreType.DMA
    scratch = []
    for lead in ((ring_size, line_size), (ring_size, line_size), (ring_size - 1, line_size), (line_size,)):
        scratch += [pltpu.VMEM(lead + grad.shape[1:], grad.dtype) for grad in grads]
    return scratch + [sems((kinds, ring_size, line_size))] * 5 + [sems((kinds, line_size))] * 2


def scatter_of(ring_size, line_size, grads, outs, scratch):
    kinds = len(grads)
    rooms = [scratch[k * kinds : (k + 1) * kinds] for k in range(4)]
    return Scatter(ring_size, line_size, grads, outs, *rooms, scratch[4 * kinds :])


def scatter_kernel(ring_size, line_size, kinds, *refs):
    job = scatter_of(ring_size, line_size, refs[:kinds], refs[kinds : 2 * kinds], refs[2 * kinds :])
    job.begin()
    for stage in job.stages():
        stage()
    job.finish()


def scatter(grads, ring_size, line_size, ident):
    kinds = len(grads)
    return pl.pallas_call(
        partial(scatter_kernel, ring_size, line_size, kinds),
        in_specs=[pl.BlockSpec(memory_space=pl.ANY)] * kinds,
        out_specs=[pl.BlockSpec(memory_space=pltpu.VMEM)] * kinds,
        out_shape=[jax.ShapeDtypeStruct(grad.shape[1:], F32) for grad in grads],
        scratch_shapes=scatter_scratch(grads, ring_size, line_size),
        compiler_params=pltpu.CompilerParams(
            collective_id=ident, has_side_effects=True, vmem_limit_bytes=60 << 20
        ),
        name="scatter_sums",
    )(*grads)


class Gather:
    def __init__(self, ring_size, line_size, shards, outs, sems):
        self.line_size = line_size
        self.shards, self.outs = shards, outs
        (
            self.own_sem,
            self.zsend,
            self.zrecv,
            self.hsend,
            self.hrecv,
            self.osend,
            self.orecv,
            self.psend,
            self.precv,
            self.qsend,
            self.qrecv,
        ) = sems
        self.me = Place(ring_size, line_size)
        self.order = [self.me.far(line_size - 1 - i) for i in range(line_size)]
        self.pair = self.me.device(self.me.d, self.me.z, 1 - self.me.core)
        self.mine = self.me.slot(self.me.d, self.me.z, self.me.core)
        self.every = range(len(shards))

    def half(self, a, way):
        width = self.shards[a].shape[-1]
        if width % 256:
            return pl.ds(0, width)
        return pl.ds(0 if way == 0 else width // 2, width // 2)

    def halved(self, a, way):
        return self.shards[a].shape[-1] % 256 == 0 or way == 0

    def beside(self, way):
        return self.me.device(self.me.ring(1 - 2 * way), self.me.z, self.me.core)

    def spot(self, a, offset, i, core):
        return self.outs[a].at[self.me.slot(self.me.ring(offset), self.order[i], core)]

    def own(self, a):
        return pltpu.make_async_copy(self.shards[a], self.outs[a].at[self.mine], self.own_sem.at[a])

    def to_line(self, a, i):
        me = self.me
        return send(
            self.shards[a],
            self.outs[a].at[self.mine],
            self.zsend.at[a, i],
            self.zrecv.at[a, me.z],
            me.device(me.d, self.order[i], me.core),
        )

    def from_line(self, a, i):
        me = self.me
        here = self.spot(a, 0, i, me.core)
        return send(
            here, here, self.zsend.at[a, i], self.zrecv.at[a, self.order[i]], me.device(me.d, self.order[i], me.core)
        )

    def to_ring(self, a, i, way):
        here = self.spot(a, 0, i, self.me.core)
        src = self.shards[a] if i == 0 else here
        return send(src, here, self.hsend.at[a, way, i], self.hrecv.at[a, way, i], self.beside(way))

    def from_ring(self, a, i, way):
        here = self.spot(a, 2 * way - 1, i, self.me.core)
        return send(here, here, self.hsend.at[a, way, i], self.hrecv.at[a, way, i], self.beside(1 - way))

    def onward(self, a, i, way):
        here = self.spot(a, 2 * way - 1, i, self.me.core).at[:, self.half(a, way)]
        return send(here, here, self.osend.at[a, way, i], self.orecv.at[a, way, i], self.beside(way))

    def from_onward(self, a, i, way):
        here = self.spot(a, 2, i, self.me.core).at[:, self.half(a, way)]
        return send(here, here, self.osend.at[a, way, i], self.orecv.at[a, way, i], self.beside(1 - way))

    def to_pair(self, a, i, lane, core):
        here = self.spot(a, (0, -1, 1)[lane], i, core)
        src = self.shards[a] if (lane == 0 and i == 0 and core is self.me.core) else here
        return send(src, here, self.psend.at[a, lane, i], self.precv.at[a, lane, i], self.pair)

    def to_pair_half(self, a, i, way, core):
        here = self.spot(a, 2, i, core).at[:, self.half(a, way)]
        return send(here, here, self.qsend.at[a, way, i], self.qrecv.at[a, way, i], self.pair)

    def begin(self):
        for a in self.every:
            self.own(a).start()
        greet(self.me, peers_of(self.me))
        for a in self.every:
            for way in range(2):
                self.to_ring(a, 0, way).start()
            for i in range(1, self.line_size):
                self.to_line(a, i).start()
        for a in self.every:
            self.to_pair(a, 0, 0, self.me.core).start()

    def line_stage(self, i):
        for a in self.every:
            self.from_line(a, i).wait_recv()
            for way in range(2):
                self.to_ring(a, i, way).start()
            self.to_pair(a, i, 0, self.me.core).start()

    def ring_stage(self, i):
        for way in range(2):
            for a in self.every:
                self.from_ring(a, i, way).wait_recv()
                if self.halved(a, way):
                    self.onward(a, i, way).start()
                self.to_pair(a, i, 1 + way, self.me.core).start()

    def far_stage(self, i):
        for way in range(2):
            for a in self.every:
                if self.halved(a, way):
                    self.from_onward(a, i, way).wait_recv()
                    self.to_pair_half(a, i, way, self.me.core).start()

    def stages(self):
        found = []
        for wave in range(self.line_size + 2):
            if 1 <= wave < self.line_size:
                found.append(partial(self.line_stage, wave))
            if 1 <= wave <= self.line_size:
                found.append(partial(self.ring_stage, wave - 1))
            if 2 <= wave:
                found.append(partial(self.far_stage, wave - 2))
        return found

    def finish(self):
        core = self.me.core
        for a in self.every:
            self.own(a).wait()
            for i in range(self.line_size):
                for lane in range(3):
                    self.to_pair(a, i, lane, 1 - core).wait_recv()
                    self.to_pair(a, i, lane, core).wait_send()
                for way in range(2):
                    self.to_ring(a, i, way).wait_send()
                    if self.halved(a, way):
                        self.to_pair_half(a, i, way, 1 - core).wait_recv()
                        self.to_pair_half(a, i, way, core).wait_send()
                        self.onward(a, i, way).wait_send()
                if i:
                    self.to_line(a, i).wait_send()


def gather_scratch(kinds, line_size):
    sems = pltpu.SemaphoreType.DMA
    return (
        [sems((kinds,))]
        + [sems((kinds, line_size))] * 2
        + [sems((kinds, 2, line_size))] * 4
        + [sems((kinds, 3, line_size))] * 2
        + [sems((kinds, 2, line_size))] * 2
    )


def gather_kernel(ring_size, line_size, kinds, *refs):
    job = Gather(ring_size, line_size, refs[:kinds], refs[kinds : 2 * kinds], refs[2 * kinds :])
    job.begin()
    for stage in job.stages():
        stage()
    job.finish()


def gather(shards, ring_size, line_size, ident):
    kinds = len(shards)
    count = 2 * ring_size * line_size
    return pl.pallas_call(
        partial(gather_kernel, ring_size, line_size, kinds),
        in_specs=[pl.BlockSpec(memory_space=pltpu.VMEM)] * kinds,
        out_specs=[pl.BlockSpec(memory_space=pl.ANY)] * kinds,
        out_shape=[jax.ShapeDtypeStruct((count,) + piece.shape, piece.dtype) for piece in shards],
        scratch_shapes=gather_scratch(kinds, line_size),
        compiler_params=pltpu.CompilerParams(collective_id=ident, has_side_effects=True),
        name="gather_shards",
    )(*shards)


def spread(stages, tick, ticks):
    for number, stage in enumerate(stages):
        pl.when(tick == number * ticks // len(stages))(stage)


def rms_factor(values, eps):
    return lax.rsqrt(jnp.mean(values * values, axis=-1, keepdims=True) + eps)


def rms_back(grad, values, factor, gain):
    scaled = values * factor
    dscaled = grad * gain
    dvalues = factor * (dscaled - scaled * jnp.mean(dscaled * scaled, axis=-1, keepdims=True))
    return dvalues, jnp.sum(grad * scaled, axis=0)


def by_kernel(sizes, ring_size, fsdp_size):
    return ring_size == 4 and fsdp_size % 4 == 0 and all(size % 8 == 0 for size in sizes)


def gather_plain(shards):
    return [lax.all_gather(piece, AXES, axis=0) for piece in shards]


def scatter_plain(grads):
    return [lax.psum_scatter(piece.astype(F32), AXES, scatter_dimension=0) for piece in grads]


def per_device(
    hidden_in,
    w_query,
    w_latent,
    w_key_up,
    w_value_up,
    w_decay,
    w_outgate,
    w_out,
    w_gate,
    w_up,
    w_down,
    vectors,
    seg_ids,
    pad_mask,
    cotangent,
    *,
    ring_size,
    fsdp_size,
):
    count = ring_size * fsdp_size
    per_group = WIDTH // GROUPS
    latents = GROUPS * LATENT
    rows_d, rows_kv, rows_ff = D // count, latents // count, FF // count
    rows_all = (rows_d, rows_kv, rows_ff)
    vec_size = (2 * D + 2 * WIDTH) // count

    def rows_of(piece, rows):
        return piece.astype(BF).reshape(rows, -1)

    in_shard = jnp.concatenate(
        [rows_of(piece, rows_d) for piece in (w_query, w_decay, w_outgate, w_latent)], axis=1
    )
    kv_shard = jnp.concatenate([rows_of(w_key_up, rows_kv), rows_of(w_value_up, rows_kv)], axis=1)
    out_shard = rows_of(w_out, rows_d)
    ff_shard = jnp.concatenate([rows_of(w_gate, rows_d), rows_of(w_up, rows_d)], axis=1)
    down_shard = rows_of(w_down, rows_ff)
    vec_shard = jnp.broadcast_to(lax.reduce_precision(vectors, 8, 7).reshape(1, -1), (8, vec_size))
    own = by_kernel(rows_all, ring_size, fsdp_size)
    comm = (ring_size, fsdp_size // 2)
    early, late = (in_shard, kv_shard, vec_shard), (out_shard, ff_shard, down_shard)
    w_in, w_kv, vecs = gather(early, *comm, 0) if own else gather_plain(early)
    w_in = w_in.reshape(D, 3 * WIDTH + latents)
    w_kv = w_kv.reshape(GROUPS, LATENT, 2 * per_group)
    vecs = vecs[:, 0].reshape(-1)
    gain_in, gain_mid = vecs[:D], vecs[D : 2 * D]
    decay_bias, out_gain = vecs[2 * D : 2 * D + WIDTH], vecs[2 * D + WIDTH :]

    seg = seg_ids.reshape(CHUNKS, SPAN)
    before = jnp.concatenate([jnp.full((1,), -1, seg.dtype), seg[:-1, -1]])
    fresh = (seg == before[:, None]).astype(F32).reshape(LEN, 1)
    to_end = (seg == seg[:, -1:]).astype(F32).reshape(LEN, 1)
    pad = pad_mask.astype(F32).reshape(LEN, 1)
    seg_col = seg_ids.astype(F32).reshape(LEN, 1)
    cols = jnp.concatenate(
        [seg_col, fresh, to_end, pad, jnp.zeros((LEN, 124), F32)], axis=1
    )
    segs = seg_ids.astype(F32).reshape(CHUNKS, 1, SPAN)

    inputs = hidden_in.astype(F32)
    factor_in = rms_factor(inputs, 1e-5)
    normed = (inputs * factor_in * gain_in).astype(BF)
    latent = mm(normed, w_in[:, 3 * WIDTH :]).astype(BF)
    bias_row, gain_row = decay_bias.reshape(1, WIDTH), out_gain.reshape(1, WIDTH)
    query, keys, values, decay_in, gate_in, mixed, heads, states, *rest = mixer_fwd(
        normed, latent, w_in, w_kv, bias_row, gain_row, cols, segs, late if own else (), comm + (0, 2) if own else None
    )
    w_output, w_ff, w_dn = rest if own else gather_plain(late)
    w_output = w_output.reshape(WIDTH, D)
    w_ff = w_ff.reshape(D, 2 * FF)
    w_dn = w_dn.reshape(FF, D)
    middle = inputs + mm(mixed, w_output)
    factor_mid = rms_factor(middle, 1e-5)
    normed_mid = (middle * factor_mid * gain_mid).astype(BF)
    gate_val = mm(normed_mid, w_ff[:, :FF])
    up_val = mm(normed_mid, w_ff[:, FF:])
    sig = jax.nn.sigmoid(gate_val)
    silu = gate_val * sig
    hidden = (silu * up_val).astype(BF)
    block_out = (middle + mm(hidden, w_dn)).astype(BF)

    d_outf = cotangent.astype(F32) * pad
    d_ffn = d_outf.astype(BF)
    grad_down = mm_tn(hidden, d_ffn)
    d_hidden = mm_nt(d_ffn, w_dn)
    d_gate = (d_hidden * up_val * (sig * (1.0 + gate_val * (1.0 - sig)))).astype(BF)
    d_up = (d_hidden * silu).astype(BF)
    d_both = jnp.concatenate([d_gate, d_up], axis=1)
    grad_ff = mm_tn(normed_mid, d_both)
    d_normed_mid = mm_nt(d_both, w_ff)
    d_middle, d_gain_mid = rms_back(d_normed_mid, middle, factor_mid, gain_mid)
    d_middle = d_middle + d_outf
    d_branch = d_middle.astype(BF)
    grad_out = mm_tn(mixed, d_branch)

    sent = (grad_ff.astype(BF).reshape(count, rows_d, -1), grad_down.astype(BF).reshape(count, rows_ff, -1))
    saved = (query, keys, values, decay_in, gate_in, gain_row, cols, segs, heads, states)
    d_query, d_keys, d_values, d_decay, d_gatein, d_bias, d_out_gain, *rest = mixer_bwd(
        saved, d_branch, w_output, sent if own else (), comm + (0, 3) if own else None
    )
    own_ff, own_down = rest if own else scatter_plain(sent)
    grad_kv, d_latent = [], []
    for g in range(GROUPS):
        d_kv = jnp.concatenate(
            [part[:, g * per_group : (g + 1) * per_group] for part in (d_keys, d_values)], axis=1
        )
        grad_kv.append(mm_tn(latent[:, g * LATENT : (g + 1) * LATENT], d_kv))
        d_latent.append(mm_nt(d_kv, w_kv[g]))
    grad_kv = jnp.concatenate(grad_kv, axis=0)
    d_latent = jnp.concatenate(d_latent, axis=1).astype(BF)
    d_in = jnp.concatenate([d_query, d_decay, d_gatein, d_latent], axis=1)
    grad_in = mm_tn(normed, d_in)
    d_normed = mm_nt(d_in, w_in)
    d_inputs, d_gain_in = rms_back(d_normed, inputs, factor_in, gain_in)
    grad_input = d_middle + d_inputs
    grad_vec = jnp.concatenate([d_gain_in, d_gain_mid, d_bias.reshape(-1), d_out_gain.reshape(-1)])

    grad_vec = jnp.broadcast_to(grad_vec.reshape(count, 1, vec_size), (count, 8, vec_size))
    sent = (
        grad_in.astype(BF).reshape(count, rows_d, -1),
        grad_kv.astype(BF).reshape(count, rows_kv, -1),
        grad_out.astype(BF).reshape(count, rows_d, -1),
        grad_vec,
    )
    own_in, own_kv, own_out, own_vec = scatter(sent, *comm, 1) if own else scatter_plain(sent)
    return (
        block_out,
        grad_input,
        own_in[:, :WIDTH].reshape(-1),
        own_in[:, 3 * WIDTH :].reshape(-1),
        own_kv[:, :per_group].reshape(-1),
        own_kv[:, per_group:].reshape(-1),
        own_in[:, WIDTH : 2 * WIDTH].reshape(-1),
        own_in[:, 2 * WIDTH : 3 * WIDTH].reshape(-1),
        own_out.reshape(-1),
        own_ff[:, :FF].reshape(-1),
        own_ff[:, FF:].reshape(-1),
        own_down.reshape(-1),
        own_vec[0],
    )


def solution(mesh):
    sizes = {"ring_size": mesh.shape["dp"], "fsdp_size": mesh.shape["fsdp"]}
    rows, flat = P(AXES, None), P(AXES)
    in_specs = (rows,) + (flat,) * 13 + (rows,)
    out_specs = (rows, rows) + (flat,) * 11
    return jax.shard_map(
        partial(per_device, **sizes), mesh=mesh, in_specs=in_specs, out_specs=out_specs, check_vma=False
    )
```

```python
from functools import partial

import jax
import jax.numpy as jnp
from jax import lax
from jax.experimental import pallas as pl
from jax.experimental.pallas import tpu as pltpu
from jax.sharding import PartitionSpec as P

D = 1024
HEADS = 16
HEAD_DIM = 64
GROUPS = 2
LATENT = 256
FF = 2816
LEN = 1024
WIDTH = HEADS * HEAD_DIM
SPAN = 128
LANES = 256
PACK = LANES // HEAD_DIM
BANDS = WIDTH // LANES
CHUNKS = LEN // SPAN
LIMIT = 85.0
AXES = ("dp", "fsdp")
BF = jnp.bfloat16
F32 = jnp.float32
MESH = pl.DeviceIdType.MESH


def mm(left, right):
    return lax.dot_general(left, right, (((1,), (0,)), ((), ())), preferred_element_type=F32)


def mm_nt(left, right):
    return lax.dot_general(left, right, (((1,), (1,)), ((), ())), preferred_element_type=F32)


def mm_tn(left, right):
    return lax.dot_general(left, right, (((0,), (0,)), ((), ())), preferred_element_type=F32)


def halves(value):
    high = value.astype(BF)
    return high, (value - high.astype(F32)).astype(BF)


def exact_left(ones, value):
    high, rest = halves(value)
    return mm(ones, high) + mm(ones, rest)


def exact_right(value, ones):
    high, rest = halves(value)
    return mm(high, ones) + mm(rest, ones)


def head_masks():
    lane = lax.broadcasted_iota(jnp.int32, (1, LANES), 1) // HEAD_DIM
    return [lane == head for head in range(PACK)]


def stacked(value, masks):
    zero = jnp.zeros_like(value)
    return jnp.concatenate([jnp.where(mask, value, zero) for mask in masks], axis=0)


def side_by_side(value):
    return jnp.concatenate([value[h * SPAN : (h + 1) * SPAN] for h in range(PACK)], axis=1)


def same_head():
    row = lax.broadcasted_iota(jnp.int32, (LANES, LANES), 0) // HEAD_DIM
    col = lax.broadcasted_iota(jnp.int32, (LANES, LANES), 1) // HEAD_DIM
    return row == col


def triangle(lower):
    row = lax.broadcasted_iota(jnp.int32, (SPAN, SPAN), 0)
    col = lax.broadcasted_iota(jnp.int32, (SPAN, SPAN), 1)
    return (row >= col) if lower else (row <= col)


def decays(decay, pad, lower_ones):
    small = jnp.exp(-jnp.abs(decay))
    log_sig = jnp.minimum(decay, 0.0) - jnp.log(1.0 + small)
    total = exact_left(lower_ones, log_sig * (pad * (1.0 / 16.0)))
    ending = total[SPAN - 1 : SPAN]
    middle = 0.5 * ending
    centred = total - middle
    up = jnp.exp(jnp.minimum(centred, LIMIT))
    down = jnp.exp(jnp.minimum(-centred, LIMIT))
    half = jnp.exp(middle)
    return up, down, half, small


def flags(seg_ref, pad_ref, index):
    seg_row = seg_ref[index]
    seg_square = jnp.transpose(jnp.broadcast_to(seg_row, (SPAN, SPAN)))
    pad = jnp.transpose(jnp.broadcast_to(pad_ref[index], (SPAN, SPAN)))[:, 0:1]
    seg_col, ending = seg_square[:, 0:1], seg_row[:, SPAN - 1 :]
    before = seg_ref[jnp.maximum(index - 1, 0)][:, SPAN - 1 :]
    fresh = (seg_col == before).astype(F32)
    to_end = (seg_col == ending).astype(F32)
    keep = (ending == before).astype(F32)
    allowed = (seg_square == seg_row) & triangle(True)
    return fresh, to_end, pad, allowed, keep


def mixer_fwd_kernel(comm, *refs):
    kinds = comm[2] if comm else 0
    normed_ref, latent_ref, wq_ref, wd_ref, wg_ref, wk_ref, wv_ref, bias_ref, gain_ref, seg_ref, pad_ref = refs[:11]
    shards, refs = refs[11 : 11 + kinds], refs[11 + kinds :]
    q_ref, k_ref, v_ref, decay_ref, gate_ref, mixed_ref, heads_ref, states_ref = refs[:8]
    gathered, state, sems = refs[8 : 8 + kinds], refs[8 + kinds], refs[9 + kinds :]
    band = pl.program_id(0)
    job = Gather(comm[0], comm[1], shards, gathered, sems) if comm else None
    stages = job.stages() if comm else []
    ticks = BANDS * (CHUNKS + 1)
    if comm:
        pl.when(band == 0)(job.begin)
    masks = head_masks()
    diag = same_head()
    diag_ones = diag.astype(F32).astype(BF)
    lower_ones = triangle(True).astype(F32).astype(BF)
    state[...] = jnp.zeros_like(state)
    gain = gain_ref[...]
    q_ref[...] = mm(normed_ref[...], wq_ref[...])
    decay_ref[...] = mm(normed_ref[...], wd_ref[...]) + bias_ref[...]
    gate_ref[...] = mm(normed_ref[...], wg_ref[...])
    k_ref[...] = mm(latent_ref[...], wk_ref[0])
    v_ref[...] = mm(latent_ref[...], wv_ref[0])

    def chunk(index, carry):
        spread(stages, band * (CHUNKS + 1) + index, ticks)
        rows = pl.ds(pl.multiple_of(index * SPAN, SPAN), SPAN)
        fresh, to_end, pad, allowed, keep = flags(seg_ref, pad_ref, index)
        up, down, half, _ = decays(decay_ref[rows, :], pad, lower_ones)
        query = q_ref[rows, :] * (HEAD_DIM**-0.5) * up
        key = k_ref[rows, :] * pad * down
        value = v_ref[rows, :].astype(BF)
        query_low, key_low = query.astype(BF), key.astype(BF)
        scores = mm_nt(stacked(query_low, masks), key_low)
        scores = scores.reshape(PACK, SPAN, SPAN)
        scores = jnp.where(allowed[None], scores, 0.0).astype(BF).reshape(PACK * SPAN, SPAN)
        old = state[...]
        old_low = old.astype(BF)
        states_ref[0, index] = old_low
        heads = mm(side_by_side(scores), stacked(value, masks))
        heads += mm_nt((query * (half * fresh)).astype(BF), old_low)
        tail = (key * (half * to_end)).astype(BF)
        state[...] = old * (half * half * keep) + jnp.where(diag, mm_tn(value, tail), 0.0)
        heads_ref[rows, :] = heads
        scale = lax.rsqrt(exact_right(heads * heads, diag_ones) * (1.0 / HEAD_DIM) + 1e-2)
        gate = gate_ref[rows, :]
        silu = gate / (1.0 + jnp.exp(-gate))
        mixed_ref[rows, :] = (heads * scale * gain * silu).astype(BF)
        return carry

    lax.fori_loop(0, CHUNKS, chunk, 0)
    spread(stages, band * (CHUNKS + 1) + CHUNKS, ticks)
    if comm:
        pl.when(band == BANDS - 1)(job.finish)


def mixer_bwd_kernel(comm, *refs):
    kinds = comm[2] if comm else 0
    q_ref, k_ref, v_ref, decay_ref, gate_ref, gain_ref, seg_ref, pad_ref, heads_ref, states_ref = refs[:10]
    dbranch_ref, wo_ref = refs[10:12]
    grads, refs = refs[12 : 12 + kinds], refs[12 + kinds :]
    dq_ref, dk_ref, dv_ref, ddecay_ref, dgate_ref, dbias_ref, dgain_ref = refs[:7]
    sums, state, dmix_ref, scratch = refs[7 : 7 + kinds], refs[7 + kinds], refs[8 + kinds], refs[9 + kinds :]
    band = pl.program_id(0)
    job = scatter_of(comm[0], comm[1], grads, sums, scratch) if comm else None
    stages = job.stages() if comm else []
    ticks = BANDS * (CHUNKS + 1)
    if comm:
        pl.when(band == 0)(job.begin)
    dmix_ref[...] = mm_nt(dbranch_ref[...], wo_ref[...])
    masks = head_masks()
    diag = same_head()
    diag_ones = diag.astype(F32).astype(BF)
    lower_ones = triangle(True).astype(F32).astype(BF)
    upper_ones = triangle(False).astype(F32).astype(BF)
    state[...] = jnp.zeros_like(state)
    dbias_ref[...] = jnp.zeros_like(dbias_ref)
    dgain_ref[...] = jnp.zeros_like(dgain_ref)
    gain = gain_ref[...]

    def chunk(step, carry):
        spread(stages, band * (CHUNKS + 1) + step, ticks)
        index = CHUNKS - 1 - step
        rows = pl.ds(pl.multiple_of(index * SPAN, SPAN), SPAN)
        fresh, to_end, pad, allowed, keep = flags(seg_ref, pad_ref, index)
        heads = heads_ref[rows, :]
        scale = lax.rsqrt(exact_right(heads * heads, diag_ones) * (1.0 / HEAD_DIM) + 1e-2)
        normed = heads * scale
        gate = gate_ref[rows, :]
        sig = 1.0 / (1.0 + jnp.exp(-gate))
        silu = gate * sig
        dmix = dmix_ref[rows, :]
        both = dmix * normed
        dgain_ref[...] += jnp.sum(both * silu, axis=0, keepdims=True)
        dgate_ref[rows, :] = (both * gain * (sig * (1.0 + gate * (1.0 - sig)))).astype(BF)
        dnormed = dmix * gain * silu
        mean = exact_right(dnormed * normed, diag_ones) * (1.0 / HEAD_DIM)
        dheads = (scale * (dnormed - normed * mean)).astype(BF)
        decay = decay_ref[rows, :]
        up, down, half, small = decays(decay, pad, lower_ones)
        unit = HEAD_DIM**-0.5
        query = q_ref[rows, :] * unit * up
        key = k_ref[rows, :] * pad * down
        value = v_ref[rows, :].astype(BF)
        query_low, key_low = query.astype(BF), key.astype(BF)
        enter = half * fresh
        leave = half * to_end
        query_in = (query * enter).astype(BF)
        tail = (key * leave).astype(BF)
        query_stack = stacked(query_low, masks)
        dheads_stack = stacked(dheads, masks)
        scores = mm_nt(query_stack, key_low).reshape(PACK, SPAN, SPAN)
        scores = jnp.where(allowed[None], scores, 0.0).astype(BF).reshape(PACK * SPAN, SPAN)
        dscores = mm_nt(dheads_stack, value).reshape(PACK, SPAN, SPAN)
        dscores = jnp.where(allowed[None], dscores, 0.0).astype(BF).reshape(PACK * SPAN, SPAN)
        dstate = state[...]
        dstate_low = dstate.astype(BF)
        old = states_ref[0, index]
        dvalue = mm_tn(scores, dheads_stack) + mm_nt(tail, dstate_low)
        dv_ref[rows, :] = dvalue.astype(BF)
        dquery = mm(side_by_side(dscores), stacked(key_low, masks))
        dkey = mm_tn(dscores, query_stack)
        dquery_in = mm(dheads, old)
        dtail = mm(value, dstate_low)
        whole = half * half * keep
        state[...] = dstate * whole + jnp.where(diag, mm_tn(dheads, query_in), 0.0)
        dq_ref[rows, :] = ((dquery + dquery_in * enter) * (up * unit)).astype(BF)
        dk_ref[rows, :] = ((dkey + dtail * leave) * (down * pad)).astype(BF)
        from_tail = dtail * tail.astype(F32)
        dtotal = (
            dquery * query_low.astype(F32)
            - dkey * key_low.astype(F32)
            + dquery_in * query_in.astype(F32)
            - from_tail
        )
        ends = jnp.sum(from_tail, axis=0, keepdims=True)
        ends += whole * jnp.sum(dstate * old.astype(F32), axis=0, keepdims=True)
        dlog = exact_left(upper_ones, dtotal) + ends
        other = jnp.where(decay >= 0, small, 1.0) / (1.0 + small)
        ddecay = dlog * (pad * (1.0 / 16.0)) * other
        dbias_ref[...] += jnp.sum(ddecay, axis=0, keepdims=True)
        ddecay_ref[rows, :] = ddecay.astype(BF)
        return carry

    lax.fori_loop(0, CHUNKS, chunk, 0)
    spread(stages, band * (CHUNKS + 1) + CHUNKS, ticks)
    if comm:
        pl.when(band == BANDS - 1)(job.finish)


def band_specs():
    tokens = pl.BlockSpec((LEN, LANES), lambda band: (0, band))
    vector = pl.BlockSpec((1, LANES), lambda band: (0, band))
    segs = pl.BlockSpec((CHUNKS, 1, SPAN), lambda band: (0, 0, 0))
    states = pl.BlockSpec((1, CHUNKS, LANES, LANES), lambda band: (band, 0, 0, 0))
    return tokens, vector, segs, states


def fixed(shape):
    return pl.BlockSpec(shape, lambda band: (0,) * len(shape), pipeline_mode=pl.Buffered(1))


def mixer_fwd(normed, latent, w_in, w_kv, bias, gain, segs, pads, shards, comm):
    tokens, vector, segs_spec, states = band_specs()
    kinds = len(shards)
    half_bands = BANDS // GROUPS
    in_specs = [fixed((LEN, D)), pl.BlockSpec((LEN, LATENT), lambda band: (0, band // half_bands))]
    for part in range(3):
        in_specs.append(pl.BlockSpec((D, LANES), lambda band, part=part: (0, part * BANDS + band)))
    for part in range(2):
        in_specs.append(
            pl.BlockSpec(
                (1, LATENT, LANES),
                lambda band, part=part: (band // half_bands, 0, part * half_bands + band % half_bands),
            )
        )
    in_specs += [vector, vector, segs_spec, segs_spec]
    wide = jax.ShapeDtypeStruct((LEN, WIDTH), F32)
    out_shape = [wide] * 5 + [
        jax.ShapeDtypeStruct((LEN, WIDTH), BF),
        wide,
        jax.ShapeDtypeStruct((BANDS, CHUNKS, LANES, LANES), BF),
    ]
    scratch = [pltpu.VMEM((LANES, LANES), F32)]
    params = {}
    if comm:
        count = 2 * comm[0] * comm[1]
        in_specs += [fixed(shard.shape) for shard in shards]
        out_shape += [jax.ShapeDtypeStruct((count,) + shard.shape, shard.dtype) for shard in shards]
        scratch += gather_scratch(kinds, comm[1])
        params = {"collective_id": comm[3], "has_side_effects": True}
        comm = comm[:2] + (kinds,)
    return pl.pallas_call(
        partial(mixer_fwd_kernel, comm),
        grid=(BANDS,),
        in_specs=in_specs,
        out_specs=[tokens] * 7 + [states] + [pl.BlockSpec(memory_space=pl.ANY)] * kinds,
        out_shape=out_shape,
        scratch_shapes=scratch,
        compiler_params=pltpu.CompilerParams(vmem_limit_bytes=52 << 20, **params),
        name="mixer_fwd",
    )(normed, latent, w_in, w_in, w_in, w_kv, w_kv, bias, gain, segs, pads, *shards)


def mixer_bwd(saved, d_branch, w_output, grads, comm):
    tokens, vector, segs_spec, states = band_specs()
    kinds = len(grads)
    low = jax.ShapeDtypeStruct((LEN, WIDTH), BF)
    sums = jax.ShapeDtypeStruct((1, WIDTH), F32)
    in_specs = [tokens] * 5 + [vector, segs_spec, segs_spec, tokens, states]
    in_specs += [fixed((LEN, D)), pl.BlockSpec((LANES, D), lambda band: (band, 0))]
    out_specs, out_shape = [tokens] * 5 + [vector, vector], [low] * 5 + [sums, sums]
    scratch = [pltpu.VMEM((LANES, LANES), F32), pltpu.VMEM((LEN, LANES), F32)]
    params = {}
    if comm:
        in_specs += [pl.BlockSpec(memory_space=pl.ANY)] * kinds
        out_specs += [fixed(grad.shape[1:]) for grad in grads]
        out_shape += [jax.ShapeDtypeStruct(grad.shape[1:], F32) for grad in grads]
        scratch += scatter_scratch(grads, comm[0], comm[1])
        params = {"collective_id": comm[3], "has_side_effects": True}
        comm = comm[:2] + (kinds,)
    return pl.pallas_call(
        partial(mixer_bwd_kernel, comm),
        grid=(BANDS,),
        in_specs=in_specs,
        out_specs=out_specs,
        out_shape=out_shape,
        scratch_shapes=scratch,
        compiler_params=pltpu.CompilerParams(vmem_limit_bytes=63 << 20, **params),
        name="mixer_bwd",
    )(*saved, d_branch, w_output, *grads)


class Place:
    def __init__(self, ring_size, line_size):
        self.ring_size, self.line_size = ring_size, line_size
        self.d, f = lax.axis_index("dp"), lax.axis_index("fsdp")
        self.z, self.core = f // 2, f % 2
        self.pos = self.at_ring(self.d)

    def at_ring(self, index):
        if self.ring_size != 4:
            return index
        return index + (index // 2) * (1 - 2 * (index % 2))

    def ring(self, offset):
        return self.at_ring((self.pos + offset + self.ring_size) % self.ring_size)

    def far(self, i):
        n = self.line_size
        low = self.z < n // 2
        near = jnp.where(low, self.z, n - 1 - self.z)
        if i == n - 1:
            return self.z
        line = n - 1 - i - jnp.where(n - 1 - i <= near, 1, 0)
        return jnp.where(low, line, n - 1 - line)

    def device(self, d, z, core):
        return (d, 2 * z + core)

    def slot(self, d, z, core):
        return d * (2 * self.line_size) + 2 * z + core


def greet(place, peers):
    barrier = pltpu.get_barrier_semaphore()
    for peer in peers:
        pl.semaphore_signal(barrier, inc=1, device_id=peer, device_id_type=MESH)
    pl.semaphore_wait(barrier, len(peers))


def peers_of(place):
    me = place
    peers = [me.device(me.d, me.z, 1 - me.core)]
    peers += [me.device(me.ring(step), me.z, me.core) for step in (1, -1)]
    peers += [me.device(me.d, me.far(i), me.core) for i in range(me.line_size - 1)]
    return peers


def send(src, dst, send_sem, recv_sem, device):
    return pltpu.make_async_remote_copy(
        src_ref=src, dst_ref=dst, send_sem=send_sem, recv_sem=recv_sem, device_id=device, device_id_type=MESH
    )


class Scatter:
    def __init__(self, ring_size, line_size, grads, outs, accs, parts, hops, tails, sems):
        self.ring_size, self.line_size = ring_size, line_size
        self.grads, self.outs = grads, outs
        self.accs, self.parts, self.hops, self.tails = accs, parts, hops, tails
        self.load_sem, self.psend, self.precv, self.hsend, self.hrecv, self.tsend, self.trecv = sems
        self.me = Place(ring_size, line_size)
        self.order = [self.me.far(i) for i in range(line_size)]
        self.every = range(len(grads))
        self.waves = [
            (step, wave - step)
            for wave in range(1, ring_size + line_size)
            for step in range(1, ring_size + 1)
            if 0 <= wave - step < line_size
        ]

    def way(self, a, i):
        return 1 if (a + i) % 2 == 0 else -1

    def dest(self, a, step, i, core):
        me = self.me
        return self.grads[a].at[me.slot(me.ring(-step * self.way(a, i)), self.order[i], core)]

    def load(self, a, step, i):
        return pltpu.make_async_copy(
            self.dest(a, step, i, self.me.core), self.accs[a].at[step - 1, i], self.load_sem.at[a, step - 1, i]
        )

    def to_pair(self, a, step, i):
        me = self.me
        return send(
            self.dest(a, step, i, 1 - me.core),
            self.parts[a].at[step - 1, i],
            self.psend.at[a, step - 1, i],
            self.precv.at[a, step - 1, i],
            me.device(me.d, me.z, 1 - me.core),
        )

    def to_ring(self, a, step, i):
        me = self.me
        return send(
            self.accs[a].at[step - 1, i],
            self.hops[a].at[step - 1, i],
            self.hsend.at[a, step - 1, i],
            self.hrecv.at[a, step - 1, i],
            me.device(me.ring(self.way(a, i)), me.z, me.core),
        )

    def to_line(self, a, i):
        me = self.me
        return send(
            self.accs[a].at[self.ring_size - 1, i],
            self.tails[a].at[me.z],
            self.tsend.at[a, i],
            self.trecv.at[a, me.z],
            me.device(me.d, self.order[i], me.core),
        )

    def from_line(self, a, i):
        me = self.me
        here = self.tails[a].at[self.order[i]]
        return send(
            here, here, self.tsend.at[a, i], self.trecv.at[a, self.order[i]], me.device(me.d, self.order[i], me.core)
        )

    def blocks(self, a):
        width = self.grads[a].shape[-1]
        block = 512 if width % 512 == 0 else width
        return width // block, block

    def add_up(self, a, step, i):
        number, block = self.blocks(a)
        acc, final = self.accs[a], step == self.ring_size and i == self.line_size - 1

        def body(j, carry):
            cols = pl.ds(pl.multiple_of(j * block, block), block)
            total = acc[step - 1, i, :, cols].astype(F32) + self.parts[a][step - 1, i, :, cols].astype(F32)
            if step > 1:
                total += self.hops[a][step - 2, i, :, cols].astype(F32)
            if final:
                self.outs[a][:, cols] = total
            else:
                acc[step - 1, i, :, cols] = total.astype(acc.dtype)
            return carry

        lax.fori_loop(0, number, body, 0)

    def begin(self):
        for step, i in self.waves:
            for a in self.every:
                self.load(a, step, i).start()
        greet(self.me, peers_of(self.me))
        for step, i in self.waves:
            for a in self.every:
                self.to_pair(a, step, i).start()

    def entry(self, step, i):
        for a in self.every:
            self.load(a, step, i).wait()
            self.to_pair(a, step, i).wait_recv()
            if step > 1:
                self.to_ring(a, step - 1, i).wait_recv()
            self.add_up(a, step, i)
            if step < self.ring_size:
                self.to_ring(a, step, i).start()
            elif i < self.line_size - 1:
                self.to_line(a, i).start()

    def stages(self):
        return [partial(self.entry, step, i) for step, i in self.waves]

    def finish(self):
        last = self.line_size - 1
        for a in self.every:
            for i in range(last):
                self.from_line(a, i).wait_recv()
            number, block = self.blocks(a)

            def body(j, carry, a=a, block=block):
                cols = pl.ds(pl.multiple_of(j * block, block), block)
                total = self.outs[a][:, cols]
                for i in range(last):
                    total += self.tails[a][self.order[i], :, cols].astype(F32)
                self.outs[a][:, cols] = total
                return carry

            lax.fori_loop(0, number, body, 0)
        for step, i in self.waves:
            for a in self.every:
                self.to_pair(a, step, i).wait_send()
                if step < self.ring_size:
                    self.to_ring(a, step, i).wait_send()
                elif i < last:
                    self.to_line(a, i).wait_send()


def scatter_scratch(grads, ring_size, line_size):
    kinds = len(grads)
    sems = pltpu.SemaphoreType.DMA
    scratch = []
    for lead in ((ring_size, line_size), (ring_size, line_size), (ring_size - 1, line_size), (line_size,)):
        scratch += [pltpu.VMEM(lead + grad.shape[1:], grad.dtype) for grad in grads]
    return scratch + [sems((kinds, ring_size, line_size))] * 5 + [sems((kinds, line_size))] * 2


def scatter_of(ring_size, line_size, grads, outs, scratch):
    kinds = len(grads)
    rooms = [scratch[k * kinds : (k + 1) * kinds] for k in range(4)]
    return Scatter(ring_size, line_size, grads, outs, *rooms, scratch[4 * kinds :])


def scatter_kernel(ring_size, line_size, kinds, *refs):
    job = scatter_of(ring_size, line_size, refs[:kinds], refs[kinds : 2 * kinds], refs[2 * kinds :])
    job.begin()
    for stage in job.stages():
        stage()
    job.finish()


def scatter(grads, ring_size, line_size, ident):
    kinds = len(grads)
    return pl.pallas_call(
        partial(scatter_kernel, ring_size, line_size, kinds),
        in_specs=[pl.BlockSpec(memory_space=pl.ANY)] * kinds,
        out_specs=[pl.BlockSpec(memory_space=pltpu.VMEM)] * kinds,
        out_shape=[jax.ShapeDtypeStruct(grad.shape[1:], F32) for grad in grads],
        scratch_shapes=scatter_scratch(grads, ring_size, line_size),
        compiler_params=pltpu.CompilerParams(
            collective_id=ident, has_side_effects=True, vmem_limit_bytes=60 << 20
        ),
        name="scatter_sums",
    )(*grads)


class Gather:
    def __init__(self, ring_size, line_size, shards, outs, sems):
        self.line_size = line_size
        self.shards, self.outs = shards, outs
        (
            self.own_sem,
            self.zsend,
            self.zrecv,
            self.hsend,
            self.hrecv,
            self.osend,
            self.orecv,
            self.psend,
            self.precv,
            self.qsend,
            self.qrecv,
        ) = sems
        self.me = Place(ring_size, line_size)
        self.order = [self.me.far(line_size - 1 - i) for i in range(line_size)]
        self.pair = self.me.device(self.me.d, self.me.z, 1 - self.me.core)
        self.mine = self.me.slot(self.me.d, self.me.z, self.me.core)
        self.every = range(len(shards))

    def half(self, a, way):
        width = self.shards[a].shape[-1]
        if width % 256:
            return pl.ds(0, width)
        return pl.ds(0 if way == 0 else width // 2, width // 2)

    def halved(self, a, way):
        return self.shards[a].shape[-1] % 256 == 0 or way == 0

    def beside(self, way):
        return self.me.device(self.me.ring(1 - 2 * way), self.me.z, self.me.core)

    def spot(self, a, offset, i, core):
        return self.outs[a].at[self.me.slot(self.me.ring(offset), self.order[i], core)]

    def own(self, a):
        return pltpu.make_async_copy(self.shards[a], self.outs[a].at[self.mine], self.own_sem.at[a])

    def along(self, a, i, up):
        me = self.me
        here = self.spot(a, 0, i, me.core)
        return send(
            self.shards[a] if i == 0 else here,
            here,
            self.zsend.at[a, up, i],
            self.zrecv.at[a, self.order[i]],
            me.device(me.d, me.z + 2 * up - 1, me.core),
        )

    def from_line(self, a, i):
        me = self.me
        here = self.spot(a, 0, i, me.core)
        return send(
            here, here, self.zsend.at[a, 0, i], self.zrecv.at[a, self.order[i]], me.device(me.d, self.order[i], me.core)
        )

    def pass_on(self, act, i):
        me, last = self.me, self.line_size - 1
        upward, downward = me.z < last, me.z > 0
        if i:
            upward &= self.order[i] < me.z
            downward &= self.order[i] > me.z
        for up, wanted in ((1, upward), (0, downward)):

            @pl.when(wanted)
            def _(up=up):
                for a in self.every:
                    act(self.along(a, i, up))

    def to_ring(self, a, i, way):
        here = self.spot(a, 0, i, self.me.core)
        src = self.shards[a] if i == 0 else here
        return send(src, here, self.hsend.at[a, way, i], self.hrecv.at[a, way, i], self.beside(way))

    def from_ring(self, a, i, way):
        here = self.spot(a, 2 * way - 1, i, self.me.core)
        return send(here, here, self.hsend.at[a, way, i], self.hrecv.at[a, way, i], self.beside(1 - way))

    def onward(self, a, i, way):
        here = self.spot(a, 2 * way - 1, i, self.me.core).at[:, self.half(a, way)]
        return send(here, here, self.osend.at[a, way, i], self.orecv.at[a, way, i], self.beside(way))

    def from_onward(self, a, i, way):
        here = self.spot(a, 2, i, self.me.core).at[:, self.half(a, way)]
        return send(here, here, self.osend.at[a, way, i], self.orecv.at[a, way, i], self.beside(1 - way))

    def to_pair(self, a, i, lane, core):
        here = self.spot(a, (0, -1, 1)[lane], i, core)
        src = self.shards[a] if (lane == 0 and i == 0 and core is self.me.core) else here
        return send(src, here, self.psend.at[a, lane, i], self.precv.at[a, lane, i], self.pair)

    def to_pair_half(self, a, i, way, core):
        here = self.spot(a, 2, i, core).at[:, self.half(a, way)]
        return send(here, here, self.qsend.at[a, way, i], self.qrecv.at[a, way, i], self.pair)

    def begin(self):
        for a in self.every:
            self.own(a).start()
        greet(self.me, peers_of(self.me))
        for a in self.every:
            for way in range(2):
                self.to_ring(a, 0, way).start()
        self.pass_on(lambda copy: copy.start(), 0)
        for a in self.every:
            self.to_pair(a, 0, 0, self.me.core).start()

    def line_stage(self, i):
        for a in self.every:
            self.from_line(a, i).wait_recv()
            for way in range(2):
                self.to_ring(a, i, way).start()
        self.pass_on(lambda copy: copy.start(), i)
        for a in self.every:
            self.to_pair(a, i, 0, self.me.core).start()

    def ring_stage(self, i):
        for way in range(2):
            for a in self.every:
                self.from_ring(a, i, way).wait_recv()
                if self.halved(a, way):
                    self.onward(a, i, way).start()
                self.to_pair(a, i, 1 + way, self.me.core).start()

    def far_stage(self, i):
        for way in range(2):
            for a in self.every:
                if self.halved(a, way):
                    self.from_onward(a, i, way).wait_recv()
                    self.to_pair_half(a, i, way, self.me.core).start()

    def stages(self):
        found = []
        for wave in range(self.line_size + 2):
            if 1 <= wave < self.line_size:
                found.append(partial(self.line_stage, wave))
            if 1 <= wave <= self.line_size:
                found.append(partial(self.ring_stage, wave - 1))
            if 2 <= wave:
                found.append(partial(self.far_stage, wave - 2))
        return found

    def finish(self):
        core = self.me.core
        for a in self.every:
            self.own(a).wait()
            for i in range(self.line_size):
                for lane in range(3):
                    self.to_pair(a, i, lane, 1 - core).wait_recv()
                    self.to_pair(a, i, lane, core).wait_send()
                for way in range(2):
                    self.to_ring(a, i, way).wait_send()
                    if self.halved(a, way):
                        self.to_pair_half(a, i, way, 1 - core).wait_recv()
                        self.to_pair_half(a, i, way, core).wait_send()
                        self.onward(a, i, way).wait_send()
        for i in range(self.line_size):
            self.pass_on(lambda copy: copy.wait_send(), i)


def gather_scratch(kinds, line_size):
    sems = pltpu.SemaphoreType.DMA
    return (
        [sems((kinds,))]
        + [sems((kinds, 2, line_size)), sems((kinds, line_size))]
        + [sems((kinds, 2, line_size))] * 4
        + [sems((kinds, 3, line_size))] * 2
        + [sems((kinds, 2, line_size))] * 2
    )


def gather_kernel(ring_size, line_size, kinds, *refs):
    job = Gather(ring_size, line_size, refs[:kinds], refs[kinds : 2 * kinds], refs[2 * kinds :])
    job.begin()
    for stage in job.stages():
        stage()
    job.finish()


def gather(shards, ring_size, line_size, ident):
    kinds = len(shards)
    count = 2 * ring_size * line_size
    return pl.pallas_call(
        partial(gather_kernel, ring_size, line_size, kinds),
        in_specs=[pl.BlockSpec(memory_space=pltpu.VMEM)] * kinds,
        out_specs=[pl.BlockSpec(memory_space=pl.ANY)] * kinds,
        out_shape=[jax.ShapeDtypeStruct((count,) + piece.shape, piece.dtype) for piece in shards],
        scratch_shapes=gather_scratch(kinds, line_size),
        compiler_params=pltpu.CompilerParams(collective_id=ident, has_side_effects=True),
        name="gather_shards",
    )(*shards)


def spread(stages, tick, ticks):
    for number, stage in enumerate(stages):
        pl.when(tick == number * ticks // len(stages))(stage)


def pack_kernel(places, *refs):
    flats, packed = refs[: len(places) + 1], refs[len(places) + 1 :]
    for flat, (target, offset, tiles) in zip(flats, places):
        out = packed[target]
        rows = out.shape[0]
        for j in range(tiles):
            out[:, offset + j * 128 : offset + (j + 1) * 128] = flat[pl.ds(j, rows, stride=tiles), :].astype(BF)
    packed[-1][...] = jnp.broadcast_to(flats[-1][...].astype(BF).astype(F32), packed[-1].shape)


def pack(flats, vectors, places, shapes):
    vmem = pl.BlockSpec(memory_space=pltpu.VMEM)
    return pl.pallas_call(
        partial(pack_kernel, places),
        in_specs=[vmem] * (len(flats) + 1),
        out_specs=[vmem] * (len(shapes) + 1),
        out_shape=[jax.ShapeDtypeStruct(shape, BF) for shape in shapes] + [jax.ShapeDtypeStruct((8, 128), F32)],
        name="pack_shards",
    )(*[flat.reshape(-1, 128) for flat in flats], vectors.reshape(1, 128))


def unpack_kernel(places, kinds, *refs):
    packed, flats = refs[: kinds + 1], refs[kinds + 1 :]
    for flat, (target, offset, tiles) in zip(flats, places):
        source = packed[target]
        rows = source.shape[0]
        for j in range(tiles):
            flat[pl.ds(j, rows, stride=tiles), :] = source[:, offset + j * 128 : offset + (j + 1) * 128]
    flats[-1][...] = packed[-1][0:1]


def unpack(packed, places):
    vmem = pl.BlockSpec(memory_space=pltpu.VMEM)
    sizes = [packed[target].shape[0] * tiles for target, _, tiles in places] + [1]
    flats = pl.pallas_call(
        partial(unpack_kernel, places, len(packed) - 1),
        in_specs=[vmem] * len(packed),
        out_specs=[vmem] * len(sizes),
        out_shape=[jax.ShapeDtypeStruct((size, 128), F32) for size in sizes],
        name="unpack_sums",
    )(*packed)
    return [flat.reshape(-1) for flat in flats]


def rms_factor(values, eps):
    return lax.rsqrt(jnp.mean(values * values, axis=-1, keepdims=True) + eps)


def rms_back(grad, values, factor, gain):
    scaled = values * factor
    dscaled = grad * gain
    dvalues = factor * (dscaled - scaled * jnp.mean(dscaled * scaled, axis=-1, keepdims=True))
    return dvalues, jnp.sum(grad * scaled, axis=0)


def by_kernel(sizes, ring_size, fsdp_size):
    return ring_size == 4 and fsdp_size % 4 == 0 and all(size % 8 == 0 for size in sizes)


def gather_plain(shards):
    return [lax.all_gather(piece, AXES, axis=0) for piece in shards]


def scatter_plain(grads):
    return [lax.psum_scatter(piece.astype(F32), AXES, scatter_dimension=0) for piece in grads]


def per_device(
    hidden_in,
    w_query,
    w_latent,
    w_key_up,
    w_value_up,
    w_decay,
    w_outgate,
    w_out,
    w_gate,
    w_up,
    w_down,
    vectors,
    seg_ids,
    pad_mask,
    cotangent,
    *,
    ring_size,
    fsdp_size,
):
    count = ring_size * fsdp_size
    per_group = WIDTH // GROUPS
    latents = GROUPS * LATENT
    rows_d, rows_kv, rows_ff = D // count, latents // count, FF // count
    rows_all = (rows_d, rows_kv, rows_ff)
    vec_size = (2 * D + 2 * WIDTH) // count

    own = by_kernel(rows_all, ring_size, fsdp_size) and vec_size == 128
    flat_weights = (w_query, w_latent, w_key_up, w_value_up, w_decay, w_outgate, w_out, w_gate, w_up, w_down)
    wide, half_kv, ff = WIDTH // 128, per_group // 128, FF // 128
    places = (
        (0, 0, wide),
        (0, 3 * WIDTH, latents // 128),
        (1, 0, half_kv),
        (1, per_group, half_kv),
        (0, WIDTH, wide),
        (0, 2 * WIDTH, wide),
        (2, 0, D // 128),
        (3, 0, ff),
        (3, FF, ff),
        (4, 0, D // 128),
    )
    if own:
        shapes = (
            (rows_d, 3 * WIDTH + latents),
            (rows_kv, 2 * per_group),
            (rows_d, D),
            (rows_d, 2 * FF),
            (rows_ff, D),
        )
        in_shard, kv_shard, out_shard, ff_shard, down_shard, vec_shard = pack(flat_weights, vectors, places, shapes)
    else:

        def rows_of(piece, rows):
            return piece.astype(BF).reshape(rows, -1)

        in_shard = jnp.concatenate(
            [rows_of(piece, rows_d) for piece in (w_query, w_decay, w_outgate, w_latent)], axis=1
        )
        kv_shard = jnp.concatenate([rows_of(w_key_up, rows_kv), rows_of(w_value_up, rows_kv)], axis=1)
        out_shard = rows_of(w_out, rows_d)
        ff_shard = jnp.concatenate([rows_of(w_gate, rows_d), rows_of(w_up, rows_d)], axis=1)
        down_shard = rows_of(w_down, rows_ff)
        vec_shard = jnp.broadcast_to(lax.reduce_precision(vectors, 8, 7).reshape(1, -1), (8, vec_size))
    comm = (ring_size, fsdp_size // 2)
    early, late = (in_shard, kv_shard, vec_shard), (out_shard, ff_shard, down_shard)
    w_in, w_kv, vecs = gather(early, *comm, 0) if own else gather_plain(early)
    w_in = w_in.reshape(D, 3 * WIDTH + latents)
    w_kv = w_kv.reshape(GROUPS, LATENT, 2 * per_group)
    vecs = vecs[:, 0].reshape(-1)
    gain_in, gain_mid = vecs[:D], vecs[D : 2 * D]
    decay_bias, out_gain = vecs[2 * D : 2 * D + WIDTH], vecs[2 * D + WIDTH :]

    segs = seg_ids.astype(F32).reshape(CHUNKS, 1, SPAN)
    pads = pad_mask.astype(F32).reshape(CHUNKS, 1, SPAN)
    pad = pad_mask.astype(F32).reshape(LEN, 1)

    inputs = hidden_in.astype(F32)
    factor_in = rms_factor(inputs, 1e-5)
    normed = (inputs * factor_in * gain_in).astype(BF)
    latent = mm(normed, w_in[:, 3 * WIDTH :]).astype(BF)
    bias_row, gain_row = decay_bias.reshape(1, WIDTH), out_gain.reshape(1, WIDTH)
    query, keys, values, decay_in, gate_in, mixed, heads, states, *rest = mixer_fwd(
        normed, latent, w_in, w_kv, bias_row, gain_row, segs, pads, late if own else (), comm + (0, 2) if own else None
    )
    w_output, w_ff, w_dn = rest if own else gather_plain(late)
    w_output = w_output.reshape(WIDTH, D)
    w_ff = w_ff.reshape(D, 2 * FF)
    w_dn = w_dn.reshape(FF, D)
    middle = inputs + mm(mixed, w_output)
    factor_mid = rms_factor(middle, 1e-5)
    normed_mid = (middle * factor_mid * gain_mid).astype(BF)
    gate_val = mm(normed_mid, w_ff[:, :FF])
    up_val = mm(normed_mid, w_ff[:, FF:])
    sig = jax.nn.sigmoid(gate_val)
    silu = gate_val * sig
    hidden = (silu * up_val).astype(BF)
    block_out = (middle + mm(hidden, w_dn)).astype(BF)

    d_outf = cotangent.astype(F32) * pad
    d_ffn = d_outf.astype(BF)
    grad_down = mm_tn(hidden, d_ffn)
    d_hidden = mm_nt(d_ffn, w_dn)
    d_gate = (d_hidden * up_val * (sig * (1.0 + gate_val * (1.0 - sig)))).astype(BF)
    d_up = (d_hidden * silu).astype(BF)
    d_both = jnp.concatenate([d_gate, d_up], axis=1)
    grad_ff = mm_tn(normed_mid, d_both)
    d_normed_mid = mm_nt(d_both, w_ff)
    d_middle, d_gain_mid = rms_back(d_normed_mid, middle, factor_mid, gain_mid)
    d_middle = d_middle + d_outf
    d_branch = d_middle.astype(BF)
    grad_out = mm_tn(mixed, d_branch)

    sent = (grad_ff.astype(BF).reshape(count, rows_d, -1), grad_down.astype(BF).reshape(count, rows_ff, -1))
    saved = (query, keys, values, decay_in, gate_in, gain_row, segs, pads, heads, states)
    d_query, d_keys, d_values, d_decay, d_gatein, d_bias, d_out_gain, *rest = mixer_bwd(
        saved, d_branch, w_output, sent if own else (), comm + (0, 3) if own else None
    )
    own_ff, own_down = rest if own else scatter_plain(sent)
    grad_kv, d_latent = [], []
    for g in range(GROUPS):
        d_kv = jnp.concatenate(
            [part[:, g * per_group : (g + 1) * per_group] for part in (d_keys, d_values)], axis=1
        )
        grad_kv.append(mm_tn(latent[:, g * LATENT : (g + 1) * LATENT], d_kv))
        d_latent.append(mm_nt(d_kv, w_kv[g]))
    grad_kv = jnp.concatenate(grad_kv, axis=0)
    d_latent = jnp.concatenate(d_latent, axis=1).astype(BF)
    d_in = jnp.concatenate([d_query, d_decay, d_gatein, d_latent], axis=1)
    grad_in = mm_tn(normed, d_in)
    d_normed = mm_nt(d_in, w_in)
    d_inputs, d_gain_in = rms_back(d_normed, inputs, factor_in, gain_in)
    grad_input = d_middle + d_inputs
    grad_vec = jnp.concatenate([d_gain_in, d_gain_mid, d_bias.reshape(-1), d_out_gain.reshape(-1)])

    grad_vec = jnp.broadcast_to(grad_vec.reshape(count, 1, vec_size), (count, 8, vec_size))
    sent = (
        grad_in.astype(BF).reshape(count, rows_d, -1),
        grad_kv.astype(BF).reshape(count, rows_kv, -1),
        grad_out.astype(BF).reshape(count, rows_d, -1),
        grad_vec,
    )
    own_in, own_kv, own_out, own_vec = scatter(sent, *comm, 1) if own else scatter_plain(sent)
    if own:
        return (block_out, grad_input, *unpack((own_in, own_kv, own_out, own_ff, own_down, own_vec), places))
    return (
        block_out,
        grad_input,
        own_in[:, :WIDTH].reshape(-1),
        own_in[:, 3 * WIDTH :].reshape(-1),
        own_kv[:, :per_group].reshape(-1),
        own_kv[:, per_group:].reshape(-1),
        own_in[:, WIDTH : 2 * WIDTH].reshape(-1),
        own_in[:, 2 * WIDTH : 3 * WIDTH].reshape(-1),
        own_out.reshape(-1),
        own_ff[:, :FF].reshape(-1),
        own_ff[:, FF:].reshape(-1),
        own_down.reshape(-1),
        own_vec[0],
    )


def solution(mesh):
    sizes = {"ring_size": mesh.shape["dp"], "fsdp_size": mesh.shape["fsdp"]}
    rows, flat = P(AXES, None), P(AXES)
    in_specs = (rows,) + (flat,) * 13 + (rows,)
    out_specs = (rows, rows) + (flat,) * 11
    return jax.shard_map(
        partial(per_device, **sizes), mesh=mesh, in_specs=in_specs, out_specs=out_specs, check_vma=False
    )
```

```python
from functools import partial

import jax
import jax.numpy as jnp
from jax import lax
from jax.experimental import pallas as pl
from jax.experimental.pallas import tpu as pltpu
from jax.sharding import PartitionSpec as P

D = 1024
HEADS = 16
HEAD_DIM = 64
GROUPS = 2
LATENT = 256
FF = 2816
LEN = 1024
WIDTH = HEADS * HEAD_DIM
SPAN = 128
LANES = 256
PACK = LANES // HEAD_DIM
BANDS = WIDTH // LANES
CHUNKS = LEN // SPAN
LIMIT = 85.0
AXES = ("dp", "fsdp")
BF = jnp.bfloat16
F32 = jnp.float32
MESH = pl.DeviceIdType.MESH


def mm(left, right):
    return lax.dot_general(left, right, (((1,), (0,)), ((), ())), preferred_element_type=F32)


def mm_nt(left, right):
    return lax.dot_general(left, right, (((1,), (1,)), ((), ())), preferred_element_type=F32)


def mm_tn(left, right):
    return lax.dot_general(left, right, (((0,), (0,)), ((), ())), preferred_element_type=F32)


def halves(value):
    high = value.astype(BF)
    return high, (value - high.astype(F32)).astype(BF)


def exact_left(ones, value):
    high, rest = halves(value)
    return mm(ones, high) + mm(ones, rest)


def exact_right(value, ones):
    high, rest = halves(value)
    return mm(high, ones) + mm(rest, ones)


def head_masks():
    lane = lax.broadcasted_iota(jnp.int32, (1, LANES), 1) // HEAD_DIM
    return [lane == head for head in range(PACK)]


def stacked(value, masks):
    zero = jnp.zeros_like(value)
    return jnp.concatenate([jnp.where(mask, value, zero) for mask in masks], axis=0)


def side_by_side(value):
    return jnp.concatenate([value[h * SPAN : (h + 1) * SPAN] for h in range(PACK)], axis=1)


def same_head():
    row = lax.broadcasted_iota(jnp.int32, (LANES, LANES), 0) // HEAD_DIM
    col = lax.broadcasted_iota(jnp.int32, (LANES, LANES), 1) // HEAD_DIM
    return row == col


def triangle(lower):
    row = lax.broadcasted_iota(jnp.int32, (SPAN, SPAN), 0)
    col = lax.broadcasted_iota(jnp.int32, (SPAN, SPAN), 1)
    return (row >= col) if lower else (row <= col)


def decays(decay, pad, lower_ones):
    small = jnp.exp(-jnp.abs(decay))
    log_sig = jnp.minimum(decay, 0.0) - jnp.log(1.0 + small)
    total = exact_left(lower_ones, log_sig * (pad * (1.0 / 16.0)))
    ending = total[SPAN - 1 : SPAN]
    middle = 0.5 * ending
    centred = total - middle
    up = jnp.exp(jnp.minimum(centred, LIMIT))
    down = jnp.exp(jnp.minimum(-centred, LIMIT))
    half = jnp.exp(middle)
    return up, down, half, small


def flags(seg_ref, pad_ref, index):
    seg_row = seg_ref[index]
    seg_square = jnp.transpose(jnp.broadcast_to(seg_row, (SPAN, SPAN)))
    pad = jnp.transpose(jnp.broadcast_to(pad_ref[index], (SPAN, SPAN)))[:, 0:1]
    seg_col, ending = seg_square[:, 0:1], seg_row[:, SPAN - 1 :]
    before = seg_ref[jnp.maximum(index - 1, 0)][:, SPAN - 1 :]
    fresh = (seg_col == before).astype(F32)
    to_end = (seg_col == ending).astype(F32)
    keep = (ending == before).astype(F32)
    allowed = (seg_square == seg_row) & triangle(True)
    return fresh, to_end, pad, allowed, keep


def mixer_fwd_kernel(comm, *refs):
    kinds = comm[2] if comm else 0
    normed_ref, latent_ref, wq_ref, wd_ref, wg_ref, wk_ref, wv_ref, bias_ref, gain_ref, seg_ref, pad_ref = refs[:11]
    shards, refs = refs[11 : 11 + kinds], refs[11 + kinds :]
    q_ref, k_ref, v_ref, decay_ref, gate_ref, mixed_ref, heads_ref, states_ref = refs[:8]
    gathered, state, sems = refs[8 : 8 + kinds], refs[8 + kinds], refs[9 + kinds :]
    band = pl.program_id(0)
    job = Gather(comm[0], comm[1], shards, gathered, sems) if comm else None
    stages = job.stages() if comm else []
    ticks = BANDS * (CHUNKS + 1)
    if comm:
        pl.when(band == 0)(job.begin)
    masks = head_masks()
    diag = same_head()
    diag_ones = diag.astype(F32).astype(BF)
    lower_ones = triangle(True).astype(F32).astype(BF)
    state[...] = jnp.zeros_like(state)
    gain = gain_ref[...]
    q_ref[...] = mm(normed_ref[...], wq_ref[...])
    decay_ref[...] = mm(normed_ref[...], wd_ref[...]) + bias_ref[...]
    gate_ref[...] = mm(normed_ref[...], wg_ref[...])
    k_ref[...] = mm(latent_ref[...], wk_ref[0])
    v_ref[...] = mm(latent_ref[...], wv_ref[0])

    def chunk(index, carry):
        spread(stages, band * (CHUNKS + 1) + index, ticks)
        rows = pl.ds(pl.multiple_of(index * SPAN, SPAN), SPAN)
        fresh, to_end, pad, allowed, keep = flags(seg_ref, pad_ref, index)
        up, down, half, _ = decays(decay_ref[rows, :], pad, lower_ones)
        query = q_ref[rows, :] * (HEAD_DIM**-0.5) * up
        key = k_ref[rows, :] * pad * down
        value = v_ref[rows, :].astype(BF)
        query_low, key_low = query.astype(BF), key.astype(BF)
        scores = mm_nt(stacked(query_low, masks), key_low)
        scores = scores.reshape(PACK, SPAN, SPAN)
        scores = jnp.where(allowed[None], scores, 0.0).astype(BF).reshape(PACK * SPAN, SPAN)
        old = state[...]
        old_low = old.astype(BF)
        states_ref[0, index] = old_low
        heads = mm(side_by_side(scores), stacked(value, masks))
        heads += mm_nt((query * (half * fresh)).astype(BF), old_low)
        tail = (key * (half * to_end)).astype(BF)
        state[...] = old * (half * half * keep) + jnp.where(diag, mm_tn(value, tail), 0.0)
        heads_ref[rows, :] = heads
        scale = lax.rsqrt(exact_right(heads * heads, diag_ones) * (1.0 / HEAD_DIM) + 1e-2)
        gate = gate_ref[rows, :]
        silu = gate / (1.0 + jnp.exp(-gate))
        mixed_ref[rows, :] = (heads * scale * gain * silu).astype(BF)
        return carry

    lax.fori_loop(0, CHUNKS, chunk, 0)
    spread(stages, band * (CHUNKS + 1) + CHUNKS, ticks)
    if comm:
        pl.when(band == BANDS - 1)(job.finish)


def mixer_bwd_kernel(comm, *refs):
    kinds = comm[2] if comm else 0
    q_ref, k_ref, v_ref, decay_ref, gate_ref, gain_ref, seg_ref, pad_ref, heads_ref, states_ref = refs[:10]
    dbranch_ref, wo_ref = refs[10:12]
    grads, refs = refs[12 : 12 + kinds], refs[12 + kinds :]
    dq_ref, dk_ref, dv_ref, ddecay_ref, dgate_ref, dbias_ref, dgain_ref = refs[:7]
    sums, state, dmix_ref, scratch = refs[7 : 7 + kinds], refs[7 + kinds], refs[8 + kinds], refs[9 + kinds :]
    band = pl.program_id(0)
    job = scatter_of(comm[0], comm[1], grads, sums, scratch) if comm else None
    stages = job.stages() if comm else []
    ticks = BANDS * (CHUNKS + 1)
    if comm:
        pl.when(band == 0)(job.begin)
    dmix_ref[...] = mm_nt(dbranch_ref[...], wo_ref[...])
    masks = head_masks()
    diag = same_head()
    diag_ones = diag.astype(F32).astype(BF)
    lower_ones = triangle(True).astype(F32).astype(BF)
    upper_ones = triangle(False).astype(F32).astype(BF)
    state[...] = jnp.zeros_like(state)
    dbias_ref[...] = jnp.zeros_like(dbias_ref)
    dgain_ref[...] = jnp.zeros_like(dgain_ref)
    gain = gain_ref[...]

    def chunk(step, carry):
        spread(stages, band * (CHUNKS + 1) + step, ticks)
        index = CHUNKS - 1 - step
        rows = pl.ds(pl.multiple_of(index * SPAN, SPAN), SPAN)
        fresh, to_end, pad, allowed, keep = flags(seg_ref, pad_ref, index)
        heads = heads_ref[rows, :]
        scale = lax.rsqrt(exact_right(heads * heads, diag_ones) * (1.0 / HEAD_DIM) + 1e-2)
        normed = heads * scale
        gate = gate_ref[rows, :]
        sig = 1.0 / (1.0 + jnp.exp(-gate))
        silu = gate * sig
        dmix = dmix_ref[rows, :]
        both = dmix * normed
        dgain_ref[...] += jnp.sum(both * silu, axis=0, keepdims=True)
        dgate_ref[rows, :] = (both * gain * (sig * (1.0 + gate * (1.0 - sig)))).astype(BF)
        dnormed = dmix * gain * silu
        mean = exact_right(dnormed * normed, diag_ones) * (1.0 / HEAD_DIM)
        dheads = (scale * (dnormed - normed * mean)).astype(BF)
        decay = decay_ref[rows, :]
        up, down, half, small = decays(decay, pad, lower_ones)
        unit = HEAD_DIM**-0.5
        query = q_ref[rows, :] * unit * up
        key = k_ref[rows, :] * pad * down
        value = v_ref[rows, :].astype(BF)
        query_low, key_low = query.astype(BF), key.astype(BF)
        enter = half * fresh
        leave = half * to_end
        query_in = (query * enter).astype(BF)
        tail = (key * leave).astype(BF)
        query_stack = stacked(query_low, masks)
        dheads_stack = stacked(dheads, masks)
        scores = mm_nt(query_stack, key_low).reshape(PACK, SPAN, SPAN)
        scores = jnp.where(allowed[None], scores, 0.0).astype(BF).reshape(PACK * SPAN, SPAN)
        dscores = mm_nt(dheads_stack, value).reshape(PACK, SPAN, SPAN)
        dscores = jnp.where(allowed[None], dscores, 0.0).astype(BF).reshape(PACK * SPAN, SPAN)
        dstate = state[...]
        dstate_low = dstate.astype(BF)
        old = states_ref[0, index]
        dvalue = mm_tn(scores, dheads_stack) + mm_nt(tail, dstate_low)
        dv_ref[rows, :] = dvalue.astype(BF)
        dquery = mm(side_by_side(dscores), stacked(key_low, masks))
        dkey = mm_tn(dscores, query_stack)
        dquery_in = mm(dheads, old)
        dtail = mm(value, dstate_low)
        whole = half * half * keep
        state[...] = dstate * whole + jnp.where(diag, mm_tn(dheads, query_in), 0.0)
        dq_ref[rows, :] = ((dquery + dquery_in * enter) * (up * unit)).astype(BF)
        dk_ref[rows, :] = ((dkey + dtail * leave) * (down * pad)).astype(BF)
        from_tail = dtail * tail.astype(F32)
        dtotal = (
            dquery * query_low.astype(F32)
            - dkey * key_low.astype(F32)
            + dquery_in * query_in.astype(F32)
            - from_tail
        )
        ends = jnp.sum(from_tail, axis=0, keepdims=True)
        ends += whole * jnp.sum(dstate * old.astype(F32), axis=0, keepdims=True)
        dlog = exact_left(upper_ones, dtotal) + ends
        other = jnp.where(decay >= 0, small, 1.0) / (1.0 + small)
        ddecay = dlog * (pad * (1.0 / 16.0)) * other
        dbias_ref[...] += jnp.sum(ddecay, axis=0, keepdims=True)
        ddecay_ref[rows, :] = ddecay.astype(BF)
        return carry

    lax.fori_loop(0, CHUNKS, chunk, 0)
    spread(stages, band * (CHUNKS + 1) + CHUNKS, ticks)
    if comm:
        pl.when(band == BANDS - 1)(job.finish)


def band_specs():
    tokens = pl.BlockSpec((LEN, LANES), lambda band: (0, band))
    vector = pl.BlockSpec((1, LANES), lambda band: (0, band))
    segs = pl.BlockSpec((CHUNKS, 1, SPAN), lambda band: (0, 0, 0))
    states = pl.BlockSpec((1, CHUNKS, LANES, LANES), lambda band: (band, 0, 0, 0))
    return tokens, vector, segs, states


def fixed(shape):
    return pl.BlockSpec(shape, lambda band: (0,) * len(shape), pipeline_mode=pl.Buffered(1))


def mixer_fwd(normed, latent, w_in, w_kv, bias, gain, segs, pads, shards, comm):
    tokens, vector, segs_spec, states = band_specs()
    kinds = len(shards)
    half_bands = BANDS // GROUPS
    in_specs = [fixed((LEN, D)), pl.BlockSpec((LEN, LATENT), lambda band: (0, band // half_bands))]
    for part in range(3):
        in_specs.append(pl.BlockSpec((D, LANES), lambda band, part=part: (0, part * BANDS + band)))
    for part in range(2):
        in_specs.append(
            pl.BlockSpec(
                (1, LATENT, LANES),
                lambda band, part=part: (band // half_bands, 0, part * half_bands + band % half_bands),
            )
        )
    in_specs += [vector, vector, segs_spec, segs_spec]
    wide = jax.ShapeDtypeStruct((LEN, WIDTH), F32)
    out_shape = [wide] * 5 + [
        jax.ShapeDtypeStruct((LEN, WIDTH), BF),
        wide,
        jax.ShapeDtypeStruct((BANDS, CHUNKS, LANES, LANES), BF),
    ]
    scratch = [pltpu.VMEM((LANES, LANES), F32)]
    params = {}
    if comm:
        count = 2 * comm[0] * comm[1]
        in_specs += [fixed(shard.shape) for shard in shards]
        out_shape += [jax.ShapeDtypeStruct((count,) + shard.shape, shard.dtype) for shard in shards]
        scratch += gather_scratch(kinds, comm[1])
        params = {"collective_id": comm[3], "has_side_effects": True}
        comm = comm[:2] + (kinds,)
    return pl.pallas_call(
        partial(mixer_fwd_kernel, comm),
        grid=(BANDS,),
        in_specs=in_specs,
        out_specs=[tokens] * 7 + [states] + [pl.BlockSpec(memory_space=pl.ANY)] * kinds,
        out_shape=out_shape,
        scratch_shapes=scratch,
        compiler_params=pltpu.CompilerParams(vmem_limit_bytes=52 << 20, **params),
        name="mixer_fwd",
    )(normed, latent, w_in, w_in, w_in, w_kv, w_kv, bias, gain, segs, pads, *shards)


def mixer_bwd(saved, d_branch, w_output, grads, comm):
    tokens, vector, segs_spec, states = band_specs()
    kinds = len(grads)
    low = jax.ShapeDtypeStruct((LEN, WIDTH), BF)
    sums = jax.ShapeDtypeStruct((1, WIDTH), F32)
    in_specs = [tokens] * 5 + [vector, segs_spec, segs_spec, tokens, states]
    in_specs += [fixed((LEN, D)), pl.BlockSpec((LANES, D), lambda band: (band, 0))]
    out_specs, out_shape = [tokens] * 5 + [vector, vector], [low] * 5 + [sums, sums]
    scratch = [pltpu.VMEM((LANES, LANES), F32), pltpu.VMEM((LEN, LANES), F32)]
    params = {}
    if comm:
        in_specs += [pl.BlockSpec(memory_space=pl.ANY)] * kinds
        out_specs += [fixed(grad.shape[1:]) for grad in grads]
        out_shape += [jax.ShapeDtypeStruct(grad.shape[1:], F32) for grad in grads]
        scratch += scatter_scratch(grads, comm[0], comm[1])
        params = {"collective_id": comm[3], "has_side_effects": True}
        comm = comm[:2] + (kinds,)
    return pl.pallas_call(
        partial(mixer_bwd_kernel, comm),
        grid=(BANDS,),
        in_specs=in_specs,
        out_specs=out_specs,
        out_shape=out_shape,
        scratch_shapes=scratch,
        compiler_params=pltpu.CompilerParams(vmem_limit_bytes=63 << 20, **params),
        name="mixer_bwd",
    )(*saved, d_branch, w_output, *grads)


class Place:
    def __init__(self, ring_size, line_size):
        self.ring_size, self.line_size = ring_size, line_size
        self.d, f = lax.axis_index("dp"), lax.axis_index("fsdp")
        self.z, self.core = f // 2, f % 2
        self.pos = self.at_ring(self.d)

    def at_ring(self, index):
        if self.ring_size != 4:
            return index
        return index + (index // 2) * (1 - 2 * (index % 2))

    def ring(self, offset):
        return self.at_ring((self.pos + offset + self.ring_size) % self.ring_size)

    def far(self, i):
        n = self.line_size
        low = self.z < n // 2
        near = jnp.where(low, self.z, n - 1 - self.z)
        if i == n - 1:
            return self.z
        line = n - 1 - i - jnp.where(n - 1 - i <= near, 1, 0)
        return jnp.where(low, line, n - 1 - line)

    def device(self, d, z, core):
        return (d, 2 * z + core)

    def slot(self, d, z, core):
        return d * (2 * self.line_size) + 2 * z + core


def greet(place, peers):
    barrier = pltpu.get_barrier_semaphore()
    for peer in peers:
        pl.semaphore_signal(barrier, inc=1, device_id=peer, device_id_type=MESH)
    pl.semaphore_wait(barrier, len(peers))


def peers_of(place):
    me = place
    peers = [me.device(me.d, me.z, 1 - me.core)]
    peers += [me.device(me.ring(step), me.z, me.core) for step in (1, -1)]
    peers += [me.device(me.d, me.far(i), me.core) for i in range(me.line_size - 1)]
    return peers


def send(src, dst, send_sem, recv_sem, device):
    return pltpu.make_async_remote_copy(
        src_ref=src, dst_ref=dst, send_sem=send_sem, recv_sem=recv_sem, device_id=device, device_id_type=MESH
    )


class Scatter:
    def __init__(self, ring_size, line_size, grads, outs, accs, parts, hops, tails, sems):
        self.ring_size, self.line_size = ring_size, line_size
        self.grads, self.outs = grads, outs
        self.accs, self.parts, self.hops, self.tails = accs, parts, hops, tails
        self.load_sem, self.psend, self.precv, self.hsend, self.hrecv, self.tsend, self.trecv = sems
        self.me = Place(ring_size, line_size)
        self.order = [self.me.far(i) for i in range(line_size)]
        self.every = range(len(grads))
        self.waves = [
            (step, wave - step)
            for wave in range(1, ring_size + line_size)
            for step in range(1, ring_size + 1)
            if 0 <= wave - step < line_size
        ]

    def way(self, a, i):
        return 1 if (a + i) % 2 == 0 else -1

    def dest(self, a, step, i, core):
        me = self.me
        return self.grads[a].at[me.slot(me.ring(-step * self.way(a, i)), self.order[i], core)]

    def load(self, a, step, i):
        return pltpu.make_async_copy(
            self.dest(a, step, i, self.me.core), self.accs[a].at[step - 1, i], self.load_sem.at[a, step - 1, i]
        )

    def to_pair(self, a, step, i):
        me = self.me
        return send(
            self.dest(a, step, i, 1 - me.core),
            self.parts[a].at[step - 1, i],
            self.psend.at[a, step - 1, i],
            self.precv.at[a, step - 1, i],
            me.device(me.d, me.z, 1 - me.core),
        )

    def to_ring(self, a, step, i):
        me = self.me
        return send(
            self.accs[a].at[step - 1, i],
            self.hops[a].at[step - 1, i],
            self.hsend.at[a, step - 1, i],
            self.hrecv.at[a, step - 1, i],
            me.device(me.ring(self.way(a, i)), me.z, me.core),
        )

    def to_line(self, a, i):
        me = self.me
        return send(
            self.accs[a].at[self.ring_size - 1, i],
            self.tails[a].at[me.z],
            self.tsend.at[a, i],
            self.trecv.at[a, me.z],
            me.device(me.d, self.order[i], me.core),
        )

    def from_line(self, a, i):
        me = self.me
        here = self.tails[a].at[self.order[i]]
        return send(
            here, here, self.tsend.at[a, i], self.trecv.at[a, self.order[i]], me.device(me.d, self.order[i], me.core)
        )

    def blocks(self, a):
        width = self.grads[a].shape[-1]
        block = 512 if width % 512 == 0 else width
        return width // block, block

    def add_up(self, a, step, i):
        number, block = self.blocks(a)
        acc, final = self.accs[a], step == self.ring_size and i == self.line_size - 1

        def body(j, carry):
            cols = pl.ds(pl.multiple_of(j * block, block), block)
            total = acc[step - 1, i, :, cols].astype(F32) + self.parts[a][step - 1, i, :, cols].astype(F32)
            if step > 1:
                total += self.hops[a][step - 2, i, :, cols].astype(F32)
            if final:
                self.outs[a][:, cols] = total
            else:
                acc[step - 1, i, :, cols] = total.astype(acc.dtype)
            return carry

        lax.fori_loop(0, number, body, 0)

    def begin(self):
        for step, i in self.waves:
            for a in self.every:
                self.load(a, step, i).start()
        greet(self.me, peers_of(self.me))
        for step, i in self.waves:
            for a in self.every:
                self.to_pair(a, step, i).start()

    def entry(self, step, i):
        for a in self.every:
            self.load(a, step, i).wait()
            self.to_pair(a, step, i).wait_recv()
            if step > 1:
                self.to_ring(a, step - 1, i).wait_recv()
            self.add_up(a, step, i)
            if step < self.ring_size:
                self.to_ring(a, step, i).start()
            elif i < self.line_size - 1:
                self.to_line(a, i).start()

    def stages(self):
        return [partial(self.entry, step, i) for step, i in self.waves]

    def finish(self):
        last = self.line_size - 1
        for a in self.every:
            for i in range(last):
                self.from_line(a, i).wait_recv()
            number, block = self.blocks(a)

            def body(j, carry, a=a, block=block):
                cols = pl.ds(pl.multiple_of(j * block, block), block)
                total = self.outs[a][:, cols]
                for i in range(last):
                    total += self.tails[a][self.order[i], :, cols].astype(F32)
                self.outs[a][:, cols] = total
                return carry

            lax.fori_loop(0, number, body, 0)
        for step, i in self.waves:
            for a in self.every:
                self.to_pair(a, step, i).wait_send()
                if step < self.ring_size:
                    self.to_ring(a, step, i).wait_send()
                elif i < last:
                    self.to_line(a, i).wait_send()


def scatter_scratch(grads, ring_size, line_size):
    kinds = len(grads)
    sems = pltpu.SemaphoreType.DMA
    scratch = []
    for lead in ((ring_size, line_size), (ring_size, line_size), (ring_size - 1, line_size), (line_size,)):
        scratch += [pltpu.VMEM(lead + grad.shape[1:], grad.dtype) for grad in grads]
    return scratch + [sems((kinds, ring_size, line_size))] * 5 + [sems((kinds, line_size))] * 2


def scatter_of(ring_size, line_size, grads, outs, scratch):
    kinds = len(grads)
    rooms = [scratch[k * kinds : (k + 1) * kinds] for k in range(4)]
    return Scatter(ring_size, line_size, grads, outs, *rooms, scratch[4 * kinds :])


def scatter_kernel(ring_size, line_size, kinds, *refs):
    job = scatter_of(ring_size, line_size, refs[:kinds], refs[kinds : 2 * kinds], refs[2 * kinds :])
    job.begin()
    for stage in job.stages():
        stage()
    job.finish()


def scatter(grads, ring_size, line_size, ident):
    kinds = len(grads)
    return pl.pallas_call(
        partial(scatter_kernel, ring_size, line_size, kinds),
        in_specs=[pl.BlockSpec(memory_space=pl.ANY)] * kinds,
        out_specs=[pl.BlockSpec(memory_space=pltpu.VMEM)] * kinds,
        out_shape=[jax.ShapeDtypeStruct(grad.shape[1:], F32) for grad in grads],
        scratch_shapes=scatter_scratch(grads, ring_size, line_size),
        compiler_params=pltpu.CompilerParams(
            collective_id=ident, has_side_effects=True, vmem_limit_bytes=60 << 20
        ),
        name="scatter_sums",
    )(*grads)


class Gather:
    def __init__(self, ring_size, line_size, shards, outs, sems):
        self.line_size = line_size
        self.shards, self.outs = shards, outs
        (
            self.own_sem,
            self.zsend,
            self.zrecv,
            self.hsend,
            self.hrecv,
            self.osend,
            self.orecv,
            self.psend,
            self.precv,
            self.qsend,
            self.qrecv,
        ) = sems
        self.me = Place(ring_size, line_size)
        self.order = [self.me.far(line_size - 1 - i) for i in range(line_size)]
        self.pair = self.me.device(self.me.d, self.me.z, 1 - self.me.core)
        self.mine = self.me.slot(self.me.d, self.me.z, self.me.core)
        self.every = range(len(shards))

    def half(self, a, way):
        width = self.shards[a].shape[-1]
        if width % 256:
            return pl.ds(0, width)
        return pl.ds(0 if way == 0 else width // 2, width // 2)

    def halved(self, a, way):
        return self.shards[a].shape[-1] % 256 == 0 or way == 0

    def beside(self, way):
        return self.me.device(self.me.ring(1 - 2 * way), self.me.z, self.me.core)

    def spot(self, a, offset, i, core):
        return self.outs[a].at[self.me.slot(self.me.ring(offset), self.order[i], core)]

    def own(self, a):
        return pltpu.make_async_copy(self.shards[a], self.outs[a].at[self.mine], self.own_sem.at[a])

    def along(self, a, i, up):
        me = self.me
        here = self.spot(a, 0, i, me.core)
        return send(
            self.shards[a] if i == 0 else here,
            here,
            self.zsend.at[a, up, i],
            self.zrecv.at[a, self.order[i]],
            me.device(me.d, me.z + 2 * up - 1, me.core),
        )

    def from_line(self, a, i):
        me = self.me
        here = self.spot(a, 0, i, me.core)
        return send(
            here, here, self.zsend.at[a, 0, i], self.zrecv.at[a, self.order[i]], me.device(me.d, self.order[i], me.core)
        )

    def pass_on(self, act, i):
        me, last = self.me, self.line_size - 1
        upward, downward = me.z < last, me.z > 0
        if i:
            upward &= self.order[i] < me.z
            downward &= self.order[i] > me.z
        for up, wanted in ((1, upward), (0, downward)):

            @pl.when(wanted)
            def _(up=up):
                for a in self.every:
                    act(self.along(a, i, up))

    def to_ring(self, a, i, way):
        here = self.spot(a, 0, i, self.me.core)
        src = self.shards[a] if i == 0 else here
        return send(src, here, self.hsend.at[a, way, i], self.hrecv.at[a, way, i], self.beside(way))

    def from_ring(self, a, i, way):
        here = self.spot(a, 2 * way - 1, i, self.me.core)
        return send(here, here, self.hsend.at[a, way, i], self.hrecv.at[a, way, i], self.beside(1 - way))

    def onward(self, a, i, way):
        here = self.spot(a, 2 * way - 1, i, self.me.core).at[:, self.half(a, way)]
        return send(here, here, self.osend.at[a, way, i], self.orecv.at[a, way, i], self.beside(way))

    def from_onward(self, a, i, way):
        here = self.spot(a, 2, i, self.me.core).at[:, self.half(a, way)]
        return send(here, here, self.osend.at[a, way, i], self.orecv.at[a, way, i], self.beside(1 - way))

    def to_pair(self, a, i, lane, core):
        here = self.spot(a, (0, -1, 1)[lane], i, core)
        src = self.shards[a] if (lane == 0 and i == 0 and core is self.me.core) else here
        return send(src, here, self.psend.at[a, lane, i], self.precv.at[a, lane, i], self.pair)

    def to_pair_half(self, a, i, way, core):
        here = self.spot(a, 2, i, core).at[:, self.half(a, way)]
        return send(here, here, self.qsend.at[a, way, i], self.qrecv.at[a, way, i], self.pair)

    def begin(self):
        for a in self.every:
            self.own(a).start()
        greet(self.me, peers_of(self.me))
        for a in self.every:
            for way in range(2):
                self.to_ring(a, 0, way).start()
        self.pass_on(lambda copy: copy.start(), 0)
        for a in self.every:
            self.to_pair(a, 0, 0, self.me.core).start()

    def line_stage(self, i):
        for a in self.every:
            self.from_line(a, i).wait_recv()
            for way in range(2):
                self.to_ring(a, i, way).start()
        self.pass_on(lambda copy: copy.start(), i)
        for a in self.every:
            self.to_pair(a, i, 0, self.me.core).start()

    def ring_stage(self, i):
        for way in range(2):
            for a in self.every:
                self.from_ring(a, i, way).wait_recv()
                if self.halved(a, way):
                    self.onward(a, i, way).start()
                self.to_pair(a, i, 1 + way, self.me.core).start()

    def far_stage(self, i):
        for way in range(2):
            for a in self.every:
                if self.halved(a, way):
                    self.from_onward(a, i, way).wait_recv()
                    self.to_pair_half(a, i, way, self.me.core).start()

    def stages(self):
        found = []
        for wave in range(self.line_size + 2):
            if 1 <= wave < self.line_size:
                found.append(partial(self.line_stage, wave))
            if 1 <= wave <= self.line_size:
                found.append(partial(self.ring_stage, wave - 1))
            if 2 <= wave:
                found.append(partial(self.far_stage, wave - 2))
        return found

    def finish(self):
        core = self.me.core
        for a in self.every:
            self.own(a).wait()
            for i in range(self.line_size):
                for lane in range(3):
                    self.to_pair(a, i, lane, 1 - core).wait_recv()
                    self.to_pair(a, i, lane, core).wait_send()
                for way in range(2):
                    self.to_ring(a, i, way).wait_send()
                    if self.halved(a, way):
                        self.to_pair_half(a, i, way, 1 - core).wait_recv()
                        self.to_pair_half(a, i, way, core).wait_send()
                        self.onward(a, i, way).wait_send()
        for i in range(self.line_size):
            self.pass_on(lambda copy: copy.wait_send(), i)


def gather_scratch(kinds, line_size):
    sems = pltpu.SemaphoreType.DMA
    return (
        [sems((kinds,))]
        + [sems((kinds, 2, line_size)), sems((kinds, line_size))]
        + [sems((kinds, 2, line_size))] * 4
        + [sems((kinds, 3, line_size))] * 2
        + [sems((kinds, 2, line_size))] * 2
    )


def gather_kernel(ring_size, line_size, kinds, *refs):
    job = Gather(ring_size, line_size, refs[:kinds], refs[kinds : 2 * kinds], refs[2 * kinds :])
    job.begin()
    for stage in job.stages():
        stage()
    job.finish()


def gather(shards, ring_size, line_size, ident):
    kinds = len(shards)
    count = 2 * ring_size * line_size
    return pl.pallas_call(
        partial(gather_kernel, ring_size, line_size, kinds),
        in_specs=[pl.BlockSpec(memory_space=pltpu.VMEM)] * kinds,
        out_specs=[pl.BlockSpec(memory_space=pl.ANY)] * kinds,
        out_shape=[jax.ShapeDtypeStruct((count,) + piece.shape, piece.dtype) for piece in shards],
        scratch_shapes=gather_scratch(kinds, line_size),
        compiler_params=pltpu.CompilerParams(collective_id=ident, has_side_effects=True),
        name="gather_shards",
    )(*shards)


def spread(stages, tick, ticks):
    for number, stage in enumerate(stages):
        pl.when(tick == number * ticks // len(stages))(stage)


BLOCK = 256
PART = 256


def ffn_kernel(
    x_ref,
    mixed_ref,
    wo_ref,
    cot_ref,
    pad_ref,
    gain_ref,
    wg_ref,
    wu_ref,
    wd_ref,
    out_ref,
    dmid_ref,
    dbranch_ref,
    ggate_ref,
    gup_ref,
    gdown_ref,
    dgain_ref,
    middle,
    normed,
    normed_t,
    dffn,
    out_acc,
    dn_acc,
    hidden,
    dgate,
    dup,
):
    step = pl.program_id(0)
    gain = gain_ref[...]

    @pl.when(step == 0)
    def _():
        middle[...] = mm(mixed_ref[...], wo_ref[...])
        out_acc[...] = jnp.zeros_like(out_acc)
        dn_acc[...] = jnp.zeros_like(dn_acc)

        def start(index, carry):
            rows = pl.ds(pl.multiple_of(index * SPAN, SPAN), SPAN)
            value = middle[rows, :] + x_ref[rows, :].astype(F32)
            middle[rows, :] = value
            low = (value * rms_factor(value, 1e-5) * gain).astype(BF)
            normed[rows, :] = low
            normed_t[:, rows] = jnp.transpose(low)
            pad = jnp.transpose(jnp.broadcast_to(pad_ref[index], (SPAN, SPAN)))[:, 0:1]
            dffn[rows, :] = (cot_ref[rows, :].astype(F32) * pad).astype(BF)
            return carry

        lax.fori_loop(0, CHUNKS, start, 0)

    wg, wu, wd = wg_ref[...], wu_ref[...], wd_ref[...]
    for part in range(LEN // PART):
        rows = pl.ds(part * PART, PART)
        gate, up = mm(normed[rows, :], wg), mm(normed[rows, :], wu)
        dhidden = mm_nt(dffn[rows, :], wd)
        sig = 1.0 / (1.0 + jnp.exp(-gate))
        silu = gate * sig
        hidden[rows, :] = (silu * up).astype(BF)
        dgate[rows, :] = (dhidden * up * (sig * (1.0 + gate * (1.0 - sig)))).astype(BF)
        dup[rows, :] = (dhidden * silu).astype(BF)
    gdown_ref[...] = mm_tn(hidden[...], dffn[...]).astype(BF)
    ggate_ref[...] = mm(normed_t[...], dgate[...]).astype(BF)
    gup_ref[...] = mm(normed_t[...], dup[...]).astype(BF)
    out_acc[...] += mm(hidden[...], wd)
    dn_acc[...] += mm_nt(dgate[...], wg) + mm_nt(dup[...], wu)

    @pl.when(step == pl.num_programs(0) - 1)
    def _():
        dgain_ref[...] = jnp.zeros_like(dgain_ref)

        def end(index, carry):
            rows = pl.ds(pl.multiple_of(index * SPAN, SPAN), SPAN)
            value = middle[rows, :]
            out_ref[rows, :] = (value + out_acc[rows, :]).astype(BF)
            factor = rms_factor(value, 1e-5)
            scaled = value * factor
            grad = dn_acc[rows, :]
            dscaled = grad * gain
            dmid = factor * (dscaled - scaled * jnp.mean(dscaled * scaled, axis=-1, keepdims=True))
            dmid += dffn[rows, :].astype(F32)
            dmid_ref[rows, :] = dmid
            dbranch_ref[rows, :] = dmid.astype(BF)
            dgain_ref[...] += jnp.sum(grad * scaled, axis=0, keepdims=True)
            return carry

        lax.fori_loop(0, CHUNKS, end, 0)


def feed_forward(hidden_in, mixed, w_output, cotangent, pads, gain_mid, w_ff, w_dn):
    blocks = FF // BLOCK
    square = fixed((LEN, D))
    column = pl.BlockSpec((D, BLOCK), lambda step: (0, step))
    band = pl.BlockSpec((BLOCK, D), lambda step: (step, 0))
    return pl.pallas_call(
        ffn_kernel,
        grid=(blocks,),
        in_specs=[
            square,
            square,
            fixed((WIDTH, D)),
            square,
            fixed((CHUNKS, 1, SPAN)),
            fixed((1, D)),
            column,
            pl.BlockSpec((D, BLOCK), lambda step: (0, blocks + step)),
            band,
        ],
        out_specs=[square, square, square, column, column, band, fixed((1, D))],
        out_shape=[
            jax.ShapeDtypeStruct((LEN, D), BF),
            jax.ShapeDtypeStruct((LEN, D), F32),
            jax.ShapeDtypeStruct((LEN, D), BF),
            jax.ShapeDtypeStruct((D, FF), BF),
            jax.ShapeDtypeStruct((D, FF), BF),
            jax.ShapeDtypeStruct((FF, D), BF),
            jax.ShapeDtypeStruct((1, D), F32),
        ],
        scratch_shapes=[
            pltpu.VMEM((LEN, D), F32),
            pltpu.VMEM((LEN, D), BF),
            pltpu.VMEM((D, LEN), BF),
            pltpu.VMEM((LEN, D), BF),
            pltpu.VMEM((LEN, D), F32),
            pltpu.VMEM((LEN, D), F32),
        ]
        + [pltpu.VMEM((LEN, BLOCK), BF)] * 3,
        compiler_params=pltpu.CompilerParams(vmem_limit_bytes=62 << 20),
        name="feed_forward",
    )(hidden_in, mixed, w_output, cotangent, pads, gain_mid, w_ff, w_ff, w_dn)


def pack_kernel(places, *refs):
    flats, packed = refs[: len(places) + 1], refs[len(places) + 1 :]
    for flat, (target, offset, tiles) in zip(flats, places):
        out = packed[target]
        rows = out.shape[0]
        for j in range(tiles):
            out[:, offset + j * 128 : offset + (j + 1) * 128] = flat[pl.ds(j, rows, stride=tiles), :].astype(BF)
    packed[-1][...] = jnp.broadcast_to(flats[-1][...].astype(BF).astype(F32), packed[-1].shape)


def pack(flats, vectors, places, shapes):
    vmem = pl.BlockSpec(memory_space=pltpu.VMEM)
    return pl.pallas_call(
        partial(pack_kernel, places),
        in_specs=[vmem] * (len(flats) + 1),
        out_specs=[vmem] * (len(shapes) + 1),
        out_shape=[jax.ShapeDtypeStruct(shape, BF) for shape in shapes] + [jax.ShapeDtypeStruct((8, 128), F32)],
        name="pack_shards",
    )(*[flat.reshape(-1, 128) for flat in flats], vectors.reshape(1, 128))


def unpack_kernel(places, kinds, *refs):
    packed, flats = refs[: kinds + 1], refs[kinds + 1 :]
    for flat, (target, offset, tiles) in zip(flats, places):
        source = packed[target]
        rows = source.shape[0]
        for j in range(tiles):
            flat[pl.ds(j, rows, stride=tiles), :] = source[:, offset + j * 128 : offset + (j + 1) * 128]
    flats[-1][...] = packed[-1][0:1]


def unpack(packed, places):
    vmem = pl.BlockSpec(memory_space=pltpu.VMEM)
    sizes = [packed[target].shape[0] * tiles for target, _, tiles in places] + [1]
    flats = pl.pallas_call(
        partial(unpack_kernel, places, len(packed) - 1),
        in_specs=[vmem] * len(packed),
        out_specs=[vmem] * len(sizes),
        out_shape=[jax.ShapeDtypeStruct((size, 128), F32) for size in sizes],
        name="unpack_sums",
    )(*packed)
    return [flat.reshape(-1) for flat in flats]


def rms_factor(values, eps):
    return lax.rsqrt(jnp.mean(values * values, axis=-1, keepdims=True) + eps)


def rms_back(grad, values, factor, gain):
    scaled = values * factor
    dscaled = grad * gain
    dvalues = factor * (dscaled - scaled * jnp.mean(dscaled * scaled, axis=-1, keepdims=True))
    return dvalues, jnp.sum(grad * scaled, axis=0)


def by_kernel(sizes, ring_size, fsdp_size):
    return ring_size == 4 and fsdp_size % 4 == 0 and all(size % 8 == 0 for size in sizes)


def gather_plain(shards):
    return [lax.all_gather(piece, AXES, axis=0) for piece in shards]


def scatter_plain(grads):
    return [lax.psum_scatter(piece.astype(F32), AXES, scatter_dimension=0) for piece in grads]


def per_device(
    hidden_in,
    w_query,
    w_latent,
    w_key_up,
    w_value_up,
    w_decay,
    w_outgate,
    w_out,
    w_gate,
    w_up,
    w_down,
    vectors,
    seg_ids,
    pad_mask,
    cotangent,
    *,
    ring_size,
    fsdp_size,
):
    count = ring_size * fsdp_size
    per_group = WIDTH // GROUPS
    latents = GROUPS * LATENT
    rows_d, rows_kv, rows_ff = D // count, latents // count, FF // count
    rows_all = (rows_d, rows_kv, rows_ff)
    vec_size = (2 * D + 2 * WIDTH) // count

    own = by_kernel(rows_all, ring_size, fsdp_size) and vec_size == 128
    flat_weights = (w_query, w_latent, w_key_up, w_value_up, w_decay, w_outgate, w_out, w_gate, w_up, w_down)
    wide, half_kv, ff = WIDTH // 128, per_group // 128, FF // 128
    places = (
        (0, 0, wide),
        (0, 3 * WIDTH, latents // 128),
        (1, 0, half_kv),
        (1, per_group, half_kv),
        (0, WIDTH, wide),
        (0, 2 * WIDTH, wide),
        (2, 0, D // 128),
        (3, 0, ff),
        (3, FF, ff),
        (4, 0, D // 128),
    )
    sums_at = places[:7] + ((3, 0, ff), (4, 0, ff), (5, 0, D // 128))
    if own:
        shapes = (
            (rows_d, 3 * WIDTH + latents),
            (rows_kv, 2 * per_group),
            (rows_d, D),
            (rows_d, 2 * FF),
            (rows_ff, D),
        )
        in_shard, kv_shard, out_shard, ff_shard, down_shard, vec_shard = pack(flat_weights, vectors, places, shapes)
    else:

        def rows_of(piece, rows):
            return piece.astype(BF).reshape(rows, -1)

        in_shard = jnp.concatenate(
            [rows_of(piece, rows_d) for piece in (w_query, w_decay, w_outgate, w_latent)], axis=1
        )
        kv_shard = jnp.concatenate([rows_of(w_key_up, rows_kv), rows_of(w_value_up, rows_kv)], axis=1)
        out_shard = rows_of(w_out, rows_d)
        ff_shard = jnp.concatenate([rows_of(w_gate, rows_d), rows_of(w_up, rows_d)], axis=1)
        down_shard = rows_of(w_down, rows_ff)
        vec_shard = jnp.broadcast_to(lax.reduce_precision(vectors, 8, 7).reshape(1, -1), (8, vec_size))
    comm = (ring_size, fsdp_size // 2)
    early, late = (in_shard, kv_shard, vec_shard), (out_shard, ff_shard, down_shard)
    w_in, w_kv, vecs = gather(early, *comm, 0) if own else gather_plain(early)
    w_in = w_in.reshape(D, 3 * WIDTH + latents)
    w_kv = w_kv.reshape(GROUPS, LATENT, 2 * per_group)
    vecs = vecs[:, 0].reshape(-1)
    gain_in, gain_mid = vecs[:D], vecs[D : 2 * D]
    decay_bias, out_gain = vecs[2 * D : 2 * D + WIDTH], vecs[2 * D + WIDTH :]

    segs = seg_ids.astype(F32).reshape(CHUNKS, 1, SPAN)
    pads = pad_mask.astype(F32).reshape(CHUNKS, 1, SPAN)

    inputs = hidden_in.astype(F32)
    factor_in = rms_factor(inputs, 1e-5)
    normed = (inputs * factor_in * gain_in).astype(BF)
    latent = mm(normed, w_in[:, 3 * WIDTH :]).astype(BF)
    bias_row, gain_row = decay_bias.reshape(1, WIDTH), out_gain.reshape(1, WIDTH)
    query, keys, values, decay_in, gate_in, mixed, heads, states, *rest = mixer_fwd(
        normed, latent, w_in, w_kv, bias_row, gain_row, segs, pads, late if own else (), comm + (0, 2) if own else None
    )
    w_output, w_ff, w_dn = rest if own else gather_plain(late)
    w_output = w_output.reshape(WIDTH, D)
    w_ff = w_ff.reshape(D, 2 * FF)
    w_dn = w_dn.reshape(FF, D)
    block_out, d_middle, d_branch, grad_gate, grad_up, grad_down, d_gain_mid = feed_forward(
        hidden_in, mixed, w_output, cotangent, pads, gain_mid.reshape(1, D), w_ff, w_dn
    )
    grad_out = mm_tn(mixed, d_branch)

    sent = (
        grad_gate.reshape(count, rows_d, -1),
        grad_up.reshape(count, rows_d, -1),
        grad_down.reshape(count, rows_ff, -1),
    )
    saved = (query, keys, values, decay_in, gate_in, gain_row, segs, pads, heads, states)
    d_query, d_keys, d_values, d_decay, d_gatein, d_bias, d_out_gain, *rest = mixer_bwd(
        saved, d_branch, w_output, sent if own else (), comm + (0, 3) if own else None
    )
    own_gate, own_up, own_down = rest if own else scatter_plain(sent)
    grad_kv, d_latent = [], []
    for g in range(GROUPS):
        d_kv = jnp.concatenate(
            [part[:, g * per_group : (g + 1) * per_group] for part in (d_keys, d_values)], axis=1
        )
        grad_kv.append(mm_tn(latent[:, g * LATENT : (g + 1) * LATENT], d_kv))
        d_latent.append(mm_nt(d_kv, w_kv[g]))
    grad_kv = jnp.concatenate(grad_kv, axis=0)
    d_latent = jnp.concatenate(d_latent, axis=1).astype(BF)
    d_in = jnp.concatenate([d_query, d_decay, d_gatein, d_latent], axis=1)
    grad_in = mm_tn(normed, d_in)
    d_normed = mm_nt(d_in, w_in)
    d_inputs, d_gain_in = rms_back(d_normed, inputs, factor_in, gain_in)
    grad_input = d_middle + d_inputs
    grad_vec = jnp.concatenate([d_gain_in, d_gain_mid.reshape(-1), d_bias.reshape(-1), d_out_gain.reshape(-1)])

    grad_vec = jnp.broadcast_to(grad_vec.reshape(count, 1, vec_size), (count, 8, vec_size))
    sent = (
        grad_in.astype(BF).reshape(count, rows_d, -1),
        grad_kv.astype(BF).reshape(count, rows_kv, -1),
        grad_out.astype(BF).reshape(count, rows_d, -1),
        grad_vec,
    )
    own_in, own_kv, own_out, own_vec = scatter(sent, *comm, 1) if own else scatter_plain(sent)
    if own:
        return (block_out, grad_input, *unpack((own_in, own_kv, own_out, own_gate, own_up, own_down, own_vec), sums_at))
    return (
        block_out,
        grad_input,
        own_in[:, :WIDTH].reshape(-1),
        own_in[:, 3 * WIDTH :].reshape(-1),
        own_kv[:, :per_group].reshape(-1),
        own_kv[:, per_group:].reshape(-1),
        own_in[:, WIDTH : 2 * WIDTH].reshape(-1),
        own_in[:, 2 * WIDTH : 3 * WIDTH].reshape(-1),
        own_out.reshape(-1),
        own_gate.reshape(-1),
        own_up.reshape(-1),
        own_down.reshape(-1),
        own_vec[0],
    )


def solution(mesh):
    sizes = {"ring_size": mesh.shape["dp"], "fsdp_size": mesh.shape["fsdp"]}
    rows, flat = P(AXES, None), P(AXES)
    in_specs = (rows,) + (flat,) * 13 + (rows,)
    out_specs = (rows, rows) + (flat,) * 11
    return jax.shard_map(
        partial(per_device, **sizes), mesh=mesh, in_specs=in_specs, out_specs=out_specs, check_vma=False
    )
```

```python
from functools import partial

import jax
import jax.numpy as jnp
from jax import lax
from jax.experimental import pallas as pl
from jax.experimental.pallas import tpu as pltpu
from jax.sharding import PartitionSpec as P

D = 1024
HEADS = 16
HEAD_DIM = 64
GROUPS = 2
LATENT = 256
FF = 2816
LEN = 1024
WIDTH = HEADS * HEAD_DIM
SPAN = 128
LANES = 256
PACK = LANES // HEAD_DIM
BANDS = WIDTH // LANES
CHUNKS = LEN // SPAN
LIMIT = 85.0
TICKS = CHUNKS + 7
AXES = ("dp", "fsdp")
BF = jnp.bfloat16
F32 = jnp.float32
MESH = pl.DeviceIdType.MESH


def mm(left, right):
    return lax.dot_general(left, right, (((1,), (0,)), ((), ())), preferred_element_type=F32)


def mm_nt(left, right):
    return lax.dot_general(left, right, (((1,), (1,)), ((), ())), preferred_element_type=F32)


def mm_tn(left, right):
    return lax.dot_general(left, right, (((0,), (0,)), ((), ())), preferred_element_type=F32)


def halves(value):
    high = value.astype(BF)
    return high, (value - high.astype(F32)).astype(BF)


def exact_left(ones, value):
    high, rest = halves(value)
    return mm(ones, high) + mm(ones, rest)


def exact_right(value, ones):
    high, rest = halves(value)
    return mm(high, ones) + mm(rest, ones)


def head_masks():
    lane = lax.broadcasted_iota(jnp.int32, (1, LANES), 1) // HEAD_DIM
    return [lane == head for head in range(PACK)]


def stacked(value, masks):
    zero = jnp.zeros_like(value)
    return jnp.concatenate([jnp.where(mask, value, zero) for mask in masks], axis=0)


def side_by_side(value):
    return jnp.concatenate([value[h * SPAN : (h + 1) * SPAN] for h in range(PACK)], axis=1)


def same_head():
    row = lax.broadcasted_iota(jnp.int32, (LANES, LANES), 0) // HEAD_DIM
    col = lax.broadcasted_iota(jnp.int32, (LANES, LANES), 1) // HEAD_DIM
    return row == col


def triangle(lower):
    row = lax.broadcasted_iota(jnp.int32, (SPAN, SPAN), 0)
    col = lax.broadcasted_iota(jnp.int32, (SPAN, SPAN), 1)
    return (row >= col) if lower else (row <= col)


def decays(decay, pad, lower_ones):
    small = jnp.exp(-jnp.abs(decay))
    log_sig = jnp.minimum(decay, 0.0) - jnp.log(1.0 + small)
    total = exact_left(lower_ones, log_sig * (pad * (1.0 / 16.0)))
    ending = total[SPAN - 1 : SPAN]
    middle = 0.5 * ending
    centred = total - middle
    up = jnp.exp(jnp.minimum(centred, LIMIT))
    down = jnp.exp(jnp.minimum(-centred, LIMIT))
    half = jnp.exp(middle)
    return up, down, half, small


def flags(seg_ref, pad_ref, index):
    seg_row = seg_ref[index]
    seg_square = jnp.transpose(jnp.broadcast_to(seg_row, (SPAN, SPAN)))
    pad = jnp.transpose(jnp.broadcast_to(pad_ref[index], (SPAN, SPAN)))[:, 0:1]
    seg_col, ending = seg_square[:, 0:1], seg_row[:, SPAN - 1 :]
    before = seg_ref[jnp.maximum(index - 1, 0)][:, SPAN - 1 :]
    fresh = (seg_col == before).astype(F32)
    to_end = (seg_col == ending).astype(F32)
    keep = (ending == before).astype(F32)
    allowed = (seg_square == seg_row) & triangle(True)
    return fresh, to_end, pad, allowed, keep


def mixer_fwd_kernel(comm, *refs):
    kinds = comm[2] if comm else 0
    normed_ref, latent_ref, wp_ref, wkv_ref, bias_ref, gain_ref, seg_ref, pad_ref = refs[:8]
    shards, refs = refs[8 : 8 + kinds], refs[8 + kinds :]
    q_ref, k_ref, v_ref, decay_ref, gate_ref, mixed_ref, heads_ref, states_ref, normed_t_ref, latent_t_ref = refs[:10]
    gathered, state, sems = refs[10 : 10 + kinds], refs[10 + kinds], refs[11 + kinds :]
    band = pl.program_id(0)
    job = Gather(comm[0], comm[1], shards, gathered, sems) if comm else None
    stages = job.stages() if comm else []
    ticks = BANDS * (CHUNKS + 1)
    if comm:
        pl.when(band == 0)(job.begin)
    masks = head_masks()
    diag = same_head()
    diag_ones = diag.astype(F32).astype(BF)
    lower_ones = triangle(True).astype(F32).astype(BF)
    state[...] = jnp.zeros_like(state)
    gain = gain_ref[...]
    q_ref[...] = mm(normed_ref[...], wp_ref[:, :LANES])
    decay_ref[...] = mm(normed_ref[...], wp_ref[:, LANES : 2 * LANES]) + bias_ref[...]
    gate_ref[...] = mm(normed_ref[...], wp_ref[:, 2 * LANES :])
    k_ref[...] = mm(latent_ref[...], wkv_ref[0, :, :LANES])
    v_ref[...] = mm(latent_ref[...], wkv_ref[0, :, LANES:])
    normed_t_ref[...] = jnp.transpose(normed_ref[:, pl.ds(pl.multiple_of(band * LANES, LANES), LANES)])
    latent_t_ref[...] = jnp.transpose(latent_ref[...])

    def chunk(index):
        rows = pl.ds(pl.multiple_of(index * SPAN, SPAN), SPAN)
        fresh, to_end, pad, allowed, keep = flags(seg_ref, pad_ref, index)
        up, down, half, _ = decays(decay_ref[rows, :], pad, lower_ones)
        query = q_ref[rows, :] * (HEAD_DIM**-0.5) * up
        key = k_ref[rows, :] * pad * down
        value = v_ref[rows, :].astype(BF)
        query_low, key_low = query.astype(BF), key.astype(BF)
        scores = mm_nt(stacked(query_low, masks), key_low)
        scores = scores.reshape(PACK, SPAN, SPAN)
        scores = jnp.where(allowed[None], scores, 0.0).astype(BF).reshape(PACK * SPAN, SPAN)
        old = state[...]
        old_low = old.astype(BF)
        states_ref[0, index] = old_low
        heads = mm(side_by_side(scores), stacked(value, masks))
        heads += mm_nt((query * (half * fresh)).astype(BF), old_low)
        tail = (key * (half * to_end)).astype(BF)
        state[...] = old * (half * half * keep) + jnp.where(diag, mm_tn(value, tail), 0.0)
        heads_ref[rows, :] = heads
        scale = lax.rsqrt(exact_right(heads * heads, diag_ones) * (1.0 / HEAD_DIM) + 1e-2)
        gate = gate_ref[rows, :]
        silu = gate / (1.0 + jnp.exp(-gate))
        mixed_ref[rows, :] = (heads * scale * gain * silu).astype(BF)

    def tick(index, carry):
        spread(stages, band * (CHUNKS + 1) + index, ticks)
        pl.when(index < CHUNKS)(lambda: chunk(index))
        return carry

    lax.fori_loop(0, CHUNKS + 1, tick, 0)
    if comm:
        pl.when(band == BANDS - 1)(job.finish)


def mixer_bwd_kernel(comm, *refs):
    kinds = comm[2] if comm else 0
    q_ref, k_ref, v_ref, decay_ref, gate_ref, gain_ref, seg_ref, pad_ref, heads_ref, states_ref = refs[:10]
    dbranch_ref, wo_ref, mixed_ref, normed_t_ref, latent_t_ref = refs[10:15]
    wp_ref, wl_ref, wkv_ref = refs[15:18]
    grads, refs = refs[18 : 18 + kinds], refs[18 + kinds :]
    gproj_ref, glat_ref, gkv_ref, gout_ref, dnormed_ref, dbias_ref, dgain_ref = refs[:7]
    sums, refs = refs[7 : 7 + kinds], refs[7 + kinds :]
    state, dmix_ref, dlatent, dproj, dkv = refs[:5]
    scratch = refs[5:]
    dq_ref, ddecay_ref, dgate_ref = (dproj.at[:, part * LANES : (part + 1) * LANES] for part in range(3))
    dk_ref, dv_ref = (dkv.at[:, part * LANES : (part + 1) * LANES] for part in range(2))
    band = pl.program_id(0)
    job = scatter_of(comm[0], comm[1], grads, sums, scratch) if comm else None
    stages = job.stages() if comm else []
    ticks = BANDS * TICKS
    if comm:
        pl.when(band == 0)(job.begin)
    dmix_ref[...] = mm_nt(dbranch_ref[...], wo_ref[...])

    @pl.when(band == 0)
    def _():
        dnormed_ref[...] = jnp.zeros_like(dnormed_ref)

    masks = head_masks()
    diag = same_head()
    diag_ones = diag.astype(F32).astype(BF)
    lower_ones = triangle(True).astype(F32).astype(BF)
    upper_ones = triangle(False).astype(F32).astype(BF)
    state[...] = jnp.zeros_like(state)
    dbias_ref[...] = jnp.zeros_like(dbias_ref)
    dgain_ref[...] = jnp.zeros_like(dgain_ref)
    gain = gain_ref[...]

    def chunk(step):
        index = CHUNKS - 1 - step
        rows = pl.ds(pl.multiple_of(index * SPAN, SPAN), SPAN)
        fresh, to_end, pad, allowed, keep = flags(seg_ref, pad_ref, index)
        heads = heads_ref[rows, :]
        scale = lax.rsqrt(exact_right(heads * heads, diag_ones) * (1.0 / HEAD_DIM) + 1e-2)
        normed = heads * scale
        gate = gate_ref[rows, :]
        sig = 1.0 / (1.0 + jnp.exp(-gate))
        silu = gate * sig
        dmix = dmix_ref[rows, :]
        both = dmix * normed
        dgain_ref[...] += jnp.sum(both * silu, axis=0, keepdims=True)
        dgate_ref[rows, :] = (both * gain * (sig * (1.0 + gate * (1.0 - sig)))).astype(BF)
        dnormed = dmix * gain * silu
        mean = exact_right(dnormed * normed, diag_ones) * (1.0 / HEAD_DIM)
        dheads = (scale * (dnormed - normed * mean)).astype(BF)
        decay = decay_ref[rows, :]
        up, down, half, small = decays(decay, pad, lower_ones)
        unit = HEAD_DIM**-0.5
        query = q_ref[rows, :] * unit * up
        key = k_ref[rows, :] * pad * down
        value = v_ref[rows, :].astype(BF)
        query_low, key_low = query.astype(BF), key.astype(BF)
        enter = half * fresh
        leave = half * to_end
        query_in = (query * enter).astype(BF)
        tail = (key * leave).astype(BF)
        query_stack = stacked(query_low, masks)
        dheads_stack = stacked(dheads, masks)
        scores = mm_nt(query_stack, key_low).reshape(PACK, SPAN, SPAN)
        scores = jnp.where(allowed[None], scores, 0.0).astype(BF).reshape(PACK * SPAN, SPAN)
        dscores = mm_nt(dheads_stack, value).reshape(PACK, SPAN, SPAN)
        dscores = jnp.where(allowed[None], dscores, 0.0).astype(BF).reshape(PACK * SPAN, SPAN)
        dstate = state[...]
        dstate_low = dstate.astype(BF)
        old = states_ref[0, index]
        dvalue = mm_tn(scores, dheads_stack) + mm_nt(tail, dstate_low)
        dv_ref[rows, :] = dvalue.astype(BF)
        dquery = mm(side_by_side(dscores), stacked(key_low, masks))
        dkey = mm_tn(dscores, query_stack)
        dquery_in = mm(dheads, old)
        dtail = mm(value, dstate_low)
        whole = half * half * keep
        state[...] = dstate * whole + jnp.where(diag, mm_tn(dheads, query_in), 0.0)
        dq_ref[rows, :] = ((dquery + dquery_in * enter) * (up * unit)).astype(BF)
        dk_ref[rows, :] = ((dkey + dtail * leave) * (down * pad)).astype(BF)
        from_tail = dtail * tail.astype(F32)
        dtotal = (
            dquery * query_low.astype(F32)
            - dkey * key_low.astype(F32)
            + dquery_in * query_in.astype(F32)
            - from_tail
        )
        ends = jnp.sum(from_tail, axis=0, keepdims=True)
        ends += whole * jnp.sum(dstate * old.astype(F32), axis=0, keepdims=True)
        dlog = exact_left(upper_ones, dtotal) + ends
        other = jnp.where(decay >= 0, small, 1.0) / (1.0 + small)
        ddecay = dlog * (pad * (1.0 / 16.0)) * other
        dbias_ref[...] += jnp.sum(ddecay, axis=0, keepdims=True)
        ddecay_ref[rows, :] = ddecay.astype(BF)

    first, last = band % (BANDS // GROUPS) == 0, band % (BANDS // GROUPS) == BANDS // GROUPS - 1

    def proj_piece(part):
        cols = slice(part * 3 * LANES // 2, (part + 1) * 3 * LANES // 2)
        gproj_ref[:, cols] = mm(normed_t_ref[...], dproj[:, cols]).astype(BF)

    def out_piece():
        gout_ref[...] = mm_tn(mixed_ref[...], dbranch_ref[...]).astype(BF)

    def kv_piece():
        gkv_ref[...] = mm(latent_t_ref[...], dkv[...]).astype(BF)
        added = mm_nt(dkv[...], wkv_ref[0])

        @pl.when(first)
        def _():
            dlatent[...] = added

        @pl.when(jnp.logical_not(first))
        def _():
            dlatent[...] += added

    def normed_piece(part):
        rows = slice(part * LEN // 2, (part + 1) * LEN // 2)
        dnormed_ref[rows, :] += mm_nt(dproj[rows, :], wp_ref[...])

    def latent_piece():
        low = dlatent[...].astype(BF)
        glat_ref[...] = mm(normed_t_ref[...], low).astype(BF)
        dnormed_ref[...] += mm_nt(low, wl_ref[...])

    pieces = [partial(proj_piece, 0), partial(proj_piece, 1), out_piece, kv_piece]
    pieces += [partial(normed_piece, 0), partial(normed_piece, 1)]

    def tick(index, carry):
        spread(stages, band * TICKS + index, ticks, 7)
        pl.when(index < CHUNKS)(lambda: chunk(index))
        for number, piece in enumerate(pieces):
            pl.when(index == CHUNKS + number)(piece)
        pl.when((index == CHUNKS + len(pieces)) & last)(latent_piece)
        return carry

    lax.fori_loop(0, TICKS, tick, 0)
    if comm:
        pl.when(band == BANDS - 1)(job.finish)


def band_specs():
    tokens = pl.BlockSpec((LEN, LANES), lambda band: (0, band))
    vector = pl.BlockSpec((1, LANES), lambda band: (0, band))
    segs = pl.BlockSpec((CHUNKS, 1, SPAN), lambda band: (0, 0, 0))
    states = pl.BlockSpec((1, CHUNKS, LANES, LANES), lambda band: (band, 0, 0, 0))
    return tokens, vector, segs, states


def fixed(shape):
    return pl.BlockSpec(shape, lambda band: (0,) * len(shape), pipeline_mode=pl.Buffered(1))


def mixer_fwd(normed, latent, w_in, w_kv, bias, gain, segs, pads, shards, comm):
    tokens, vector, segs_spec, states = band_specs()
    kinds = len(shards)
    half_bands = BANDS // GROUPS
    in_specs = [fixed((LEN, D)), pl.BlockSpec((LEN, LATENT), lambda band: (0, band // half_bands))]
    in_specs.append(pl.BlockSpec((D, 3 * LANES), lambda band: (0, band)))
    in_specs.append(
        pl.BlockSpec((1, LATENT, 2 * LANES), lambda band: (band // half_bands, 0, band % half_bands))
    )
    in_specs += [vector, vector, segs_spec, segs_spec]
    wide = jax.ShapeDtypeStruct((LEN, WIDTH), F32)
    out_shape = [wide] * 5 + [
        jax.ShapeDtypeStruct((LEN, WIDTH), BF),
        wide,
        jax.ShapeDtypeStruct((BANDS, CHUNKS, LANES, LANES), BF),
        jax.ShapeDtypeStruct((D, LEN), BF),
        jax.ShapeDtypeStruct((GROUPS * LATENT, LEN), BF),
    ]
    scratch = [pltpu.VMEM((LANES, LANES), F32)]
    params = {}
    if comm:
        count = 2 * comm[0] * comm[1]
        in_specs += [fixed(shard.shape) for shard in shards]
        out_shape += [jax.ShapeDtypeStruct((count,) + shard.shape, shard.dtype) for shard in shards]
        scratch += gather_scratch(kinds, comm[1])
        params = {"collective_id": comm[3], "has_side_effects": True}
        comm = comm[:2] + (kinds,)
    return pl.pallas_call(
        partial(mixer_fwd_kernel, comm),
        grid=(BANDS,),
        in_specs=in_specs,
        out_specs=[tokens] * 7
        + [states, pl.BlockSpec((LANES, LEN), lambda band: (band, 0))]
        + [pl.BlockSpec((LATENT, LEN), lambda band: (band // half_bands, 0))]
        + [pl.BlockSpec(memory_space=pl.ANY)] * kinds,
        out_shape=out_shape,
        scratch_shapes=scratch,
        compiler_params=pltpu.CompilerParams(vmem_limit_bytes=52 << 20, **params),
        name="mixer_fwd",
    )(normed, latent, w_in, w_kv, bias, gain, segs, pads, *shards)


def mixer_bwd(saved, d_branch, w_output, mixed, normed_t, latent_t, w_in, w_kv, grads, comm):
    _, vector, segs_spec, states = band_specs()
    kinds, half_bands = len(grads), BANDS // GROUPS
    once = pl.Buffered(1)
    tokens = pl.BlockSpec((LEN, LANES), lambda band: (0, band))
    rows = pl.BlockSpec((LANES, D), lambda band: (band, 0))
    sums = jax.ShapeDtypeStruct((1, WIDTH), F32)
    in_specs = [tokens] * 5 + [vector, segs_spec, segs_spec, tokens, states]
    in_specs += [fixed((LEN, D)), rows, tokens, fixed((D, LEN))]
    in_specs.append(pl.BlockSpec((LATENT, LEN), lambda band: (band // half_bands, 0), pipeline_mode=once))
    in_specs.append(pl.BlockSpec((D, 3 * LANES), lambda band: (0, band)))
    in_specs.append(
        pl.BlockSpec((D, LATENT), lambda band: (0, 3 * BANDS + band // half_bands), pipeline_mode=once)
    )
    in_specs.append(
        pl.BlockSpec((1, LATENT, 2 * LANES), lambda band: (band // half_bands, 0, band % half_bands))
    )
    out_specs = [
        pl.BlockSpec((D, 3 * LANES), lambda band: (0, band)),
        pl.BlockSpec((D, LATENT), lambda band: (0, band // half_bands)),
        pl.BlockSpec((LATENT, 2 * LANES), lambda band: (band // half_bands, band % half_bands)),
        rows,
        fixed((LEN, D)),
        vector,
        vector,
    ]
    out_shape = [
        jax.ShapeDtypeStruct((D, 3 * WIDTH), BF),
        jax.ShapeDtypeStruct((D, GROUPS * LATENT), BF),
        jax.ShapeDtypeStruct((GROUPS * LATENT, 2 * WIDTH // GROUPS), BF),
        jax.ShapeDtypeStruct((WIDTH, D), BF),
        jax.ShapeDtypeStruct((LEN, D), F32),
        sums,
        sums,
    ]
    scratch = [pltpu.VMEM((LANES, LANES), F32), pltpu.VMEM((LEN, LANES), F32), pltpu.VMEM((LEN, LATENT), F32)]
    scratch += [pltpu.VMEM((LEN, 3 * LANES), BF), pltpu.VMEM((LEN, 2 * LANES), BF)]
    params = {}
    if comm:
        in_specs += [pl.BlockSpec(memory_space=pl.ANY)] * kinds
        out_specs += [fixed(grad.shape[1:]) for grad in grads]
        out_shape += [jax.ShapeDtypeStruct(grad.shape[1:], F32) for grad in grads]
        scratch += scatter_scratch(grads, comm[0], comm[1])
        params = {"collective_id": comm[3], "has_side_effects": True}
        comm = comm[:2] + (kinds,)
    return pl.pallas_call(
        partial(mixer_bwd_kernel, comm),
        grid=(BANDS,),
        in_specs=in_specs,
        out_specs=out_specs,
        out_shape=out_shape,
        scratch_shapes=scratch,
        compiler_params=pltpu.CompilerParams(vmem_limit_bytes=63 << 20, **params),
        name="mixer_bwd",
    )(*saved, d_branch, w_output, mixed, normed_t, latent_t, w_in, w_in, w_kv, *grads)


class Place:
    def __init__(self, ring_size, line_size):
        self.ring_size, self.line_size = ring_size, line_size
        self.d, f = lax.axis_index("dp"), lax.axis_index("fsdp")
        self.z, self.core = f // 2, f % 2
        self.pos = self.at_ring(self.d)

    def at_ring(self, index):
        if self.ring_size != 4:
            return index
        return index + (index // 2) * (1 - 2 * (index % 2))

    def ring(self, offset):
        return self.at_ring((self.pos + offset + self.ring_size) % self.ring_size)

    def far(self, i):
        n = self.line_size
        low = self.z < n // 2
        near = jnp.where(low, self.z, n - 1 - self.z)
        if i == n - 1:
            return self.z
        line = n - 1 - i - jnp.where(n - 1 - i <= near, 1, 0)
        return jnp.where(low, line, n - 1 - line)

    def device(self, d, z, core):
        return (d, 2 * z + core)

    def slot(self, d, z, core):
        return d * (2 * self.line_size) + 2 * z + core


def greet(place, peers):
    barrier = pltpu.get_barrier_semaphore()
    for peer in peers:
        pl.semaphore_signal(barrier, inc=1, device_id=peer, device_id_type=MESH)
    pl.semaphore_wait(barrier, len(peers))


def peers_of(place):
    me = place
    peers = [me.device(me.d, me.z, 1 - me.core)]
    peers += [me.device(me.ring(step), me.z, me.core) for step in (1, -1)]
    peers += [me.device(me.d, me.far(i), me.core) for i in range(me.line_size - 1)]
    return peers


def send(src, dst, send_sem, recv_sem, device):
    return pltpu.make_async_remote_copy(
        src_ref=src, dst_ref=dst, send_sem=send_sem, recv_sem=recv_sem, device_id=device, device_id_type=MESH
    )


AHEAD = 4


class Scatter:
    def __init__(self, ring_size, line_size, grads, outs, accs, parts, hops, tails, sems):
        self.ring_size, self.line_size = ring_size, line_size
        self.grads, self.outs = grads, outs
        self.accs, self.parts, self.hops, self.tails = accs, parts, hops, tails
        self.load_sem, self.psend, self.precv, self.hsend, self.hrecv, self.tsend, self.trecv = sems
        self.me = Place(ring_size, line_size)
        self.order = [self.me.far(i) for i in range(line_size)]
        self.every = range(len(grads))
        self.waves = [
            (step, wave - step)
            for wave in range(1, ring_size + line_size)
            for step in range(1, ring_size + 1)
            if 0 <= wave - step < line_size
        ]

    def way(self, a, i):
        return 1 if (a + i) % 2 == 0 else -1

    def dest(self, a, step, i, core):
        me = self.me
        return self.grads[a].at[me.slot(me.ring(-step * self.way(a, i)), self.order[i], core)]

    def load(self, a, number):
        step, i = self.waves[number]
        slot = number % AHEAD
        return pltpu.make_async_copy(
            self.dest(a, step, i, self.me.core), self.accs[a].at[slot], self.load_sem.at[a, slot]
        )

    def to_pair(self, a, step, i):
        me = self.me
        return send(
            self.dest(a, step, i, 1 - me.core),
            self.parts[a].at[step - 1, i],
            self.psend.at[a, step - 1, i],
            self.precv.at[a, step - 1, i],
            me.device(me.d, me.z, 1 - me.core),
        )

    def to_ring(self, a, step, i):
        me = self.me
        return send(
            self.parts[a].at[step - 1, i],
            self.hops[a].at[step - 1, i],
            self.hsend.at[a, step - 1, i],
            self.hrecv.at[a, step - 1, i],
            me.device(me.ring(self.way(a, i)), me.z, me.core),
        )

    def to_line(self, a, i):
        me = self.me
        return send(
            self.parts[a].at[self.ring_size - 1, i],
            self.tails[a].at[me.z],
            self.tsend.at[a, i],
            self.trecv.at[a, me.z],
            me.device(me.d, self.order[i], me.core),
        )

    def from_line(self, a, i):
        me = self.me
        here = self.tails[a].at[self.order[i]]
        return send(
            here, here, self.tsend.at[a, i], self.trecv.at[a, self.order[i]], me.device(me.d, self.order[i], me.core)
        )

    def blocks(self, a):
        width = self.grads[a].shape[-1]
        block = 512 if width % 512 == 0 else width
        return width // block, block

    def add_up(self, a, number):
        step, i = self.waves[number]
        count, block = self.blocks(a)
        here, own = self.parts[a], self.accs[a]
        final = step == self.ring_size and i == self.line_size - 1

        def body(j, carry):
            cols = pl.ds(pl.multiple_of(j * block, block), block)
            total = own[number % AHEAD, :, cols].astype(F32) + here[step - 1, i, :, cols].astype(F32)
            if step > 1:
                total += self.hops[a][step - 2, i, :, cols].astype(F32)
            if final:
                self.outs[a][:, cols] = total
            else:
                here[step - 1, i, :, cols] = total.astype(here.dtype)
            return carry

        lax.fori_loop(0, count, body, 0)

    def begin(self):
        for number in range(min(AHEAD, len(self.waves))):
            for a in self.every:
                self.load(a, number).start()
        greet(self.me, peers_of(self.me))
        for step, i in self.waves:
            for a in self.every:
                self.to_pair(a, step, i).start()

    def entry(self, number):
        step, i = self.waves[number]
        for a in self.every:
            self.load(a, number).wait()
            self.to_pair(a, step, i).wait_recv()
            if step > 1:
                self.to_ring(a, step - 1, i).wait_recv()
            self.add_up(a, number)
            if step < self.ring_size:
                self.to_ring(a, step, i).start()
            elif i < self.line_size - 1:
                self.to_line(a, i).start()
            if number + AHEAD < len(self.waves):
                self.load(a, number + AHEAD).start()

    def stages(self):
        return [partial(self.entry, number) for number in range(len(self.waves))]

    def finish(self):
        last = self.line_size - 1
        for a in self.every:
            for i in range(last):
                self.from_line(a, i).wait_recv()
            number, block = self.blocks(a)

            def body(j, carry, a=a, block=block):
                cols = pl.ds(pl.multiple_of(j * block, block), block)
                total = self.outs[a][:, cols]
                for i in range(last):
                    total += self.tails[a][self.order[i], :, cols].astype(F32)
                self.outs[a][:, cols] = total
                return carry

            lax.fori_loop(0, number, body, 0)
        for step, i in self.waves:
            for a in self.every:
                self.to_pair(a, step, i).wait_send()
                if step < self.ring_size:
                    self.to_ring(a, step, i).wait_send()
                elif i < last:
                    self.to_line(a, i).wait_send()


def scatter_scratch(grads, ring_size, line_size):
    kinds = len(grads)
    sems = pltpu.SemaphoreType.DMA
    scratch = []
    for lead in ((AHEAD,), (ring_size, line_size), (ring_size - 1, line_size), (line_size,)):
        scratch += [pltpu.VMEM(lead + grad.shape[1:], grad.dtype) for grad in grads]
    return (
        scratch
        + [sems((kinds, AHEAD))]
        + [sems((kinds, ring_size, line_size))] * 4
        + [sems((kinds, line_size))] * 2
    )


def scatter_of(ring_size, line_size, grads, outs, scratch):
    kinds = len(grads)
    rooms = [scratch[k * kinds : (k + 1) * kinds] for k in range(4)]
    return Scatter(ring_size, line_size, grads, outs, *rooms, scratch[4 * kinds :])


def scatter_kernel(ring_size, line_size, kinds, *refs):
    job = scatter_of(ring_size, line_size, refs[:kinds], refs[kinds : 2 * kinds], refs[2 * kinds :])
    job.begin()
    for stage in job.stages():
        stage()
    job.finish()


def scatter(grads, ring_size, line_size, ident):
    kinds = len(grads)
    return pl.pallas_call(
        partial(scatter_kernel, ring_size, line_size, kinds),
        in_specs=[pl.BlockSpec(memory_space=pl.ANY)] * kinds,
        out_specs=[pl.BlockSpec(memory_space=pltpu.VMEM)] * kinds,
        out_shape=[jax.ShapeDtypeStruct(grad.shape[1:], F32) for grad in grads],
        scratch_shapes=scatter_scratch(grads, ring_size, line_size),
        compiler_params=pltpu.CompilerParams(
            collective_id=ident, has_side_effects=True, vmem_limit_bytes=60 << 20
        ),
        name="scatter_sums",
    )(*grads)


class Gather:
    def __init__(self, ring_size, line_size, shards, outs, sems):
        self.line_size = line_size
        self.shards, self.outs = shards, outs
        (
            self.own_sem,
            self.zsend,
            self.zrecv,
            self.hsend,
            self.hrecv,
            self.osend,
            self.orecv,
            self.psend,
            self.precv,
            self.qsend,
            self.qrecv,
        ) = sems
        self.me = Place(ring_size, line_size)
        self.order = [self.me.far(line_size - 1 - i) for i in range(line_size)]
        self.pair = self.me.device(self.me.d, self.me.z, 1 - self.me.core)
        self.mine = self.me.slot(self.me.d, self.me.z, self.me.core)
        self.every = range(len(shards))

    def half(self, a, way):
        width = self.shards[a].shape[-1]
        if width % 256:
            return pl.ds(0, width)
        return pl.ds(0 if way == 0 else width // 2, width // 2)

    def halved(self, a, way):
        return self.shards[a].shape[-1] % 256 == 0 or way == 0

    def beside(self, way):
        return self.me.device(self.me.ring(1 - 2 * way), self.me.z, self.me.core)

    def spot(self, a, offset, i, core):
        return self.outs[a].at[self.me.slot(self.me.ring(offset), self.order[i], core)]

    def own(self, a):
        return pltpu.make_async_copy(self.shards[a], self.outs[a].at[self.mine], self.own_sem.at[a])

    def along(self, a, i, up):
        me = self.me
        here = self.spot(a, 0, i, me.core)
        return send(
            self.shards[a] if i == 0 else here,
            here,
            self.zsend.at[a, up, i],
            self.zrecv.at[a, self.order[i]],
            me.device(me.d, me.z + 2 * up - 1, me.core),
        )

    def from_line(self, a, i):
        me = self.me
        here = self.spot(a, 0, i, me.core)
        return send(
            here, here, self.zsend.at[a, 0, i], self.zrecv.at[a, self.order[i]], me.device(me.d, self.order[i], me.core)
        )

    def pass_on(self, act, i):
        me, last = self.me, self.line_size - 1
        upward, downward = me.z < last, me.z > 0
        if i:
            upward &= self.order[i] < me.z
            downward &= self.order[i] > me.z
        for up, wanted in ((1, upward), (0, downward)):

            @pl.when(wanted)
            def _(up=up):
                for a in self.every:
                    act(self.along(a, i, up))

    def to_ring(self, a, i, way):
        here = self.spot(a, 0, i, self.me.core)
        src = self.shards[a] if i == 0 else here
        return send(src, here, self.hsend.at[a, way, i], self.hrecv.at[a, way, i], self.beside(way))

    def from_ring(self, a, i, way):
        here = self.spot(a, 2 * way - 1, i, self.me.core)
        return send(here, here, self.hsend.at[a, way, i], self.hrecv.at[a, way, i], self.beside(1 - way))

    def onward(self, a, i, way):
        here = self.spot(a, 2 * way - 1, i, self.me.core).at[:, self.half(a, way)]
        return send(here, here, self.osend.at[a, way, i], self.orecv.at[a, way, i], self.beside(way))

    def from_onward(self, a, i, way):
        here = self.spot(a, 2, i, self.me.core).at[:, self.half(a, way)]
        return send(here, here, self.osend.at[a, way, i], self.orecv.at[a, way, i], self.beside(1 - way))

    def to_pair(self, a, i, lane, core):
        here = self.spot(a, (0, -1, 1)[lane], i, core)
        src = self.shards[a] if (lane == 0 and i == 0 and core is self.me.core) else here
        return send(src, here, self.psend.at[a, lane, i], self.precv.at[a, lane, i], self.pair)

    def to_pair_half(self, a, i, way, core):
        here = self.spot(a, 2, i, core).at[:, self.half(a, way)]
        return send(here, here, self.qsend.at[a, way, i], self.qrecv.at[a, way, i], self.pair)

    def begin(self):
        for a in self.every:
            self.own(a).start()
        greet(self.me, peers_of(self.me))
        for a in self.every:
            for way in range(2):
                self.to_ring(a, 0, way).start()
        self.pass_on(lambda copy: copy.start(), 0)
        for a in self.every:
            self.to_pair(a, 0, 0, self.me.core).start()

    def line_stage(self, i):
        for a in self.every:
            self.from_line(a, i).wait_recv()
            for way in range(2):
                self.to_ring(a, i, way).start()
        self.pass_on(lambda copy: copy.start(), i)
        for a in self.every:
            self.to_pair(a, i, 0, self.me.core).start()

    def ring_stage(self, i):
        for way in range(2):
            for a in self.every:
                self.from_ring(a, i, way).wait_recv()
                if self.halved(a, way):
                    self.onward(a, i, way).start()
                self.to_pair(a, i, 1 + way, self.me.core).start()

    def far_stage(self, i):
        for way in range(2):
            for a in self.every:
                if self.halved(a, way):
                    self.from_onward(a, i, way).wait_recv()
                    self.to_pair_half(a, i, way, self.me.core).start()

    def stages(self):
        found = []
        for wave in range(self.line_size + 2):
            if 1 <= wave < self.line_size:
                found.append(partial(self.line_stage, wave))
            if 1 <= wave <= self.line_size:
                found.append(partial(self.ring_stage, wave - 1))
            if 2 <= wave:
                found.append(partial(self.far_stage, wave - 2))
        return found

    def finish(self):
        core = self.me.core
        for a in self.every:
            self.own(a).wait()
            for i in range(self.line_size):
                for lane in range(3):
                    self.to_pair(a, i, lane, 1 - core).wait_recv()
                    self.to_pair(a, i, lane, core).wait_send()
                for way in range(2):
                    self.to_ring(a, i, way).wait_send()
                    if self.halved(a, way):
                        self.to_pair_half(a, i, way, 1 - core).wait_recv()
                        self.to_pair_half(a, i, way, core).wait_send()
                        self.onward(a, i, way).wait_send()
        for i in range(self.line_size):
            self.pass_on(lambda copy: copy.wait_send(), i)


def gather_scratch(kinds, line_size):
    sems = pltpu.SemaphoreType.DMA
    return (
        [sems((kinds,))]
        + [sems((kinds, 2, line_size)), sems((kinds, line_size))]
        + [sems((kinds, 2, line_size))] * 4
        + [sems((kinds, 3, line_size))] * 2
        + [sems((kinds, 2, line_size))] * 2
    )


def gather_kernel(ring_size, line_size, kinds, *refs):
    job = Gather(ring_size, line_size, refs[:kinds], refs[kinds : 2 * kinds], refs[2 * kinds :])
    job.begin()
    for stage in job.stages():
        stage()
    job.finish()


def gather(shards, ring_size, line_size, ident):
    kinds = len(shards)
    count = 2 * ring_size * line_size
    return pl.pallas_call(
        partial(gather_kernel, ring_size, line_size, kinds),
        in_specs=[pl.BlockSpec(memory_space=pltpu.VMEM)] * kinds,
        out_specs=[pl.BlockSpec(memory_space=pl.ANY)] * kinds,
        out_shape=[jax.ShapeDtypeStruct((count,) + piece.shape, piece.dtype) for piece in shards],
        scratch_shapes=gather_scratch(kinds, line_size),
        compiler_params=pltpu.CompilerParams(collective_id=ident, has_side_effects=True),
        name="gather_shards",
    )(*shards)


def spread(stages, tick, ticks, reach=8):
    for number, stage in enumerate(stages):
        pl.when(tick == number * (ticks * reach // 8) // len(stages))(stage)


BLOCK = 256
PART = 256


def ffn_kernel(
    x_ref,
    mixed_ref,
    wo_ref,
    cot_ref,
    pad_ref,
    gain_ref,
    wg_ref,
    wu_ref,
    wd_ref,
    out_ref,
    dmid_ref,
    dbranch_ref,
    ggate_ref,
    gup_ref,
    gdown_ref,
    dgain_ref,
    middle,
    normed,
    normed_t,
    dffn,
    out_acc,
    dn_acc,
    hidden,
    dgate,
    dup,
):
    step = pl.program_id(0)
    gain = gain_ref[...]

    @pl.when(step == 0)
    def _():
        middle[...] = mm(mixed_ref[...], wo_ref[...])
        out_acc[...] = jnp.zeros_like(out_acc)
        dn_acc[...] = jnp.zeros_like(dn_acc)

        def start(index, carry):
            rows = pl.ds(pl.multiple_of(index * SPAN, SPAN), SPAN)
            value = middle[rows, :] + x_ref[rows, :].astype(F32)
            middle[rows, :] = value
            low = (value * rms_factor(value, 1e-5) * gain).astype(BF)
            normed[rows, :] = low
            normed_t[:, rows] = jnp.transpose(low)
            pad = jnp.transpose(jnp.broadcast_to(pad_ref[index], (SPAN, SPAN)))[:, 0:1]
            dffn[rows, :] = (cot_ref[rows, :].astype(F32) * pad).astype(BF)
            return carry

        lax.fori_loop(0, CHUNKS, start, 0)

    wg, wu, wd = wg_ref[...], wu_ref[...], wd_ref[...]
    for part in range(LEN // PART):
        rows = pl.ds(part * PART, PART)
        gate, up = mm(normed[rows, :], wg), mm(normed[rows, :], wu)
        dhidden = mm_nt(dffn[rows, :], wd)
        sig = 1.0 / (1.0 + jnp.exp(-gate))
        silu = gate * sig
        hidden[rows, :] = (silu * up).astype(BF)
        dgate[rows, :] = (dhidden * up * (sig * (1.0 + gate * (1.0 - sig)))).astype(BF)
        dup[rows, :] = (dhidden * silu).astype(BF)
    gdown_ref[...] = mm_tn(hidden[...], dffn[...]).astype(BF)
    ggate_ref[...] = mm(normed_t[...], dgate[...]).astype(BF)
    gup_ref[...] = mm(normed_t[...], dup[...]).astype(BF)
    out_acc[...] += mm(hidden[...], wd)
    dn_acc[...] += mm_nt(dgate[...], wg) + mm_nt(dup[...], wu)

    @pl.when(step == pl.num_programs(0) - 1)
    def _():
        dgain_ref[...] = jnp.zeros_like(dgain_ref)

        def end(index, carry):
            rows = pl.ds(pl.multiple_of(index * SPAN, SPAN), SPAN)
            value = middle[rows, :]
            out_ref[rows, :] = (value + out_acc[rows, :]).astype(BF)
            factor = rms_factor(value, 1e-5)
            scaled = value * factor
            grad = dn_acc[rows, :]
            dscaled = grad * gain
            dmid = factor * (dscaled - scaled * jnp.mean(dscaled * scaled, axis=-1, keepdims=True))
            dmid += dffn[rows, :].astype(F32)
            dmid_ref[rows, :] = dmid
            dbranch_ref[rows, :] = dmid.astype(BF)
            dgain_ref[...] += jnp.sum(grad * scaled, axis=0, keepdims=True)
            return carry

        lax.fori_loop(0, CHUNKS, end, 0)


def feed_forward(hidden_in, mixed, w_output, cotangent, pads, gain_mid, w_ff, w_dn):
    blocks = FF // BLOCK
    square = fixed((LEN, D))
    column = pl.BlockSpec((D, BLOCK), lambda step: (0, step))
    band = pl.BlockSpec((BLOCK, D), lambda step: (step, 0))
    return pl.pallas_call(
        ffn_kernel,
        grid=(blocks,),
        in_specs=[
            square,
            square,
            fixed((WIDTH, D)),
            square,
            fixed((CHUNKS, 1, SPAN)),
            fixed((1, D)),
            column,
            pl.BlockSpec((D, BLOCK), lambda step: (0, blocks + step)),
            band,
        ],
        out_specs=[square, square, square, column, column, band, fixed((1, D))],
        out_shape=[
            jax.ShapeDtypeStruct((LEN, D), BF),
            jax.ShapeDtypeStruct((LEN, D), F32),
            jax.ShapeDtypeStruct((LEN, D), BF),
            jax.ShapeDtypeStruct((D, FF), BF),
            jax.ShapeDtypeStruct((D, FF), BF),
            jax.ShapeDtypeStruct((FF, D), BF),
            jax.ShapeDtypeStruct((1, D), F32),
        ],
        scratch_shapes=[
            pltpu.VMEM((LEN, D), F32),
            pltpu.VMEM((LEN, D), BF),
            pltpu.VMEM((D, LEN), BF),
            pltpu.VMEM((LEN, D), BF),
            pltpu.VMEM((LEN, D), F32),
            pltpu.VMEM((LEN, D), F32),
        ]
        + [pltpu.VMEM((LEN, BLOCK), BF)] * 3,
        compiler_params=pltpu.CompilerParams(vmem_limit_bytes=62 << 20),
        name="feed_forward",
    )(hidden_in, mixed, w_output, cotangent, pads, gain_mid, w_ff, w_ff, w_dn)


def pack_kernel(places, *refs):
    flats, packed = refs[: len(places) + 1], refs[len(places) + 1 :]
    for flat, (target, offsets) in zip(flats, places):
        out = packed[target]
        rows = out.shape[0]
        for j, offset in enumerate(offsets):
            out[:, offset : offset + 128] = flat[pl.ds(j, rows, stride=len(offsets)), :].astype(BF)
    packed[-1][...] = jnp.broadcast_to(flats[-1][...].astype(BF).astype(F32), packed[-1].shape)


def pack(flats, vectors, places, shapes):
    vmem = pl.BlockSpec(memory_space=pltpu.VMEM)
    return pl.pallas_call(
        partial(pack_kernel, places),
        in_specs=[vmem] * (len(flats) + 1),
        out_specs=[vmem] * (len(shapes) + 1),
        out_shape=[jax.ShapeDtypeStruct(shape, BF) for shape in shapes] + [jax.ShapeDtypeStruct((8, 128), F32)],
        name="pack_shards",
    )(*[flat.reshape(-1, 128) for flat in flats], vectors.reshape(1, 128))


def unpack_kernel(places, kinds, *refs):
    packed, flats = refs[:kinds], refs[kinds:]
    for flat, (target, offsets) in zip(flats, places):
        source = packed[target]
        rows = source.shape[0]
        for j, offset in enumerate(offsets):
            flat[pl.ds(j, rows, stride=len(offsets)), :] = source[:, offset : offset + 128]
    flats[-1][...] = packed[-1][0:1]


def unpack(packed, places):
    vmem = pl.BlockSpec(memory_space=pltpu.VMEM)
    sizes = [packed[target].shape[0] * len(offsets) for target, offsets in places] + [1]
    flats = pl.pallas_call(
        partial(unpack_kernel, places, len(packed)),
        in_specs=[vmem] * len(packed),
        out_specs=[vmem] * len(sizes),
        out_shape=[jax.ShapeDtypeStruct((size, 128), F32) for size in sizes],
        name="unpack_sums",
    )(*packed)
    return [flat.reshape(-1) for flat in flats]


def rms_factor(values, eps):
    return lax.rsqrt(jnp.mean(values * values, axis=-1, keepdims=True) + eps)


def rms_back(grad, values, factor, gain):
    scaled = values * factor
    dscaled = grad * gain
    dvalues = factor * (dscaled - scaled * jnp.mean(dscaled * scaled, axis=-1, keepdims=True))
    return dvalues, jnp.sum(grad * scaled, axis=0)


def by_kernel(sizes, ring_size, fsdp_size):
    return ring_size == 4 and fsdp_size % 4 == 0 and all(size % 8 == 0 for size in sizes)


def gather_plain(shards):
    return [lax.all_gather(piece, AXES, axis=0) for piece in shards]


def scatter_plain(grads):
    return [lax.psum_scatter(piece.astype(F32), AXES, scatter_dimension=0) for piece in grads]


def per_device(
    hidden_in,
    w_query,
    w_latent,
    w_key_up,
    w_value_up,
    w_decay,
    w_outgate,
    w_out,
    w_gate,
    w_up,
    w_down,
    vectors,
    seg_ids,
    pad_mask,
    cotangent,
    *,
    ring_size,
    fsdp_size,
):
    count = ring_size * fsdp_size
    per_group = WIDTH // GROUPS
    latents = GROUPS * LATENT
    rows_d, rows_kv, rows_ff = D // count, latents // count, FF // count
    rows_all = (rows_d, rows_kv, rows_ff)
    vec_size = (2 * D + 2 * WIDTH) // count

    own = by_kernel(rows_all, ring_size, fsdp_size) and vec_size == 128
    flat_weights = (w_query, w_latent, w_key_up, w_value_up, w_decay, w_outgate, w_out, w_gate, w_up, w_down)
    def proj(part):
        return [tile // 2 * 3 * LANES + part * LANES + tile % 2 * 128 for tile in range(WIDTH // 128)]

    def kv(part):
        return [tile // 2 * 2 * LANES + part * LANES + tile % 2 * 128 for tile in range(per_group // 128)]

    def straight(width, start=0):
        return list(range(start, start + width, 128))

    places = (
        (0, proj(0)),
        (0, straight(latents, 3 * WIDTH)),
        (1, kv(0)),
        (1, kv(1)),
        (0, proj(1)),
        (0, proj(2)),
        (2, straight(D)),
        (3, straight(FF)),
        (3, straight(FF, FF)),
        (4, straight(D)),
    )

    sums_at = (
        (0, proj(0)),
        (1, straight(latents)),
        (2, kv(0)),
        (2, kv(1)),
        (0, proj(1)),
        (0, proj(2)),
        (3, straight(D)),
        (4, straight(FF)),
        (5, straight(FF)),
        (6, straight(D)),
    )
    if own:
        shapes = (
            (rows_d, 3 * WIDTH + latents),
            (rows_kv, 2 * per_group),
            (rows_d, D),
            (rows_d, 2 * FF),
            (rows_ff, D),
        )
        in_shard, kv_shard, out_shard, ff_shard, down_shard, vec_shard = pack(flat_weights, vectors, places, shapes)
    else:

        def rows_of(piece, rows):
            return piece.astype(BF).reshape(rows, -1)

        def by_band(pieces, rows):
            bands = [rows_of(piece, rows).reshape(rows, -1, 1, LANES) for piece in pieces]
            return jnp.concatenate(bands, axis=2).reshape(rows, -1)

        in_shard = jnp.concatenate(
            [by_band((w_query, w_decay, w_outgate), rows_d), rows_of(w_latent, rows_d)], axis=1
        )
        kv_shard = by_band((w_key_up, w_value_up), rows_kv)
        out_shard = rows_of(w_out, rows_d)
        ff_shard = jnp.concatenate([rows_of(w_gate, rows_d), rows_of(w_up, rows_d)], axis=1)
        down_shard = rows_of(w_down, rows_ff)
        vec_shard = jnp.broadcast_to(lax.reduce_precision(vectors, 8, 7).reshape(1, -1), (8, vec_size))
    comm = (ring_size, fsdp_size // 2)
    early, late = (in_shard, kv_shard, vec_shard), (out_shard, ff_shard, down_shard)
    w_in, w_kv, vecs = gather(early, *comm, 0) if own else gather_plain(early)
    w_in = w_in.reshape(D, 3 * WIDTH + latents)
    w_kv = w_kv.reshape(GROUPS, LATENT, 2 * per_group)
    vecs = vecs[:, 0].reshape(-1)
    gain_in, gain_mid = vecs[:D], vecs[D : 2 * D]
    decay_bias, out_gain = vecs[2 * D : 2 * D + WIDTH], vecs[2 * D + WIDTH :]

    segs = seg_ids.astype(F32).reshape(CHUNKS, 1, SPAN)
    pads = pad_mask.astype(F32).reshape(CHUNKS, 1, SPAN)

    inputs = hidden_in.astype(F32)
    factor_in = rms_factor(inputs, 1e-5)
    normed = (inputs * factor_in * gain_in).astype(BF)
    latent = mm(normed, w_in[:, 3 * WIDTH :]).astype(BF)
    bias_row, gain_row = decay_bias.reshape(1, WIDTH), out_gain.reshape(1, WIDTH)
    query, keys, values, decay_in, gate_in, mixed, heads, states, normed_t, latent_t, *rest = mixer_fwd(
        normed, latent, w_in, w_kv, bias_row, gain_row, segs, pads, late if own else (), comm + (0, 2) if own else None
    )
    w_output, w_ff, w_dn = rest if own else gather_plain(late)
    w_output = w_output.reshape(WIDTH, D)
    w_ff = w_ff.reshape(D, 2 * FF)
    w_dn = w_dn.reshape(FF, D)
    block_out, d_middle, d_branch, grad_gate, grad_up, grad_down, d_gain_mid = feed_forward(
        hidden_in, mixed, w_output, cotangent, pads, gain_mid.reshape(1, D), w_ff, w_dn
    )

    sent = (
        grad_gate.reshape(count, rows_d, -1),
        grad_up.reshape(count, rows_d, -1),
        grad_down.reshape(count, rows_ff, -1),
    )
    saved = (query, keys, values, decay_in, gate_in, gain_row, segs, pads, heads, states)
    grad_proj, grad_lat, grad_kv, grad_out, d_normed, d_bias, d_out_gain, *rest = mixer_bwd(
        saved,
        d_branch,
        w_output,
        mixed,
        normed_t,
        latent_t,
        w_in,
        w_kv,
        sent if own else (),
        comm + (0, 3) if own else None,
    )
    own_gate, own_up, own_down = rest if own else scatter_plain(sent)
    d_inputs, d_gain_in = rms_back(d_normed, inputs, factor_in, gain_in)
    grad_input = d_middle + d_inputs
    grad_vec = jnp.concatenate([d_gain_in, d_gain_mid.reshape(-1), d_bias.reshape(-1), d_out_gain.reshape(-1)])

    grad_vec = jnp.broadcast_to(grad_vec.reshape(count, 1, vec_size), (count, 8, vec_size))
    sent = (
        grad_proj.reshape(count, rows_d, -1),
        grad_lat.reshape(count, rows_d, -1),
        grad_kv.reshape(count, rows_kv, -1),
        grad_out.reshape(count, rows_d, -1),
        grad_vec,
    )
    own_proj, own_lat, own_kv, own_out, own_vec = scatter(sent, *comm, 1) if own else scatter_plain(sent)
    sums = (own_proj, own_lat, own_kv, own_out, own_gate, own_up, own_down, own_vec)
    if own:
        return (block_out, grad_input, *unpack(sums, sums_at))
    flats = []
    for target, offsets in sums_at:
        tiles = [sums[target][:, offset : offset + 128] for offset in offsets]
        flats.append(jnp.concatenate(tiles, axis=1).reshape(-1))
    return (block_out, grad_input, *flats, own_vec[0])


def solution(mesh):
    sizes = {"ring_size": mesh.shape["dp"], "fsdp_size": mesh.shape["fsdp"]}
    rows, flat = P(AXES, None), P(AXES)
    in_specs = (rows,) + (flat,) * 13 + (rows,)
    out_specs = (rows, rows) + (flat,) * 11
    return jax.shard_map(
        partial(per_device, **sizes), mesh=mesh, in_specs=in_specs, out_specs=out_specs, check_vma=False
    )
```
